16 devices in a mesh: dp: 2 (over y, z), tp: 8 (over x, core).
Axes of the slice: x: 4, y: 2, z: 1, core: 2. Of those that a mesh axis runs over, the one named last changes fastest.
The devices are a block of a 4x4x8 slice.
Arguments:
- tokens: bfloat16 [6, 768, 5120], P('dp'), parts along dimension 0
- positions: int32 [6, 768], P('dp'), parts along dimension 0
- lengths: int32 [6], P('dp'), parts along dimension 0
- norm_attn: bfloat16 [5120], replicated
- norm_mlp: bfloat16 [5120], replicated
- q_gain: bfloat16 [128], replicated
- k_gain: bfloat16 [128], replicated
- w_query: bfloat16 [5120, 8192], P(None, 'tp')
- w_key: bfloat16 [5120, 1024], replicated
- w_value: bfloat16 [5120, 1024], replicated
- w_out: bfloat16 [8192, 5120], P('tp')
- w_gate: bfloat16 [5120, 25600], P(None, 'tp')
- w_up: bfloat16 [5120, 25600], P(None, 'tp')
- w_down: bfloat16 [25600, 5120], P('tp')
Outputs:
- output 1: bfloat16 [6, 768, 5120], P('dp'), parts along dimension 0
- output 2: bfloat16 [6, 768, 8, 128], P('dp', None, 'tp'), parts along dimension 0
- output 3: bfloat16 [6, 768, 8, 128], P('dp', None, 'tp'), parts along dimension 0
There are 2 independent parts. The reference program is written for one: setup_inputs(seed, part) draws one part's arguments, and reference() takes and returns one part's arrays. A program takes and returns all parts, laid end to end along the dimension named above; an argument that names none is the same for every part.
All inputs are finite; a program needn't handle non-finite values.
Results may differ from the reference program's by a relative error of at most 0.0149066.
Values are sent between devices in bfloat16 or wider.
A program may use at most 768 MiB of HBM per device.

```python
import jax
import jax.numpy as jnp
from jax import lax

PROMPTS = 3
SEQ_LEN = 768
HIDDEN = 5120
Q_HEADS = 64
KV_HEADS = 8
HEAD_DIM = 128
FFN_DIM = 25600
CACHE_SLOTS = 8

EPSILON = 1e-6
ROPE_THETA = 1000000.0
GROUP_SIZE = Q_HEADS // KV_HEADS
SLOT_REPEAT = CACHE_SLOTS // KV_HEADS


def make_gain(key_gain, size_n, center, spread):
    return (center + spread * jax.random.normal(key_gain, (size_n,), jnp.float32)).astype(jnp.bfloat16)


def make_matrix(key_mat, rows_n, cols_n, scale_f):
    normal_draw = jax.random.normal(key_mat, (rows_n, cols_n), jnp.float32)
    return (normal_draw * (scale_f * rows_n ** -0.5)).astype(jnp.bfloat16)


def setup_inputs(seed: int = 0, part: int = 0) -> dict:
    part_keys = jax.random.split(jax.random.fold_in(jax.random.key(seed), part), 4)
    shared_keys = jax.random.split(jax.random.key(seed + 1), 11)
    tokens = jax.random.normal(part_keys[0], (PROMPTS, SEQ_LEN, HIDDEN), jnp.float32).astype(jnp.bfloat16)
    starts = jax.random.randint(part_keys[1], (PROMPTS, 1), 0, 1024)
    positions = (starts + jnp.arange(SEQ_LEN)[None, :]).astype(jnp.int32)
    lengths = jax.random.randint(part_keys[2], (PROMPTS,), SEQ_LEN // 4, SEQ_LEN + 1)
    full_slot = jax.random.randint(part_keys[3], (), 0, PROMPTS)
    lengths = jnp.where(jnp.arange(PROMPTS) == full_slot, SEQ_LEN, lengths).astype(jnp.int32)
    return {
        'tokens': tokens,
        'positions': positions,
        'lengths': lengths,
        'norm_attn': make_gain(shared_keys[0], HIDDEN, 1.0, 0.3),
        'norm_mlp': make_gain(shared_keys[1], HIDDEN, 1.0, 0.3),
        'q_gain': make_gain(shared_keys[2], HEAD_DIM, 1.5, 0.3),
        'k_gain': make_gain(shared_keys[3], HEAD_DIM, 1.5, 0.3),
        'w_query': make_matrix(shared_keys[4], HIDDEN, Q_HEADS * HEAD_DIM, 1.0),
        'w_key': make_matrix(shared_keys[5], HIDDEN, KV_HEADS * HEAD_DIM, 1.0),
        'w_value': make_matrix(shared_keys[6], HIDDEN, KV_HEADS * HEAD_DIM, 1.0),
        'w_out': make_matrix(shared_keys[7], Q_HEADS * HEAD_DIM, HIDDEN, 2.0),
        'w_gate': make_matrix(shared_keys[8], HIDDEN, FFN_DIM, 1.0),
        'w_up': make_matrix(shared_keys[9], HIDDEN, FFN_DIM, 1.0),
        'w_down': make_matrix(shared_keys[10], FFN_DIM, HIDDEN, 1.0),
    }


def rms_scale(values, gain_vec):
    mean_sq = jnp.mean(values * values, axis=-1, keepdims=True)
    return values * lax.rsqrt(mean_sq + EPSILON) * gain_vec.astype(jnp.float32)


def rope_rotate(values, positions):
    half_dim = HEAD_DIM // 2
    inv_freq = ROPE_THETA ** (-jnp.arange(half_dim, dtype=jnp.float32) / half_dim)
    angles = positions.astype(jnp.float32)[:, :, None] * inv_freq
    cosine = jnp.cos(angles)[:, :, None, :]
    sine_tab = jnp.sin(angles)[:, :, None, :]
    first_half = values[..., :half_dim]
    second_half = values[..., half_dim:]
    return jnp.concatenate([first_half * cosine - second_half * sine_tab, second_half * cosine + first_half * sine_tab], axis=-1)


def head_attention(head_item):
    q_head, k_head, v_head, length = head_item
    scores = jnp.dot(q_head, k_head.T, preferred_element_type=jnp.float32) * HEAD_DIM ** -0.5
    row_idx = jnp.arange(SEQ_LEN)[:, None]
    col_idx = jnp.arange(SEQ_LEN)[None, :]
    allowed = (col_idx <= row_idx) & (col_idx < length)
    attn_probs = jax.nn.softmax(jnp.where(allowed, scores, -1e30), axis=-1).astype(jnp.bfloat16)
    return jnp.dot(attn_probs, v_head, preferred_element_type=jnp.float32).astype(jnp.bfloat16)


def reference(tokens, positions, lengths, norm_attn, norm_mlp, q_gain, k_gain, w_query, w_key, w_value, w_out, w_gate, w_up, w_down):
    rows_n = PROMPTS * SEQ_LEN
    tokens_f32 = tokens.astype(jnp.float32).reshape(rows_n, HIDDEN)
    normed = rms_scale(tokens_f32, norm_attn).astype(jnp.bfloat16)
    q_proj = jnp.dot(normed, w_query, preferred_element_type=jnp.float32).reshape(PROMPTS, SEQ_LEN, Q_HEADS, HEAD_DIM)
    k_proj = jnp.dot(normed, w_key, preferred_element_type=jnp.float32).reshape(PROMPTS, SEQ_LEN, KV_HEADS, HEAD_DIM)
    v_vals = jnp.dot(normed, w_value, preferred_element_type=jnp.float32).astype(jnp.bfloat16).reshape(PROMPTS, SEQ_LEN, KV_HEADS, HEAD_DIM)
    q_rot = rope_rotate(rms_scale(q_proj, q_gain), positions).astype(jnp.bfloat16)
    k_rot = rope_rotate(rms_scale(k_proj, k_gain), positions).astype(jnp.bfloat16)
    q_items = jnp.transpose(q_rot, (0, 2, 1, 3)).reshape(PROMPTS * Q_HEADS, SEQ_LEN, HEAD_DIM)
    k_items = jnp.transpose(jnp.repeat(k_rot, GROUP_SIZE, axis=2), (0, 2, 1, 3)).reshape(PROMPTS * Q_HEADS, SEQ_LEN, HEAD_DIM)
    v_items = jnp.transpose(jnp.repeat(v_vals, GROUP_SIZE, axis=2), (0, 2, 1, 3)).reshape(PROMPTS * Q_HEADS, SEQ_LEN, HEAD_DIM)
    len_items = jnp.repeat(lengths, Q_HEADS)
    attn_items = lax.map(head_attention, (q_items, k_items, v_items, len_items))
    attn_rows = jnp.transpose(attn_items.reshape(PROMPTS, Q_HEADS, SEQ_LEN, HEAD_DIM), (0, 2, 1, 3)).reshape(rows_n, Q_HEADS * HEAD_DIM)
    attn_out = jnp.dot(attn_rows, w_out, preferred_element_type=jnp.float32)
    hidden = (tokens_f32 + attn_out).astype(jnp.bfloat16).astype(jnp.float32)
    normed_mlp = rms_scale(hidden, norm_mlp).astype(jnp.bfloat16)
    gate_proj = jnp.dot(normed_mlp, w_gate, preferred_element_type=jnp.float32)
    up_proj = jnp.dot(normed_mlp, w_up, preferred_element_type=jnp.float32)
    gated = (jax.nn.silu(gate_proj) * up_proj).astype(jnp.bfloat16)
    down_proj = jnp.dot(gated, w_down, preferred_element_type=jnp.float32)
    output = (hidden + down_proj).astype(jnp.bfloat16).reshape(PROMPTS, SEQ_LEN, HIDDEN)
    valid_mask = (jnp.arange(SEQ_LEN)[None, :] < lengths[:, None])[:, :, None, None]
    k_cache = jnp.repeat(jnp.where(valid_mask, k_rot, 0).astype(jnp.bfloat16), SLOT_REPEAT, axis=2)
    v_cache = jnp.repeat(jnp.where(valid_mask, v_vals, 0).astype(jnp.bfloat16), SLOT_REPEAT, axis=2)
    return output, k_cache, v_cache
```

```python
import functools
import jax
import jax.numpy as jnp
from jax import lax
from jax.experimental import pallas as pl
from jax.experimental.pallas import tpu as pltpu
from jax.sharding import PartitionSpec as P

EPSILON = 1e-6
ROPE_THETA = 1000000.0
MESH = pl.DeviceIdType.MESH
CORES = 2
TILE = 256
UNITS = 2
GU_BUFS = 3
WD_BUFS = 4
BF = jnp.bfloat16
F32 = jnp.float32


def rope_tables(positions, half_dim):
    inv_freq = ROPE_THETA ** (-jnp.arange(half_dim, dtype=F32) / half_dim)
    angles = positions.astype(F32)[:, None] * inv_freq
    cosine, sine = jnp.cos(angles), jnp.sin(angles)
    return jnp.concatenate([cosine, cosine], axis=-1), jnp.concatenate([-sine, sine], axis=-1)


def dot(a, b):
    return jnp.dot(a, b, preferred_element_type=F32)


def layer_kernel(tp, prompts, seq, head_dim, kv_heads, dims,
                 tokens, cos_h, sin_h, lens, n_attn, n_mlp, q_gain, k_gain, wq, wk, wv, wo, wg, wu, wdn,
                 ho, kc, vc,
                 n2, act, kk, vv, kco, vco, cosb, sinb, gu, wd, pp, xp, land, ownh,
                 s_x, s_cs, s_gu, s_wd, s_stage, s_xp, s_res, s_kv, s_own,
                 rs_send, rs_recv, ag_send, ag_recv, dd_send, dd_recv):
    hidden, width_q, width_f = dims
    chips = tp // CORES
    half = hidden // CORES
    unit = half // UNITS
    unit_tiles = unit // TILE
    rows_b = seq // chips
    heads = width_q // head_dim
    q_tiles = width_q // TILE
    f_tiles = width_f // head_dim
    n_tiles = hidden // TILE
    per_ar = 6 * UNITS
    lanes = head_dim

    me = lax.axis_index('tp')
    core = lax.rem(me, CORES)
    chip = me // CORES
    ring = lax.rem(chip + core * (chips - 2 * chip), chips)
    nxt = CORES * lax.rem(chip + chips + 1 - 2 * core, chips) + core
    prv = CORES * lax.rem(chip + chips - 1 + 2 * core, chips) + core
    partner = me + 1 - 2 * core
    kv_col = pl.multiple_of((me // (tp // kv_heads)) * head_dim, head_dim)

    barrier = pltpu.get_barrier_semaphore()
    for other in (nxt, prv, partner):
        pl.semaphore_signal(barrier, inc=1, device_id={'tp': other}, device_id_type=MESH)
    pl.semaphore_wait(barrier, 3)

    def remote(src, dst, send, recv, to):
        return pltpu.make_async_remote_copy(src_ref=src, dst_ref=dst, send_sem=send, recv_sem=recv,
                                            device_id={'tp': to}, device_id_type=MESH)

    def local(src, dst, sem):
        return pltpu.make_async_copy(src, dst, sem)

    def block_rows(b):
        return pl.ds(pl.multiple_of(b * rows_b, rows_b), rows_b)

    def ho_block(c, g, b, side):
        rows = pl.ds(pl.multiple_of(c * seq + b * rows_b, rows_b), rows_b)
        return ho.at[rows, pl.ds(pl.multiple_of(side * half + g * unit, TILE), unit)]

    def send_partial(e, c, g):
        i, par = lax.rem(c, prompts), lax.rem(c, 2)
        rows = block_rows(lax.rem(ring + 2 * chips - 1 - e, chips))
        u = i * UNITS + g
        if e == 0:
            local(xp.at[u], xp.at[u], s_xp.at[u]).wait()
        else:
            local(land.at[par, g, e - 1], land.at[par, g, e - 1], rs_recv.at[par, g, e - 1]).wait()
        mine, theirs, came = pp.at[u, rows], xp.at[u, rows], land.at[par, g, max(e - 1, 0)]

        def add(r, _):
            rr = pl.ds(pl.multiple_of(r * 16, 16), 16)
            total = mine[rr, :].astype(F32) + theirs[rr, :].astype(F32)
            if e > 0:
                total = total + came[rr, :].astype(F32)
            mine[rr, :] = total.astype(BF)
            return 0
        lax.fori_loop(0, rows_b // 16, add, 0)
        remote(mine, land.at[par, g, e], rs_send.at[par, g, e], rs_recv.at[par, g, e], nxt).start()

    def finish_sum(c, g):
        i, par = lax.rem(c, prompts), lax.rem(c, 2)
        u = i * UNITS + g
        rows = block_rows(ring)
        local(land.at[par, g, 2], land.at[par, g, 2], rs_recv.at[par, g, 2]).wait()

        @pl.when(c < prompts)
        def _():
            local(ownh.at[u], ownh.at[u], s_res.at[u]).wait()
        mine, theirs, came, own = pp.at[u, rows], xp.at[u, rows], land.at[par, g, 2], ownh.at[u]

        def add(r, _):
            rr = pl.ds(pl.multiple_of(r * 16, 16), 16)
            total = came[rr, :].astype(F32) + (mine[rr, :].astype(F32) + theirs[rr, :].astype(F32))
            own[rr, :] = (own[rr, :].astype(F32) + total).astype(BF)
            return 0
        lax.fori_loop(0, rows_b // 16, add, 0)
        place = ho_block(c, g, ring, core)
        remote(own, place, ag_send.at[par, g, 0], ag_recv.at[par, g, 0], nxt).start()
        remote(own, place, dd_send.at[par, g, 0], dd_recv.at[par, g, 0], partner).start()
        local(own, place, s_own.at[par, g]).start()

    def pass_on(e, c, g):
        par = lax.rem(c, 2)
        place = ho_block(c, g, lax.rem(ring + 2 * chips - e, chips), core)
        local(place, place, ag_recv.at[par, g, e - 1]).wait()
        if e < 3:
            remote(place, place, ag_send.at[par, g, e], ag_recv.at[par, g, e], nxt).start()
        remote(place, place, dd_send.at[par, g, e], dd_recv.at[par, g, e], partner).start()

    def settle(c, g):
        par = lax.rem(c, 2)
        u = lax.rem(c, prompts) * UNITS + g
        place = ho_block(c, g, ring, core)
        local(ownh.at[u], ownh.at[u], s_own.at[par, g]).wait()
        for e in range(3):
            local(land.at[par, g, e], land.at[par, g, e], rs_send.at[par, g, e]).wait()
            local(place, place, ag_send.at[par, g, e]).wait()
        for e in range(4):
            local(place, place, dd_send.at[par, g, e]).wait()
        for e in range(4):
            local(place, place, dd_recv.at[par, g, e]).wait()

    def slot(k):
        c, j = k // per_ar, lax.rem(k, per_ar)
        e, g = j // UNITS, lax.rem(j, UNITS)
        live = c < 2 * prompts
        for s in range(3):
            @pl.when(live & (e == s))
            def _(s=s):
                send_partial(s, c, g)

        @pl.when(live & (e == 3))
        def _():
            finish_sum(c, g)
        for s in range(2):
            @pl.when(live & (e == 4 + s))
            def _(s=s):
                pass_on(s + 1, c, g)

        @pl.when((e == 0) & (c > 0))
        def _():
            pass_on(3, c - 1, g)

        @pl.when((e == 1) & (c > 0))
        def _():
            settle(c - 1, g)

    def run_slots(lo, hi):
        def body(k, _):
            slot(k)
            return 0
        lax.fori_loop(lo, hi, body, 0)

    def q_tile(t):
        b = lax.rem(t, GU_BUFS)
        return local(wq.at[:, pl.ds(pl.multiple_of(t * TILE, TILE), TILE)], gu.at[b], s_gu.at[b, 0])

    def kv_tile():
        b = q_tiles % GU_BUFS
        return (local(wk.at[:, pl.ds(kv_col, lanes)], gu.at[b, :, pl.ds(0, lanes)], s_gu.at[b, 0]),
                local(wv.at[:, pl.ds(kv_col, lanes)], gu.at[b, :, pl.ds(lanes, lanes)], s_gu.at[b, 1]))

    def f_tile(t):
        b = lax.rem(t, GU_BUFS)
        cols = pl.ds(pl.multiple_of(t * lanes, lanes), lanes)
        return (local(wg.at[:, cols], gu.at[b, :, pl.ds(0, lanes)], s_gu.at[b, 0]),
                local(wu.at[:, cols], gu.at[b, :, pl.ds(lanes, lanes)], s_gu.at[b, 1]))

    def tile_place(n):
        g, w = n // (2 * unit_tiles), lax.rem(n, 2 * unit_tiles)
        away = w < unit_tiles
        t = lax.rem(w, unit_tiles)
        side = jnp.where(away, 1 - core, core)
        return g, away, t, pl.ds(pl.multiple_of(side * half + g * unit + t * TILE, TILE), TILE)

    def o_tile(n):
        b = lax.rem(n, WD_BUFS)
        return local(wo.at[:, tile_place(n)[3]], wd.at[b, pl.ds(0, width_q), :], s_wd.at[b])

    def d_tile(n):
        b = lax.rem(n, WD_BUFS)
        return local(wdn.at[:, tile_place(n)[3]], wd.at[b], s_wd.at[b])

    def project(lhs, depth, fetch, i, group0, bounds):
        def body(n, _):
            @pl.when(n + WD_BUFS - 1 < n_tiles)
            def _():
                fetch(n + WD_BUFS - 1).start()
            fetch(n).wait()
            g, away, t, _cols = tile_place(n)
            u = jnp.where(away, prompts * UNITS, i * UNITS + g)
            cols = pl.ds(pl.multiple_of(t * TILE, TILE), TILE)

            @pl.when(away & (group0 + g > 0))
            def _():
                local(pp.at[u, :, cols], pp.at[u, :, cols], s_stage.at[t]).wait()
            pp[u, :, cols] = dot(lhs[...], wd[lax.rem(n, WD_BUFS), :depth, :]).astype(BF)

            @pl.when(away)
            def _():
                to = i * UNITS + g
                remote(pp.at[u, :, cols], xp.at[to, :, cols], s_stage.at[t], s_xp.at[to], partner).start()
            run_slots(*bounds(n))
            return 0
        lax.fori_loop(0, n_tiles, body, 0)

    def rms_rows(gain):
        def body(r, _):
            rr = pl.ds(pl.multiple_of(r * 16, 16), 16)
            v = n2[rr, :].astype(F32)
            scale = lax.rsqrt(jnp.mean(v * v, axis=-1, keepdims=True) + EPSILON)
            n2[rr, :] = (v * scale * gain[...].astype(F32)).astype(BF)
            return 0
        lax.fori_loop(0, seq // 16, body, 0)

    def turned(v, gain):
        v = v * lax.rsqrt(jnp.mean(v * v, axis=-1, keepdims=True) + EPSILON) * gain[...].astype(F32)
        return v * cosb[...] + pltpu.roll(v, lanes // 2, 1) * sinb[...]

    def load_x(i):
        rows = pl.ds(pl.multiple_of(i * seq, seq), seq)
        return (local(tokens.at[rows, :], n2, s_x),
                local(cos_h.at[rows, :], cosb, s_cs.at[0]),
                local(sin_h.at[rows, :], sinb, s_cs.at[1]))

    def load_h(i):
        return local(ho.at[pl.ds(pl.multiple_of(i * seq, seq), seq), :], n2, s_x)

    for cp in load_x(0):
        cp.start()
    for t in range(GU_BUFS - 1):
        q_tile(t).start()
    for n in range(WD_BUFS - 1):
        o_tile(n).start()
    for i in range(prompts):
        for g in range(UNITS):
            rows = pl.ds(pl.multiple_of(i * seq + ring * rows_b, rows_b), rows_b)
            cols = pl.ds(pl.multiple_of(core * half + g * unit, TILE), unit)
            local(tokens.at[rows, cols], ownh.at[i * UNITS + g], s_res.at[i * UNITS + g]).start()

    w_q, w_h, w_o = 4, 2, 1
    weight_a = w_q * (q_tiles + 1) + w_h * heads + w_o * n_tiles

    def attention_phase(i, _):
        def upto(w):
            return jnp.maximum(0, ((i - 1) * weight_a + w) * per_ar // ((prompts - 1) * weight_a))

        for cp in load_x(i):
            cp.wait()
        rms_rows(n_attn)
        length = lens[i]

        def q_body(t, _):
            @pl.when(t + GU_BUFS - 1 < q_tiles)
            def _():
                q_tile(t + GU_BUFS - 1).start()

            @pl.when(t + GU_BUFS - 1 == q_tiles)
            def _():
                for cp in kv_tile():
                    cp.start()
            q_tile(t).wait()
            y = dot(n2[...], gu[lax.rem(t, GU_BUFS)])
            for s in range(TILE // lanes):
                act[:, pl.ds(pl.multiple_of(t * TILE + s * lanes, lanes), lanes)] = turned(y[:, s * lanes:(s + 1) * lanes], q_gain).astype(BF)
            run_slots(upto(t * w_q), upto((t + 1) * w_q))
            return 0
        lax.fori_loop(0, q_tiles, q_body, 0)
        for cp in kv_tile():
            cp.wait()
        y = dot(n2[...], gu[q_tiles % GU_BUFS])
        k_rot = turned(y[:, :lanes], k_gain).astype(BF)
        v_val = y[:, lanes:].astype(BF)
        kk[...] = k_rot
        vv[...] = v_val
        valid = lax.broadcasted_iota(jnp.int32, (seq, lanes), 0) < length
        kco[...] = jnp.where(valid, k_rot.astype(F32), 0.0).astype(BF)
        vco[...] = jnp.where(valid, v_val.astype(F32), 0.0).astype(BF)
        rows = pl.ds(pl.multiple_of(i * seq, seq), seq)
        caches = (local(kco, kc.at[rows, :], s_kv.at[0]), local(vco, vc.at[rows, :], s_kv.at[1]))
        for cp in caches:
            cp.start()

        @pl.when(i + 1 < prompts)
        def _():
            for cp in load_x(i + 1):
                cp.start()
            for t in range(GU_BUFS - 1):
                q_tile(t).start()

        @pl.when(i + 1 == prompts)
        def _():
            for t in range(GU_BUFS - 1):
                for cp in f_tile(t):
                    cp.start()
        run_slots(upto(q_tiles * w_q), upto((q_tiles + 1) * w_q))
        base = (q_tiles + 1) * w_q
        q_rows = seq // 3

        def head_body(hd, _):
            q_cols = pl.ds(pl.multiple_of(hd * lanes, lanes), lanes)
            o_cols = pl.ds(pl.multiple_of(width_q + hd * lanes, lanes), lanes)
            for qb in range(3):
                span = (qb + 1) * q_rows
                q = act[qb * q_rows:span, q_cols]
                s = lax.dot_general(q, kk[:span, :], (((1,), (1,)), ((), ())), preferred_element_type=F32) * head_dim ** -0.5
                row = lax.broadcasted_iota(jnp.int32, (q_rows, span), 0) + qb * q_rows
                col = lax.broadcasted_iota(jnp.int32, (q_rows, span), 1)
                s = jnp.where((col <= row) & (col < length), s, -1e30)
                p = jnp.exp(s - jnp.max(s, axis=-1, keepdims=True))
                p = p * (1.0 / jnp.sum(p, axis=-1, keepdims=True))
                act[qb * q_rows:span, o_cols] = dot(p.astype(BF), vv[:span, :]).astype(BF)
            run_slots(upto(base + hd * w_h), upto(base + (hd + 1) * w_h))
            return 0
        lax.fori_loop(0, heads, head_body, 0)
        for cp in caches:
            cp.wait()
        base2 = base + heads * w_h
        project(act.at[:, pl.ds(width_q, width_q)], width_q, o_tile, i, i * UNITS,
                lambda n: (upto(base2 + n * w_o), upto(base2 + (n + 1) * w_o)))

        @pl.when(i + 1 < prompts)
        def _():
            for n in range(WD_BUFS - 1):
                o_tile(n).start()

        @pl.when(i + 1 == prompts)
        def _():
            for n in range(WD_BUFS - 1):
                d_tile(n).start()
        return 0
    lax.fori_loop(0, prompts, attention_phase, 0)

    lead = 2 * UNITS
    run_slots(per_ar, per_ar + lead)
    load_h(0).start()
    stride = (2 * prompts - 2 - 1) * per_ar - lead

    def mlp_phase(i, _):
        k0 = per_ar + lead + i * stride // (prompts - 1)
        k1 = (i + 2) * per_ar + lead
        k2 = jnp.minimum(per_ar + lead + (i + 1) * stride // (prompts - 1), (2 * prompts - 1) * per_ar)
        k1 = jnp.minimum(k1, k2)
        load_h(i).wait()
        rms_rows(n_mlp)

        def f_body(t, _):
            @pl.when(t + GU_BUFS - 1 < f_tiles)
            def _():
                for cp in f_tile(t + GU_BUFS - 1):
                    cp.start()
            for cp in f_tile(t):
                cp.wait()
            y = dot(n2[...], gu[lax.rem(t, GU_BUFS)])
            gate, up = y[:, :lanes], y[:, lanes:]
            act[:, pl.ds(pl.multiple_of(t * lanes, lanes), lanes)] = (gate * jax.nn.sigmoid(gate) * up).astype(BF)
            run_slots(k0 + t * (k1 - k0) // f_tiles, k0 + (t + 1) * (k1 - k0) // f_tiles)
            return 0
        lax.fori_loop(0, f_tiles, f_body, 0)

        @pl.when(i + 1 < prompts)
        def _():
            load_h(i + 1).start()
            for t in range(GU_BUFS - 1):
                for cp in f_tile(t):
                    cp.start()
        project(act, width_f, d_tile, i, (prompts + i) * UNITS,
                lambda n: (k1 + n * (k2 - k1) // n_tiles, k1 + (n + 1) * (k2 - k1) // n_tiles))

        @pl.when(i + 1 < prompts)
        def _():
            for n in range(WD_BUFS - 1):
                d_tile(n).start()
        return 0
    lax.fori_loop(0, prompts, mlp_phase, 0)

    run_slots((2 * prompts - 1) * per_ar, 2 * prompts * per_ar + lead)
    for t in range(unit_tiles):
        cols = pl.ds(t * TILE, TILE)
        local(pp.at[prompts * UNITS, :, cols], pp.at[prompts * UNITS, :, cols], s_stage.at[t]).wait()


def layer_body(tokens, positions, lengths, norm_attn, norm_mlp, q_gain, k_gain, w_query, w_key, w_value, w_out, w_gate, w_up, w_down, tp_size):
    prompts, seq, hidden = tokens.shape
    head_dim = q_gain.shape[0]
    width_q, width_f = w_query.shape[1], w_gate.shape[1]
    kv_heads = w_key.shape[1] // head_dim
    chips = tp_size // CORES
    half = hidden // CORES
    unit = half // UNITS
    rows_n = prompts * seq
    cos_t, sin_t = rope_tables(positions.reshape(rows_n), head_dim // 2)
    any_spec = pl.BlockSpec(memory_space=pl.ANY)
    vmem = pl.BlockSpec(memory_space=pltpu.VMEM)
    smem = pl.BlockSpec(memory_space=pltpu.SMEM)
    kernel = functools.partial(layer_kernel, tp_size, prompts, seq, head_dim, kv_heads, (hidden, width_q, width_f))
    dma = pltpu.SemaphoreType.DMA
    pieces = prompts * UNITS
    ho, kc, vc = pl.pallas_call(
        kernel,
        name='decoder_layer',
        out_shape=(jax.ShapeDtypeStruct((2 * rows_n, hidden), BF),
                   jax.ShapeDtypeStruct((rows_n, head_dim), BF),
                   jax.ShapeDtypeStruct((rows_n, head_dim), BF)),
        in_specs=[any_spec, any_spec, any_spec, smem, vmem, vmem, vmem, vmem] + [any_spec] * 7,
        out_specs=(any_spec, any_spec, any_spec),
        scratch_shapes=[
            pltpu.VMEM((seq, hidden), BF),
            pltpu.VMEM((seq, width_f), BF),
            pltpu.VMEM((seq, head_dim), BF), pltpu.VMEM((seq, head_dim), BF),
            pltpu.VMEM((seq, head_dim), BF), pltpu.VMEM((seq, head_dim), BF),
            pltpu.VMEM((seq, head_dim), F32), pltpu.VMEM((seq, head_dim), F32),
            pltpu.VMEM((GU_BUFS, hidden, TILE), BF),
            pltpu.VMEM((WD_BUFS, width_f, TILE), BF),
            pltpu.VMEM((pieces + 1, seq, unit), BF),
            pltpu.VMEM((pieces, seq, unit), BF),
            pltpu.VMEM((2, UNITS, 3, seq // chips, unit), BF),
            pltpu.VMEM((pieces, seq // chips, unit), BF),
            dma, dma((2,)), dma((GU_BUFS, 2)), dma((WD_BUFS,)), dma((unit // TILE,)), dma((pieces,)), dma((pieces,)), dma((2,)), dma((2, UNITS)),
            dma((2, UNITS, 3)), dma((2, UNITS, 3)), dma((2, UNITS, 3)), dma((2, UNITS, 3)), dma((2, UNITS, 4)), dma((2, UNITS, 4)),
        ],
        compiler_params=pltpu.CompilerParams(collective_id=0, has_side_effects=True, vmem_limit_bytes=67043328),
    )(tokens.reshape(rows_n, hidden), cos_t, sin_t, lengths, norm_attn[None], norm_mlp[None], q_gain[None], k_gain[None],
      w_query, w_key, w_value, w_out, w_gate, w_up, w_down)
    shape = (prompts, seq, 1, head_dim)
    return ho[rows_n:].reshape(prompts, seq, hidden), kc.reshape(shape), vc.reshape(shape)


def solution(mesh):
    body = functools.partial(layer_body, tp_size=mesh.shape['tp'])
    in_specs = (P('dp', None, None), P('dp', None), P('dp'), P(), P(), P(), P(), P(None, 'tp'), P(), P(), P('tp', None), P(None, 'tp'), P(None, 'tp'), P('tp', None))
    out_specs = (P('dp', None, None), P('dp', None, 'tp', None), P('dp', None, 'tp', None))
    return jax.shard_map(body, mesh=mesh, in_specs=in_specs, out_specs=out_specs, check_vma=False)
```

```python
import functools
import jax
import jax.numpy as jnp
from jax import lax
from jax.experimental import pallas as pl
from jax.experimental.pallas import tpu as pltpu
from jax.sharding import PartitionSpec as P

EPSILON = 1e-6
ROPE_THETA = 1000000.0
MESH = pl.DeviceIdType.MESH
CORES = 2
TILE = 256
UNITS = 5
HOPS = 6
GU_BUFS = 3
X_PARTS = 4
HEADS_AT_ONCE = 4
BF = jnp.bfloat16
F32 = jnp.float32


def dot(a, b):
    return jnp.dot(a, b, preferred_element_type=F32)


def dot_nt(a, b):
    return lax.dot_general(a, b, (((1,), (1,)), ((), ())), preferred_element_type=F32)


def pick(i, values):
    out = values[0]
    for n, v in enumerate(values[1:], 1):
        out = jnp.where(i >= n, v, out)
    return out


def layer_kernel(tp, prompts, seq, head_dim, kv_heads, dims,
                 tokens, positions, lens, n_attn, n_mlp, q_gain, k_gain, freq, wq, wk, wv, wo, wg, wu, wdn,
                 ho, kc, vc,
                 n2, act, kk, vt, kco, vco, cosb, sinb, ybuf, seen, tri, gains, gu, wd, pp, xp, land, ownh,
                 s_x, s_gu, s_wd, s_stage, s_xp, s_res, s_kv, s_own,
                 rs_send, rs_recv, ag_send, ag_recv, dd_send, dd_recv):
    hidden, width_q, width_f = dims
    chips = tp // CORES
    half = hidden // CORES
    unit = half // UNITS
    rows_b = seq // chips
    heads = width_q // head_dim
    q_tiles = width_q // TILE
    f_tiles = width_f // head_dim
    n_tiles = CORES * UNITS
    per_ar = HOPS * UNITS
    lead = UNITS + 1
    last = 2 * prompts - 1
    lanes = head_dim
    o_bufs = 2 * (width_f // width_q)
    row_groups = min(4, seq // X_PARTS // 16)
    norm_tiles = n_tiles - 2
    norm_rows = seq // norm_tiles
    span_q = min(lanes, seq)
    hidden_score = -1e30 * head_dim ** 0.5
    to_exp2 = head_dim ** -0.5 * 1.4426950408889634

    me = lax.axis_index('tp')
    core = lax.rem(me, CORES)
    chip = me // CORES
    ring = lax.rem(chip + core * (chips - 2 * chip), chips)
    nxt = CORES * lax.rem(chip + chips + 1 - 2 * core, chips) + core
    prv = CORES * lax.rem(chip + chips - 1 + 2 * core, chips) + core
    partner = me + 1 - 2 * core
    kv_col = pl.multiple_of((me // (tp // kv_heads)) * head_dim, head_dim)

    def remote(src, dst, send, recv, to):
        return pltpu.make_async_remote_copy(src_ref=src, dst_ref=dst, send_sem=send, recv_sem=recv,
                                            device_id={'tp': to}, device_id_type=MESH)

    def local(src, dst, sem):
        return pltpu.make_async_copy(src, dst, sem)

    def await_copy(ref, sem):
        local(ref, ref, sem).wait()

    def block_rows(b):
        return pl.ds(pl.multiple_of(b * rows_b, rows_b), rows_b)

    def a_tile(t):
        b = t % GU_BUFS
        if t == 0:
            return (local(wk.at[:, pl.ds(kv_col, lanes)], gu.at[b, :, pl.ds(0, lanes)], s_gu.at[b, 0]),
                    local(wv.at[:, pl.ds(kv_col, lanes)], gu.at[b, :, pl.ds(lanes, lanes)], s_gu.at[b, 1]))
        return (local(wq.at[:, pl.ds((t - 1) * TILE, TILE)], gu.at[b], s_gu.at[b, 0]),)

    def f_tile(t):
        b = lax.rem(t, GU_BUFS)
        cols = pl.ds(pl.multiple_of(t * lanes, lanes), lanes)
        return (local(wg.at[:, cols], gu.at[b, :, pl.ds(0, lanes)], s_gu.at[b, 0]),
                local(wu.at[:, cols], gu.at[b, :, pl.ds(lanes, lanes)], s_gu.at[b, 1]))

    def start_all(copies):
        for cp in copies:
            cp.start()

    def wait_all(copies):
        for cp in copies:
            cp.wait()

    def out_cols(n):
        side = jnp.where(lax.rem(n, 2) == 0, 1 - core, core)
        return pl.ds(pl.multiple_of(side * half + (n // 2) * unit, unit), unit)

    def o_place(n):
        b = lax.rem(n, o_bufs)
        return wd.at[b // (o_bufs // 2), pl.ds(pl.multiple_of(lax.rem(b, o_bufs // 2) * width_q, width_q), width_q), :]

    def o_tile(n):
        return local(wo.at[:, out_cols(n)], o_place(n), s_wd.at[lax.rem(n, o_bufs)])

    def d_place(n):
        return wd.at[lax.rem(n, 2)]

    def d_tile(n):
        return local(wdn.at[:, out_cols(n)], d_place(n), s_wd.at[lax.rem(n, 2)])

    def load_rows(src, i):
        part = seq // X_PARTS
        return [local(src.at[pl.ds(pl.multiple_of(i * seq + b * part, part), part), :], n2.at[pl.ds(b * part, part), :], s_x.at[b])
                for b in range(X_PARTS)]

    start_all(load_rows(tokens, 0))
    for t in range(GU_BUFS - 1):
        start_all(a_tile(t))
    for n in range(o_bufs - 1):
        o_tile(n).start()
    for i in range(prompts):
        for g in range(UNITS):
            rows = pl.ds(pl.multiple_of(i * seq + ring * rows_b, rows_b), rows_b)
            cols = pl.ds(pl.multiple_of(core * half + g * unit, unit), unit)
            local(tokens.at[rows, cols], ownh.at[i * UNITS + g], s_res.at[i * UNITS + g]).start()
    barrier = pltpu.get_barrier_semaphore()
    for other in (nxt, prv, partner):
        pl.semaphore_signal(barrier, inc=1, device_id={'tp': other}, device_id_type=MESH)

    for v, gain in enumerate((n_attn, n_mlp)):
        wide = gain[...].astype(F32)
        for j in range(hidden // lanes):
            gains[v, :, j * lanes:(j + 1) * lanes] = jnp.broadcast_to(wide[None, j * lanes:(j + 1) * lanes], (16, lanes))
    key_at = lax.broadcasted_iota(jnp.int32, (span_q, span_q), 0)
    tri[...] = jnp.where(key_at <= lax.broadcasted_iota(jnp.int32, (span_q, span_q), 1), 1.0, 0.0)
    pl.semaphore_wait(barrier, 3)

    def ho_block(c, g, b, side):
        rows = pl.ds(pl.multiple_of(c * seq + b * rows_b, rows_b), rows_b)
        return ho.at[rows, pl.ds(pl.multiple_of(side * half + g * unit, unit), unit)]

    def send_partial(e, c, g):
        par = lax.rem(c, 2)
        u = par * UNITS + g
        rows = block_rows(lax.rem(ring + 2 * chips - 1 - e, chips))
        with jax.named_scope('w_rs'):
            if e == 0:
                await_copy(xp.at[u], s_xp.at[u])
            else:
                await_copy(land.at[par, g, e - 1], rs_recv.at[par, g, e - 1])
        mine, theirs, came = pp.at[u, rows], xp.at[u, rows], land.at[par, g, max(e - 1, 0)]

        def add(r, _):
            rr = pl.ds(pl.multiple_of(r * 16, 16), 16)
            total = mine[rr, :].astype(F32) + theirs[rr, :].astype(F32)
            if e > 0:
                total = total + came[rr, :].astype(F32)
            mine[rr, :] = total.astype(BF)
            return 0
        lax.fori_loop(0, rows_b // 16, add, 0, unroll=2)
        remote(mine, land.at[par, g, e], rs_send.at[par, g, e], rs_recv.at[par, g, e], nxt).start()

    def finish_sum(c, g):
        par = lax.rem(c, 2)
        u, w = par * UNITS + g, lax.rem(c, prompts) * UNITS + g
        rows = block_rows(ring)
        with jax.named_scope('w_rs3'):
            await_copy(land.at[par, g, 2], rs_recv.at[par, g, 2])

        @pl.when(c < prompts)
        def _():
            await_copy(ownh.at[w], s_res.at[w])
        mine, theirs, came, own = pp.at[u, rows], xp.at[u, rows], land.at[par, g, 2], ownh.at[w]

        def add(r, _):
            rr = pl.ds(pl.multiple_of(r * 16, 16), 16)
            total = came[rr, :].astype(F32) + (mine[rr, :].astype(F32) + theirs[rr, :].astype(F32))
            own[rr, :] = (own[rr, :].astype(F32) + total).astype(BF)
            return 0
        lax.fori_loop(0, rows_b // 16, add, 0, unroll=2)
        place = ho_block(c, g, ring, core)
        remote(own, place, ag_send.at[par, g, 0], ag_recv.at[par, g, 0], nxt).start()
        remote(own, place, dd_send.at[par, g, 0], dd_recv.at[par, g, 0], partner).start()
        local(own, place, s_own.at[par, g]).start()

    def pass_on(e, c, g):
        par = lax.rem(c, 2)
        place = ho_block(c, g, lax.rem(ring + 2 * chips - e, chips), core)
        with jax.named_scope('w_ag'):
            await_copy(place, ag_recv.at[par, g, e - 1])
        if e < 3:
            remote(place, place, ag_send.at[par, g, e], ag_recv.at[par, g, e], nxt).start()
        remote(place, place, dd_send.at[par, g, e], dd_recv.at[par, g, e], partner).start()
        if e == 1:
            await_copy(place, dd_recv.at[par, g, 0])
            for s in range(3):
                await_copy(land.at[par, g, s], rs_send.at[par, g, s])

    def settle(c, g):
        par = lax.rem(c, 2)
        place = ho_block(c, g, ring, core)
        await_copy(land.at[par, g, 0], s_own.at[par, g])
        for e in range(3):
            await_copy(place, ag_send.at[par, g, e])
        for e in range(4):
            await_copy(place, dd_send.at[par, g, e])
        for e in range(1, 4):
            await_copy(place, dd_recv.at[par, g, e])

    def slot(k):
        c = k // per_ar
        j = k - c * per_ar
        e, g = j // UNITS, lax.rem(j, UNITS)
        for s in range(3):
            @pl.when(e == s)
            def _(s=s):
                send_partial(s, c, g)

        @pl.when(e == 3)
        def _():
            finish_sum(c, g)
        for s in range(2):
            @pl.when(e == 4 + s)
            def _(s=s):
                pass_on(s + 1, c, g)

        @pl.when((e == 0) & (c > 0))
        def _():
            pass_on(3, c - 1, g)

        @pl.when((c > 0) & (j >= 1) & (j <= UNITS))
        def _():
            settle(c - 1, j - 1)

    def run_slots(lo, hi):
        def body(k, _):
            slot(k)
            return 0
        lax.fori_loop(lo, hi, body, 0)

    def norm_all(v):
        part = seq // X_PARTS
        for b in range(X_PARTS):
            await_copy(n2.at[pl.ds(b * part, part), :], s_x.at[b])

            def scales(r, _):
                for q in range(row_groups):
                    rr = pl.ds(pl.multiple_of(b * part + (r * row_groups + q) * 16, 16), 16)
                    acc = jnp.zeros((16, lanes), F32)
                    for j in range(hidden // lanes):
                        x = n2[rr, j * lanes:(j + 1) * lanes].astype(F32)
                        acc = acc + x * x
                    scale = lax.rsqrt(jnp.sum(acc, axis=-1, keepdims=True) * (1.0 / hidden) + EPSILON)
                    ybuf[0, rr, :lanes] = jnp.broadcast_to(scale, (16, lanes))
                return 0
            lax.fori_loop(0, part // 16 // row_groups, scales, 0)

        def apply(r, _):
            rr = pl.ds(pl.multiple_of(r * 16, 16), 16)
            scale = ybuf[0, rr, :lanes]
            for j in range(hidden // lanes):
                cols = slice(j * lanes, (j + 1) * lanes)
                n2[rr, cols] = (n2[rr, cols].astype(F32) * scale * gains[v, :, cols]).astype(BF)
            return 0
        lax.fori_loop(0, seq // 16, apply, 0)

    def norm_some(v, first):
        for q in range(norm_rows // 16):
            rr = pl.ds(pl.multiple_of(first + q * 16, 16), 16)
            acc = jnp.zeros((16, lanes), F32)
            for j in range(hidden // lanes):
                x = n2[rr, j * lanes:(j + 1) * lanes].astype(F32)
                acc = acc + x * x
            scale = jnp.broadcast_to(lax.rsqrt(jnp.sum(acc, axis=-1, keepdims=True) * (1.0 / hidden) + EPSILON), (16, lanes))
            for j in range(hidden // lanes):
                cols = slice(j * lanes, (j + 1) * lanes)
                n2[rr, cols] = (n2[rr, cols].astype(F32) * scale * gains[v, :, cols]).astype(BF)

    def project(lhs, fetch, place, ahead, c, v, bounds, begin, loaded):
        par = lax.rem(c, 2)

        def tile(n, norm):
            @pl.when(n + ahead < n_tiles)
            def _():
                fetch(n + ahead).start()
            with jax.named_scope('w_wd'):
                fetch(n).wait()
            g = n // 2
            away = lax.rem(n, 2) == 0
            count = c * UNITS + g
            stage = lax.rem(count, 2)
            u = jnp.where(away, 2 * UNITS + stage, par * UNITS + g)

            @pl.when(away & (count >= 2))
            def _():
                await_copy(pp.at[u], s_stage.at[stage])
            if norm:
                norm_some(v, pl.multiple_of((n - 2) * norm_rows, 16))
            pp[u] = dot(lhs[...], place(n)[...]).astype(BF)

            @pl.when(away)
            def _():
                to = par * UNITS + g
                remote(pp.at[u], xp.at[to], s_stage.at[stage], s_xp.at[to], partner).start()
            run_slots(*bounds(n))

        def plain(n, _):
            tile(n, False)
            return 0

        def normed(n, _):
            tile(n, True)
            return 0
        lax.fori_loop(0, 1, plain, 0)
        begin()
        lax.fori_loop(1, 2, plain, 0)
        loaded()
        lax.fori_loop(2, n_tiles, normed, 0)

    def turned(v, gain):
        v = v * lax.rsqrt(jnp.mean(v * v, axis=-1, keepdims=True) + EPSILON) * gain[...].astype(F32)[None]
        return v * cosb[...] + pltpu.roll(v, lanes // 2, 1) * sinb[...]

    def rope_rows(i):
        where = jnp.broadcast_to(positions[pl.ds(i, 1), :].astype(F32), (lanes, seq)).T * freq[...]
        sine = jnp.sin(where)
        cosb[...] = jnp.cos(where)
        sinb[...] = jnp.where(lax.broadcasted_iota(jnp.int32, (seq, lanes), 1) < lanes // 2, -sine, sine)

    def keep_kv(y, length):
        k_rot = turned(y[:, :lanes], k_gain)
        v_val = y[:, lanes:]
        kk[...] = k_rot.astype(BF)
        vt[...] = v_val.T.astype(BF)
        valid = lax.broadcasted_iota(jnp.int32, (seq, lanes), 0) < length
        seen[...] = jnp.where(valid, 1.0, 0.0)
        kco[...] = jnp.where(valid, k_rot, 0.0).astype(BF)
        vco[...] = jnp.where(valid, v_val, 0.0).astype(BF)

    def keep_q(t, y):
        for s in range(TILE // lanes):
            act[:, t * TILE + s * lanes:t * TILE + (s + 1) * lanes] = turned(y[:, s * lanes:(s + 1) * lanes], q_gain).astype(BF)

    def attend(hd):
        for lo in range(0, seq, span_q):
            hi = lo + span_q
            q = act[lo:hi, hd * lanes:(hd + 1) * lanes]
            s = dot_nt(kk[:hi, :], q)
            parts = [jnp.where((seen[lo:hi, :span_q] > 0.0) & (tri[...] > 0.0), s[lo:hi, :], hidden_score)]
            for r in range(0, lo, span_q):
                parts.append(jnp.where(seen[r:r + span_q, :span_q] > 0.0, s[r:r + span_q, :], hidden_score))
            top = parts[0].max(0, keepdims=True)
            for x in parts[1:]:
                top = jnp.maximum(top, x.max(0, keepdims=True))
            parts = [jnp.exp2((x - top) * to_exp2) for x in parts]
            total = parts[0].sum(0, keepdims=True)
            for x in parts[1:]:
                total = total + x.sum(0, keepdims=True)
            scale = 1.0 / total
            probs = [(x * scale).astype(BF) for x in parts[1:] + parts[:1]]
            probs = jnp.concatenate(probs, axis=0) if len(probs) > 1 else probs[0]
            act[lo:hi, width_q + hd * lanes:width_q + (hd + 1) * lanes] = dot(vt[:, :hi], probs).T.astype(BF)

    step_a = per_ar // (prompts - 1)
    w_q, w_h, w_o = 4, 7, 2
    weight_a = w_q * (q_tiles + 1) + w_h * (heads // HEADS_AT_ONCE) + w_o * n_tiles

    with jax.named_scope('norm_x'):
        norm_all(0)

    def attention_phase(i, _):
        def upto(w):
            return jnp.where(i == 0, 0, UNITS + (i - 1) * step_a + w * step_a // weight_a)
        length = lens[i]
        for t in range(q_tiles + 1):
            if t + GU_BUFS - 1 <= q_tiles:
                start_all(a_tile(t + GU_BUFS - 1))
            with jax.named_scope('qkv'):
                wait_all(a_tile(t))
                if t == 0:
                    rope_rows(i)
                elif t == 1:
                    keep_kv(ybuf[0], length)
                else:
                    keep_q(t - 2, ybuf[(t - 1) % 2])
                ybuf[t % 2] = dot(n2[...], gu[t % GU_BUFS])
            if t % 2 == 1:
                run_slots(upto((t - 1) * w_q), upto((t + 1) * w_q))

        @pl.when(i + 1 < prompts)
        def _():
            start_all(load_rows(tokens, i + 1))
            for t in range(GU_BUFS - 1):
                start_all(a_tile(t))

        @pl.when(i + 1 == prompts)
        def _():
            for t in range(GU_BUFS - 1):
                start_all(f_tile(t))
        rows = pl.ds(pl.multiple_of(i * seq, seq), seq)
        caches = (local(kco, kc.at[rows, :], s_kv.at[0]), local(vco, vc.at[rows, :], s_kv.at[1]))
        start_all(caches)
        with jax.named_scope('keep_q'):
            keep_q(q_tiles - 1, ybuf[q_tiles % 2])
        done = (q_tiles + 1) // 2 * 2 * w_q
        base = (q_tiles + 1) * w_q
        run_slots(upto(done), upto(base))
        for h0 in range(0, heads, HEADS_AT_ONCE):
            with jax.named_scope('attend'):
                for hd in range(h0, h0 + HEADS_AT_ONCE):
                    attend(hd)
            run_slots(upto(base), upto(base + w_h))
            base += w_h
        wait_all(caches)

        def bounds(n):
            return (jnp.where(i == 0, n // 2, upto(base + n * w_o)),
                    jnp.where(i == 0, (n + 1) // 2, upto(base + (n + 1) * w_o)))

        def loaded():
            @pl.when(i + 1 < prompts)
            def _():
                wait_all(load_rows(tokens, i + 1))
        with jax.named_scope('project_o'):
            project(act.at[:, pl.ds(width_q, width_q)], o_tile, o_place, o_bufs - 1, i, 0, bounds, lambda: None, loaded)

        @pl.when(i + 1 < prompts)
        def _():
            for n in range(o_bufs - 1):
                o_tile(n).start()

        @pl.when(i + 1 == prompts)
        def _():
            d_tile(0).start()
        return 0
    lax.fori_loop(0, prompts, attention_phase, 0)

    a_end = UNITS + (prompts - 1) * step_a
    with jax.named_scope('pre_mlp'):
        run_slots(a_end, per_ar + lead)
    start_all(load_rows(ho, 0))
    with jax.named_scope('norm_h'):
        norm_all(1)
    starts = [(m + 1) * per_ar + v for m, v in zip(range(prompts), (lead, 17, 26))]
    mids = [(m + 2) * per_ar + v for m, v in zip(range(prompts), (2, 12, 22))]
    ones = [max((m + 2) * per_ar + lead, mids[m] + 2) for m in range(prompts)]
    ends = starts[1:] + [last * per_ar + UNITS]

    def mlp_phase(i, _):
        k0, k1, kt, k2 = pick(i, starts), pick(i, mids), pick(i, ones), pick(i, ends)

        def f_body(t, _):
            @pl.when(t + GU_BUFS - 1 < f_tiles)
            def _():
                start_all(f_tile(t + GU_BUFS - 1))
            with jax.named_scope('w_gu'):
                wait_all(f_tile(t))
            y = dot(n2[...], gu[lax.rem(t, GU_BUFS)])
            gate, up = y[:, :lanes], y[:, lanes:]
            act[:, pl.ds(pl.multiple_of(t * lanes, lanes), lanes)] = (gate * jax.nn.sigmoid(gate) * up).astype(BF)
            run_slots(k0 + t * (k1 - k0) // f_tiles, k0 + (t + 1) * (k1 - k0) // f_tiles)
            return 0
        with jax.named_scope('f_loop'):
            lax.fori_loop(0, f_tiles, f_body, 0)

        @pl.when(i + 1 < prompts)
        def _():
            for t in range(GU_BUFS - 1):
                start_all(f_tile(t))

        def upto(n):
            return jnp.where(n <= 1, k1 + n * (kt - k1), kt + jnp.maximum(n - 1, 0) * (k2 - kt) // (n_tiles - 1))

        def begin():
            @pl.when(i + 1 < prompts)
            def _():
                start_all(load_rows(ho, i + 1))

        def loaded():
            @pl.when(i + 1 < prompts)
            def _():
                wait_all(load_rows(ho, i + 1))
        with jax.named_scope('project_d'):
            project(act, d_tile, d_place, 1, prompts + i, 1, lambda n: (upto(n), upto(n + 1)), begin, loaded)

        @pl.when(i + 1 < prompts)
        def _():
            d_tile(0).start()
        return 0
    lax.fori_loop(0, prompts, mlp_phase, 0)

    with jax.named_scope('tail'):
        run_slots(last * per_ar + UNITS, (last + 1) * per_ar)

        def ring_end(g, _):
            pass_on(3, last, g)
            return 0
        lax.fori_loop(0, UNITS, ring_end, 0)

        def all_end(g, _):
            settle(last, g)
            return 0
        lax.fori_loop(0, UNITS, all_end, 0)
        for s in range(2):
            await_copy(pp.at[2 * UNITS + s], s_stage.at[s])


def layer_body(tokens, positions, lengths, norm_attn, norm_mlp, q_gain, k_gain, w_query, w_key, w_value, w_out, w_gate, w_up, w_down, tp_size):
    prompts, seq, hidden = tokens.shape
    head_dim = q_gain.shape[0]
    width_q, width_f = w_query.shape[1], w_gate.shape[1]
    kv_heads = w_key.shape[1] // head_dim
    chips = tp_size // CORES
    unit = hidden // CORES // UNITS
    rows_n = prompts * seq
    inv_freq = ROPE_THETA ** (-jnp.arange(head_dim // 2, dtype=F32) / (head_dim // 2))
    freq = jnp.concatenate([inv_freq, inv_freq])[None]
    any_spec = pl.BlockSpec(memory_space=pl.ANY)
    vmem = pl.BlockSpec(memory_space=pltpu.VMEM)
    smem = pl.BlockSpec(memory_space=pltpu.SMEM)
    kernel = functools.partial(layer_kernel, tp_size, prompts, seq, head_dim, kv_heads, (hidden, width_q, width_f))
    dma = pltpu.SemaphoreType.DMA
    o_bufs = 2 * (width_f // width_q)
    span_q = min(head_dim, seq)
    ho, kc, vc = pl.pallas_call(
        kernel,
        name='decoder_layer',
        out_shape=(jax.ShapeDtypeStruct((2 * rows_n, hidden), BF),
                   jax.ShapeDtypeStruct((rows_n, head_dim), BF),
                   jax.ShapeDtypeStruct((rows_n, head_dim), BF)),
        in_specs=[any_spec, vmem, smem, vmem, vmem, vmem, vmem, vmem] + [any_spec] * 7,
        out_specs=(any_spec, any_spec, any_spec),
        scratch_shapes=[
            pltpu.VMEM((seq, hidden), BF),
            pltpu.VMEM((seq, width_f), BF),
            pltpu.VMEM((seq, head_dim), BF), pltpu.VMEM((head_dim, seq), BF),
            pltpu.VMEM((seq, head_dim), BF), pltpu.VMEM((seq, head_dim), BF),
            pltpu.VMEM((seq, head_dim), F32), pltpu.VMEM((seq, head_dim), F32),
            pltpu.VMEM((2, seq, TILE), F32),
            pltpu.VMEM((seq, head_dim), F32),
            pltpu.VMEM((span_q, span_q), F32),
            pltpu.VMEM((2, 16, hidden), F32),
            pltpu.VMEM((GU_BUFS, hidden, TILE), BF),
            pltpu.VMEM((2, width_f, unit), BF),
            pltpu.VMEM((2 * UNITS + 2, seq, unit), BF),
            pltpu.VMEM((2 * UNITS, seq, unit), BF),
            pltpu.VMEM((2, UNITS, 3, seq // chips, unit), BF),
            pltpu.VMEM((prompts * UNITS, seq // chips, unit), BF),
            dma((X_PARTS,)), dma((GU_BUFS, 2)), dma((o_bufs,)), dma((2,)), dma((2 * UNITS,)), dma((prompts * UNITS,)), dma((2,)), dma((2, UNITS)),
            dma((2, UNITS, 3)), dma((2, UNITS, 3)), dma((2, UNITS, 3)), dma((2, UNITS, 3)), dma((2, UNITS, 4)), dma((2, UNITS, 4)),
        ],
        compiler_params=pltpu.CompilerParams(collective_id=0, has_side_effects=True, vmem_limit_bytes=67043328),
    )(tokens.reshape(rows_n, hidden), positions, lengths, norm_attn, norm_mlp, q_gain, k_gain, freq,
      w_query, w_key, w_value, w_out, w_gate, w_up, w_down)
    shape = (prompts, seq, 1, head_dim)
    return ho[rows_n:].reshape(prompts, seq, hidden), kc.reshape(shape), vc.reshape(shape)


def solution(mesh):
    body = functools.partial(layer_body, tp_size=mesh.shape['tp'])
    in_specs = (P('dp', None, None), P('dp', None), P('dp'), P(), P(), P(), P(), P(None, 'tp'), P(), P(), P('tp', None), P(None, 'tp'), P(None, 'tp'), P('tp', None))
    out_specs = (P('dp', None, None), P('dp', None, 'tp', None), P('dp', None, 'tp', None))
    return jax.shard_map(body, mesh=mesh, in_specs=in_specs, out_specs=out_specs, check_vma=False)
```

```python
import functools
import jax
import jax.numpy as jnp
import numpy as np
from jax import lax
from jax.experimental import pallas as pl
from jax.experimental.pallas import tpu as pltpu
from jax.sharding import PartitionSpec as P

EPSILON = 1e-6
ROPE_THETA = 1000000.0
MESH = pl.DeviceIdType.MESH
CORES = 2
TILE = 256
UNITS = 5
HOPS = 6
GU_BUFS = 3
X_PARTS = 4
HEADS_AT_ONCE = 4
BF = jnp.bfloat16
F32 = jnp.float32


def dot(a, b):
    return jnp.dot(a, b, preferred_element_type=F32)


def dot_nt(a, b):
    return lax.dot_general(a, b, (((1,), (1,)), ((), ())), preferred_element_type=F32)


def pick(i, values):
    out = values[0]
    for n, v in enumerate(values[1:], 1):
        out = jnp.where(i >= n, v, out)
    return out


def layer_kernel(tp, prompts, seq, head_dim, kv_heads, dims,
                 tokens, positions, lens, n_attn, n_mlp, q_gain, k_gain, freq, wq, wk, wv, wo, wg, wu, wdn,
                 ho, kc, vc,
                 n2, act, qs, os, kk, vt, kco, vco, cosb, sinb, ybuf, seen, tri, gains, gu, wd, pp, xp, land, ownh,
                 s_x, s_gu, s_wd, s_stage, s_xp, s_res, s_kv, s_own,
                 rs_send, rs_recv, ag_send, ag_recv, dd_send, dd_recv):
    hidden, width_q, width_f = dims
    chips = tp // CORES
    half = hidden // CORES
    unit = half // UNITS
    rows_b = seq // chips
    heads = width_q // head_dim
    q_tiles = width_q // TILE
    f_tiles = width_f // head_dim
    n_tiles = CORES * UNITS
    per_ar = HOPS * UNITS
    lead = UNITS + 1
    last = 2 * prompts - 1
    lanes = head_dim
    add_rows = rows_b // 4 if rows_b % 64 == 0 else 16
    o_bufs = 2 * (width_f // width_q)
    row_groups = min(4, seq // X_PARTS // 16)
    norm_tiles = n_tiles - 2
    norm_rows = seq // norm_tiles
    span_q = min(lanes, seq)
    hidden_score = -1e30 * head_dim ** 0.5
    to_exp2 = head_dim ** -0.5 * 1.4426950408889634

    me = lax.axis_index('tp')
    core = lax.rem(me, CORES)
    chip = me // CORES
    ring = lax.rem(chip + core * (chips - 2 * chip), chips)
    nxt = CORES * lax.rem(chip + chips + 1 - 2 * core, chips) + core
    prv = CORES * lax.rem(chip + chips - 1 + 2 * core, chips) + core
    partner = me + 1 - 2 * core
    kv_col = pl.multiple_of((me // (tp // kv_heads)) * head_dim, head_dim)

    def remote(src, dst, send, recv, to):
        return pltpu.make_async_remote_copy(src_ref=src, dst_ref=dst, send_sem=send, recv_sem=recv,
                                            device_id={'tp': to}, device_id_type=MESH)

    def local(src, dst, sem):
        return pltpu.make_async_copy(src, dst, sem)

    def await_copy(ref, sem):
        local(ref, ref, sem).wait()

    def block_rows(b):
        return pl.ds(pl.multiple_of(b * rows_b, rows_b), rows_b)

    def a_tile(t):
        b = t % GU_BUFS
        if t == 0:
            return (local(wk.at[:, pl.ds(kv_col, lanes)], gu.at[b, :, pl.ds(0, lanes)], s_gu.at[b, 0]),
                    local(wv.at[:, pl.ds(kv_col, lanes)], gu.at[b, :, pl.ds(lanes, lanes)], s_gu.at[b, 1]))
        return (q_tile(t),)

    def q_tile(t):
        b = lax.rem(t, GU_BUFS)
        return local(wq.at[:, pl.ds(pl.multiple_of((t - 1) * TILE, TILE), TILE)], gu.at[b], s_gu.at[b, 0])

    def f_tile(t):
        b = lax.rem(t, GU_BUFS)
        cols = pl.ds(pl.multiple_of(t * lanes, lanes), lanes)
        return (local(wg.at[:, cols], gu.at[b, :, pl.ds(0, lanes)], s_gu.at[b, 0]),
                local(wu.at[:, cols], gu.at[b, :, pl.ds(lanes, lanes)], s_gu.at[b, 1]))

    def start_all(copies):
        for cp in copies:
            cp.start()

    def wait_all(copies):
        for cp in copies:
            cp.wait()

    def out_cols(n):
        side = jnp.where(lax.rem(n, 2) == 0, 1 - core, core)
        return pl.ds(pl.multiple_of(side * half + (n // 2) * unit, unit), unit)

    def o_place(n):
        b = lax.rem(n, o_bufs)
        return wd.at[b // (o_bufs // 2), pl.ds(pl.multiple_of(lax.rem(b, o_bufs // 2) * width_q, width_q), width_q), :]

    def o_tile(n):
        return local(wo.at[:, out_cols(n)], o_place(n), s_wd.at[lax.rem(n, o_bufs)])

    def d_place(n):
        return wd.at[lax.rem(n, 2)]

    def d_tile(n):
        return local(wdn.at[:, out_cols(n)], d_place(n), s_wd.at[lax.rem(n, 2)])

    def load_rows(src, i):
        part = seq // X_PARTS
        return [local(src.at[pl.ds(pl.multiple_of(i * seq + b * part, part), part), :], n2.at[pl.ds(b * part, part), :], s_x.at[b])
                for b in range(X_PARTS)]

    start_all(load_rows(tokens, 0))
    for t in range(GU_BUFS - 1):
        start_all(a_tile(t))
    for n in range(o_bufs - 1):
        o_tile(n).start()
    for i in range(prompts):
        for g in range(UNITS):
            rows = pl.ds(pl.multiple_of(i * seq + ring * rows_b, rows_b), rows_b)
            cols = pl.ds(pl.multiple_of(core * half + g * unit, unit), unit)
            local(tokens.at[rows, cols], ownh.at[i * UNITS + g], s_res.at[i * UNITS + g]).start()
    barrier = pltpu.get_barrier_semaphore()
    for other in (nxt, prv, partner):
        pl.semaphore_signal(barrier, inc=1, device_id={'tp': other}, device_id_type=MESH)

    for v, gain in enumerate((n_attn, n_mlp)):
        wide = gain[...].astype(F32)
        for j in range(hidden // lanes):
            gains[v, :, j * lanes:(j + 1) * lanes] = jnp.broadcast_to(wide[None, j * lanes:(j + 1) * lanes], (16, lanes))
    key_at = lax.broadcasted_iota(jnp.int32, (span_q, span_q), 0)
    tri[...] = jnp.where(key_at <= lax.broadcasted_iota(jnp.int32, (span_q, span_q), 1), 1.0, 0.0)
    pl.semaphore_wait(barrier, 3)

    def ho_block(c, g, b, side):
        rows = pl.ds(pl.multiple_of(c * seq + b * rows_b, rows_b), rows_b)
        return ho.at[rows, pl.ds(pl.multiple_of(side * half + g * unit, unit), unit)]

    def send_partial(e, c, g):
        par = lax.rem(c, 2)
        u = par * UNITS + g
        rows = block_rows(lax.rem(ring + 2 * chips - 1 - e, chips))
        with jax.named_scope('w_rs'):
            if e == 0:
                await_copy(xp.at[u], s_xp.at[u])
            else:
                await_copy(land.at[par, g, e - 1], rs_recv.at[par, g, e - 1])
        mine, theirs, came = pp.at[u, rows], xp.at[u, rows], land.at[par, g, max(e - 1, 0)]

        def add(r, _):
            rr = pl.ds(pl.multiple_of(r * add_rows, 16), add_rows)
            total = mine[rr, :].astype(F32) + theirs[rr, :].astype(F32)
            if e > 0:
                total = total + came[rr, :].astype(F32)
            mine[rr, :] = total.astype(BF)
            return 0
        lax.fori_loop(0, rows_b // add_rows, add, 0)
        remote(mine, land.at[par, g, e], rs_send.at[par, g, e], rs_recv.at[par, g, e], nxt).start()

    def finish_sum(c, g):
        par = lax.rem(c, 2)
        u, w = par * UNITS + g, lax.rem(c, prompts) * UNITS + g
        rows = block_rows(ring)
        with jax.named_scope('w_rs3'):
            await_copy(land.at[par, g, 2], rs_recv.at[par, g, 2])

        @pl.when(c < prompts)
        def _():
            await_copy(ownh.at[w], s_res.at[w])
        mine, theirs, came, own = pp.at[u, rows], xp.at[u, rows], land.at[par, g, 2], ownh.at[w]

        def add(r, _):
            rr = pl.ds(pl.multiple_of(r * add_rows, 16), add_rows)
            total = came[rr, :].astype(F32) + (mine[rr, :].astype(F32) + theirs[rr, :].astype(F32))
            own[rr, :] = (own[rr, :].astype(F32) + total).astype(BF)
            return 0
        lax.fori_loop(0, rows_b // add_rows, add, 0)
        place = ho_block(c, g, ring, core)
        remote(own, place, ag_send.at[par, g, 0], ag_recv.at[par, g, 0], nxt).start()
        remote(own, place, dd_send.at[par, g, 0], dd_recv.at[par, g, 0], partner).start()
        local(own, place, s_own.at[par, g]).start()

    def pass_on(e, c, g):
        par = lax.rem(c, 2)
        place = ho_block(c, g, lax.rem(ring + 2 * chips - e, chips), core)
        with jax.named_scope('w_ag'):
            await_copy(place, ag_recv.at[par, g, e - 1])
        if e < 3:
            remote(place, place, ag_send.at[par, g, e], ag_recv.at[par, g, e], nxt).start()
        remote(place, place, dd_send.at[par, g, e], dd_recv.at[par, g, e], partner).start()
        if e == 1:
            await_copy(place, dd_recv.at[par, g, 0])
            for s in range(3):
                await_copy(land.at[par, g, s], rs_send.at[par, g, s])

    def settle(c, g):
        par = lax.rem(c, 2)
        place = ho_block(c, g, ring, core)
        await_copy(land.at[par, g, 0], s_own.at[par, g])
        for e in range(3):
            await_copy(place, ag_send.at[par, g, e])
        for e in range(4):
            await_copy(place, dd_send.at[par, g, e])
        for e in range(1, 4):
            await_copy(place, dd_recv.at[par, g, e])

    def slot(k):
        c = jnp.minimum(k // per_ar, last)
        j = k - c * per_ar
        diagonal = c == last
        e_d = lax.rem(HOPS - lax.rem(j, HOPS), HOPS)
        at = j - (HOPS - 1) * e_d
        g_d = jnp.maximum(at, 0) // HOPS
        live = jnp.logical_not(diagonal) | ((at >= 0) & (g_d < UNITS))
        e = jnp.where(live, jnp.where(diagonal, e_d, j // UNITS), HOPS)
        g = jnp.where(diagonal, jnp.minimum(g_d, UNITS - 1), lax.rem(j, UNITS))
        for s in range(3):
            @pl.when(e == s)
            def _(s=s):
                send_partial(s, c, g)

        @pl.when(e == 3)
        def _():
            finish_sum(c, g)
        for s in range(2):
            @pl.when(e == 4 + s)
            def _(s=s):
                pass_on(s + 1, c, g)

        @pl.when((e == 0) & (c > 0))
        def _():
            pass_on(3, c - 1, g)

        @pl.when((c > 0) & (j >= 1) & (j <= UNITS) & jnp.logical_not(diagonal))
        def _():
            settle(c - 1, j - 1)

        @pl.when(diagonal & (e == 1))
        def _():
            settle(c - 1, g)

    def run_slots(lo, hi):
        def body(k, _):
            slot(k)
            return 0
        lax.fori_loop(lo, hi, body, 0)

    def norm_all(v):
        part = seq // X_PARTS
        for b in range(X_PARTS):
            await_copy(n2.at[pl.ds(b * part, part), :], s_x.at[b])

            def scales(r, _):
                for q in range(row_groups):
                    rr = pl.ds(pl.multiple_of(b * part + (r * row_groups + q) * 16, 16), 16)
                    acc = jnp.zeros((16, lanes), F32)
                    for j in range(hidden // lanes):
                        x = n2[rr, j * lanes:(j + 1) * lanes].astype(F32)
                        acc = acc + x * x
                    scale = lax.rsqrt(jnp.sum(acc, axis=-1, keepdims=True) * (1.0 / hidden) + EPSILON)
                    ybuf[0, rr, :lanes] = jnp.broadcast_to(scale, (16, lanes))
                return 0
            lax.fori_loop(0, part // 16 // row_groups, scales, 0)

        def apply(r, _):
            rr = pl.ds(pl.multiple_of(r * 16, 16), 16)
            scale = ybuf[0, rr, :lanes]
            for j in range(hidden // lanes):
                cols = slice(j * lanes, (j + 1) * lanes)
                n2[rr, cols] = (n2[rr, cols].astype(F32) * scale * gains[v, :, cols]).astype(BF)
            return 0
        lax.fori_loop(0, seq // 16, apply, 0)

    def norm_some(v, first):
        for q in range(norm_rows // 16):
            rr = pl.ds(pl.multiple_of(first + q * 16, 16), 16)
            acc = jnp.zeros((16, lanes), F32)
            for j in range(hidden // lanes):
                x = n2[rr, j * lanes:(j + 1) * lanes].astype(F32)
                acc = acc + x * x
            scale = jnp.broadcast_to(lax.rsqrt(jnp.sum(acc, axis=-1, keepdims=True) * (1.0 / hidden) + EPSILON), (16, lanes))
            for j in range(hidden // lanes):
                cols = slice(j * lanes, (j + 1) * lanes)
                n2[rr, cols] = (n2[rr, cols].astype(F32) * scale * gains[v, :, cols]).astype(BF)

    def project(lhs, fetch, place, ahead, c, v, bounds, begin, loaded):
        par = lax.rem(c, 2)

        def tile(n, norm):
            @pl.when(n + ahead < n_tiles)
            def _():
                fetch(n + ahead).start()
            with jax.named_scope('w_wd'):
                fetch(n).wait()
            g = n // 2
            away = lax.rem(n, 2) == 0
            count = c * UNITS + g
            stage = lax.rem(count, 2)
            u = jnp.where(away, 2 * UNITS + stage, par * UNITS + g)

            @pl.when(away & (count >= 2))
            def _():
                await_copy(pp.at[u], s_stage.at[stage])
            if norm:
                norm_some(v, pl.multiple_of((n - 2) * norm_rows, 16))
            pp[u] = dot(lhs[...], place(n)[...]).astype(BF)

            @pl.when(away)
            def _():
                to = par * UNITS + g
                remote(pp.at[u], xp.at[to], s_stage.at[stage], s_xp.at[to], partner).start()
            run_slots(*bounds(n))

        def plain(n, _):
            tile(n, False)
            return 0

        def normed(n, _):
            tile(n, True)
            return 0
        lax.fori_loop(0, 1, plain, 0)
        begin()
        lax.fori_loop(1, 2, plain, 0)
        loaded()
        lax.fori_loop(2, n_tiles, normed, 0)

    def turned(v, gain):
        v = v * lax.rsqrt(jnp.mean(v * v, axis=-1, keepdims=True) + EPSILON) * gain[...].astype(F32)[None]
        return v * cosb[...] + pltpu.roll(v, lanes // 2, 1) * sinb[...]

    def rope_rows(i):
        where = jnp.broadcast_to(positions[pl.ds(i, 1), :].astype(F32), (lanes, seq)).T * freq[...]
        sine = jnp.sin(where)
        cosb[...] = jnp.cos(where)
        sinb[...] = jnp.where(lax.broadcasted_iota(jnp.int32, (seq, lanes), 1) < lanes // 2, -sine, sine)

    def keep_kv(y, length):
        k_rot = turned(y[:, :lanes], k_gain)
        v_val = y[:, lanes:]
        kk[...] = k_rot.astype(BF)
        vt[...] = v_val.T.astype(BF)
        valid = lax.broadcasted_iota(jnp.int32, (seq, lanes), 0) < length
        seen[...] = jnp.where(valid, 1.0, 0.0)
        kco[...] = jnp.where(valid, k_rot, 0.0).astype(BF)
        vco[...] = jnp.where(valid, v_val, 0.0).astype(BF)

    def keep_q(t, y):
        for s in range(TILE // lanes):
            qs[:, pl.ds(pl.multiple_of(t * TILE + s * lanes, lanes), lanes)] = turned(y[:, s * lanes:(s + 1) * lanes], q_gain).astype(BF)

    def attend(hd):
        cols = pl.ds(pl.multiple_of(hd * lanes, lanes), lanes)
        for lo in range(0, seq, span_q):
            hi = lo + span_q
            q = qs[lo:hi, cols]
            s = dot_nt(kk[:hi, :], q)
            parts = [jnp.where((seen[lo:hi, :span_q] > 0.0) & (tri[...] > 0.0), s[lo:hi, :], hidden_score)]
            for r in range(0, lo, span_q):
                parts.append(jnp.where(seen[r:r + span_q, :span_q] > 0.0, s[r:r + span_q, :], hidden_score))
            top = parts[0].max(0, keepdims=True)
            for x in parts[1:]:
                top = jnp.maximum(top, x.max(0, keepdims=True))
            parts = [jnp.exp2((x - top) * to_exp2) for x in parts]
            total = parts[0].sum(0, keepdims=True)
            for x in parts[1:]:
                total = total + x.sum(0, keepdims=True)
            scale = 1.0 / total
            probs = [(x * scale).astype(BF) for x in parts[1:] + parts[:1]]
            probs = jnp.concatenate(probs, axis=0) if len(probs) > 1 else probs[0]
            os[lo:hi, cols] = dot(vt[:, :hi], probs).T.astype(BF)

    step_a = (per_ar + lead - UNITS) // (prompts - 1)
    w_q, w_h, w_o = 4, 7, 2
    weight_a = w_q * (q_tiles + 1) + w_h * (heads // HEADS_AT_ONCE) + w_o * n_tiles

    with jax.named_scope('norm_x'):
        norm_all(0)

    def attention_phase(i, _):
        def upto(w):
            return jnp.where(i == 0, 0, UNITS + (i - 1) * step_a + w * step_a // weight_a)
        length = lens[i]
        def kv_body(t, _):
            start_all(a_tile(2))
            with jax.named_scope('qkv'):
                wait_all(a_tile(0))
                rope_rows(i)
                ybuf[0] = dot(n2[...], gu[0])
            return 0
        lax.fori_loop(i, i + 1, kv_body, 0)

        def q0_body(t, _):
            start_all(a_tile(3))
            with jax.named_scope('qkv'):
                wait_all(a_tile(1))
                keep_kv(ybuf[0], length)
                ybuf[1] = dot(n2[...], gu[1])
            return 0
        lax.fori_loop(i, i + 1, q0_body, 0)
        run_slots(upto(0), upto(2 * w_q))

        def q_body(t, _):
            @pl.when(t + GU_BUFS - 1 <= q_tiles)
            def _():
                q_tile(t + GU_BUFS - 1).start()
            with jax.named_scope('qkv'):
                q_tile(t).wait()
                keep_q(t - 2, ybuf[lax.rem(t - 1, 2)])
                ybuf[lax.rem(t, 2)] = dot(n2[...], gu[lax.rem(t, GU_BUFS)])
            run_slots(upto(t * w_q), upto((t + 1) * w_q))
            return 0
        lax.fori_loop(2, q_tiles + 1, q_body, 0)

        @pl.when(i + 1 < prompts)
        def _():
            start_all(load_rows(tokens, i + 1))
            for t in range(GU_BUFS - 1):
                start_all(a_tile(t))

        @pl.when(i + 1 == prompts)
        def _():
            for t in range(GU_BUFS - 1):
                start_all(f_tile(t))
        rows = pl.ds(pl.multiple_of(i * seq, seq), seq)
        caches = (local(kco, kc.at[rows, :], s_kv.at[0]), local(vco, vc.at[rows, :], s_kv.at[1]))
        start_all(caches)
        with jax.named_scope('keep_q'):
            keep_q(q_tiles - 1, ybuf[q_tiles % 2])
        base1 = (q_tiles + 1) * w_q

        def heads_body(t, _):
            with jax.named_scope('attend'):
                for hd in range(HEADS_AT_ONCE):
                    attend(t * HEADS_AT_ONCE + hd)
            run_slots(upto(base1 + t * w_h), upto(base1 + (t + 1) * w_h))
            return 0
        lax.fori_loop(0, heads // HEADS_AT_ONCE, heads_body, 0)
        base = base1 + heads // HEADS_AT_ONCE * w_h
        wait_all(caches)

        def bounds(n):
            return (jnp.where(i == 0, n // 2, upto(base + n * w_o)),
                    jnp.where(i == 0, (n + 1) // 2, upto(base + (n + 1) * w_o)))

        def loaded():
            @pl.when(i + 1 < prompts)
            def _():
                wait_all(load_rows(tokens, i + 1))
        with jax.named_scope('project_o'):
            project(os, o_tile, o_place, o_bufs - 1, i, 0, bounds, lambda: None, loaded)

        @pl.when(i + 1 < prompts)
        def _():
            for n in range(o_bufs - 1):
                o_tile(n).start()

        @pl.when(i + 1 == prompts)
        def _():
            d_tile(0).start()
        return 0
    lax.fori_loop(0, prompts, attention_phase, 0)

    a_end = UNITS + (prompts - 1) * step_a
    with jax.named_scope('pre_mlp'):
        run_slots(a_end, per_ar + lead)
    start_all(load_rows(ho, 0))
    with jax.named_scope('norm_h'):
        norm_all(1)
    starts = [(m + 1) * per_ar + v for m, v in zip(range(prompts), (lead, 18, 32))]
    mids = [(m + 2) * per_ar + v for m, v in zip(range(prompts), (3, 15, 30))]
    ones = [max((m + 2) * per_ar + lead, mids[m] + 2) if m + 1 < prompts else mids[m] for m in range(prompts)]
    ends = starts[1:] + [last * per_ar + UNITS * UNITS]

    def mlp_phase(i, _):
        k0, k1, kt, k2 = pick(i, starts), pick(i, mids), pick(i, ones), pick(i, ends)

        def f_body(t, _):
            @pl.when(t + GU_BUFS - 1 < f_tiles)
            def _():
                start_all(f_tile(t + GU_BUFS - 1))
            with jax.named_scope('w_gu'):
                wait_all(f_tile(t))
            y = dot(n2[...], gu[lax.rem(t, GU_BUFS)])
            gate, up = y[:, :lanes], y[:, lanes:]
            act[:, pl.ds(pl.multiple_of(t * lanes, lanes), lanes)] = (gate * jax.nn.sigmoid(gate) * up).astype(BF)
            run_slots(k0 + t * (k1 - k0) // f_tiles, k0 + (t + 1) * (k1 - k0) // f_tiles)
            return 0
        with jax.named_scope('f_loop'):
            lax.fori_loop(0, f_tiles, f_body, 0)

        @pl.when(i + 1 < prompts)
        def _():
            for t in range(GU_BUFS - 1):
                start_all(f_tile(t))

        def upto(n):
            spread = jnp.where(n <= 1, k1 + n * (kt - k1), kt + jnp.maximum(n - 1, 0) * (k2 - kt) // (n_tiles - 1))
            return jnp.where(i == prompts - 1, k1 + n // 2 * UNITS, spread)

        def begin():
            @pl.when(i + 1 < prompts)
            def _():
                start_all(load_rows(ho, i + 1))

        def loaded():
            @pl.when(i + 1 < prompts)
            def _():
                wait_all(load_rows(ho, i + 1))
        with jax.named_scope('project_d'):
            project(act, d_tile, d_place, 1, prompts + i, 1, lambda n: (upto(n), upto(n + 1)), begin, loaded)

        @pl.when(i + 1 < prompts)
        def _():
            d_tile(0).start()
        return 0
    lax.fori_loop(0, prompts, mlp_phase, 0)

    with jax.named_scope('tail'):
        run_slots(last * per_ar + UNITS * UNITS, last * per_ar + (UNITS - 1) * HOPS + (HOPS - 1) * (HOPS - 1) + 1)

        def ring_end(g, _):
            pass_on(3, last, g)
            return 0
        lax.fori_loop(0, UNITS, ring_end, 0)

        def all_end(g, _):
            settle(last, g)
            return 0
        lax.fori_loop(0, UNITS, all_end, 0)
        for s in range(2):
            await_copy(pp.at[2 * UNITS + s], s_stage.at[s])


def copy_kernel(a, b, c, a_out, b_out, c_out):
    a_out[...] = a[...]
    b_out[...] = b[...]
    c_out[...] = c[...]


def layer_body(tokens, positions, lengths, norm_attn, norm_mlp, q_gain, k_gain, w_query, w_key, w_value, w_out, w_gate, w_up, w_down, tp_size):
    prompts, seq, hidden = tokens.shape
    head_dim = q_gain.shape[0]
    width_q, width_f = w_query.shape[1], w_gate.shape[1]
    kv_heads = w_key.shape[1] // head_dim
    chips = tp_size // CORES
    unit = hidden // CORES // UNITS
    rows_n = prompts * seq
    inv_freq = ROPE_THETA ** (-np.arange(head_dim // 2) / (head_dim // 2))
    freq = jnp.asarray(np.concatenate([inv_freq, inv_freq])[None], F32)
    any_spec = pl.BlockSpec(memory_space=pl.ANY)
    vmem = pl.BlockSpec(memory_space=pltpu.VMEM)
    smem = pl.BlockSpec(memory_space=pltpu.SMEM)
    kernel = functools.partial(layer_kernel, tp_size, prompts, seq, head_dim, kv_heads, (hidden, width_q, width_f))
    dma = pltpu.SemaphoreType.DMA
    o_bufs = 2 * (width_f // width_q)
    span_q = min(head_dim, seq)
    ho, kc, vc = pl.pallas_call(
        kernel,
        name='decoder_layer',
        out_shape=(jax.ShapeDtypeStruct((2 * rows_n, hidden), BF),
                   jax.ShapeDtypeStruct((rows_n, head_dim), BF),
                   jax.ShapeDtypeStruct((rows_n, head_dim), BF)),
        in_specs=[any_spec, vmem, smem, vmem, vmem, vmem, vmem, vmem] + [any_spec] * 7,
        out_specs=(any_spec, any_spec, any_spec),
        scratch_shapes=[
            pltpu.VMEM((seq, hidden), BF),
            pltpu.VMEM((seq, width_f), BF),
            pltpu.VMEM((seq, width_q), BF), pltpu.VMEM((seq, width_q), BF),
            pltpu.VMEM((seq, head_dim), BF), pltpu.VMEM((head_dim, seq), BF),
            pltpu.VMEM((seq, head_dim), BF), pltpu.VMEM((seq, head_dim), BF),
            pltpu.VMEM((seq, head_dim), F32), pltpu.VMEM((seq, head_dim), F32),
            pltpu.VMEM((2, seq, TILE), F32),
            pltpu.VMEM((seq, head_dim), F32),
            pltpu.VMEM((span_q, span_q), F32),
            pltpu.VMEM((2, 16, hidden), F32),
            pltpu.VMEM((GU_BUFS, hidden, TILE), BF),
            pltpu.VMEM((2, width_f, unit), BF),
            pltpu.VMEM((2 * UNITS + 2, seq, unit), BF),
            pltpu.VMEM((2 * UNITS, seq, unit), BF),
            pltpu.VMEM((2, UNITS, 3, seq // chips, unit), BF),
            pltpu.VMEM((prompts * UNITS, seq // chips, unit), BF),
            dma((X_PARTS,)), dma((GU_BUFS, 2)), dma((o_bufs,)), dma((2,)), dma((2 * UNITS,)), dma((prompts * UNITS,)), dma((2,)), dma((2, UNITS)),
            dma((2, UNITS, 3)), dma((2, UNITS, 3)), dma((2, UNITS, 3)), dma((2, UNITS, 3)), dma((2, UNITS, 4)), dma((2, UNITS, 4)),
        ],
        compiler_params=pltpu.CompilerParams(collective_id=0, has_side_effects=True, vmem_limit_bytes=67043328),
    )(tokens.reshape(rows_n, hidden), positions, lengths, norm_attn, norm_mlp, q_gain, k_gain, freq,
      w_query, w_key, w_value, w_out, w_gate, w_up, w_down)
    shape = (prompts, seq, 1, head_dim)
    parts = 2 * prompts
    block = rows_n // parts
    out, kc, vc = pl.pallas_call(
        copy_kernel,
        name='copy_out',
        grid=(parts,),
        out_shape=(jax.ShapeDtypeStruct((rows_n, hidden), BF), jax.ShapeDtypeStruct(kc.shape, BF), jax.ShapeDtypeStruct(vc.shape, BF)),
        in_specs=[pl.BlockSpec((block, hidden), lambda b: (b + parts, 0))] + [pl.BlockSpec((block, head_dim), lambda b: (b, 0))] * 2,
        out_specs=[pl.BlockSpec((block, hidden), lambda b: (b, 0))] + [pl.BlockSpec((block, head_dim), lambda b: (b, 0))] * 2,
        compiler_params=pltpu.CompilerParams(vmem_limit_bytes=40 * 1024 * 1024),
    )(ho, kc, vc)
    return out.reshape(prompts, seq, hidden), kc.reshape(shape), vc.reshape(shape)


def solution(mesh):
    body = functools.partial(layer_body, tp_size=mesh.shape['tp'])
    in_specs = (P('dp', None, None), P('dp', None), P('dp'), P(), P(), P(), P(), P(None, 'tp'), P(), P(), P('tp', None), P(None, 'tp'), P(None, 'tp'), P('tp', None))
    out_specs = (P('dp', None, None), P('dp', None, 'tp', None), P('dp', None, 'tp', None))
    return jax.shard_map(body, mesh=mesh, in_specs=in_specs, out_specs=out_specs, check_vma=False)
```

```python
import functools
import jax
import jax.numpy as jnp
import numpy as np
from jax import lax
from jax.experimental import pallas as pl
from jax.experimental.pallas import tpu as pltpu
from jax.sharding import PartitionSpec as P

EPSILON = 1e-6
ROPE_THETA = 1000000.0
MESH = pl.DeviceIdType.MESH
CORES = 2
TILE = 256
UNITS = 5
HOPS = 6
A_BUFS = 4
X_PARTS = 4
HEADS_AT_ONCE = 4
BF = jnp.bfloat16
F32 = jnp.float32


def dot(a, b):
    return jnp.dot(a, b, preferred_element_type=F32)


def dot_nt(a, b):
    return lax.dot_general(a, b, (((1,), (1,)), ((), ())), preferred_element_type=F32)


def over(x, n):
    return lax.shift_right_logical(x * (65536 // n + 1), 16)


def split(x, n):
    q = over(x, n)
    return q, x - q * n


def pick(i, values):
    out = values[0]
    for n, v in enumerate(values[1:], 1):
        out = jnp.where(i >= n, v, out)
    return out


def layer_kernel(tp, prompts, seq, head_dim, kv_heads, dims,
                 tokens, positions, lens, n_attn, n_mlp, q_gain, k_gain, freq, wq, wk, wv, wo, wg, wu, wdn,
                 ho, kc, vc,
                 n2, act, qs, os, kk, vt, kco, vco, cosb, sinb, ybuf, seen, tri, gains, gu, wd, pp, xp, land, ownh,
                 s_x, s_gu, s_wd, s_stage, s_xp, s_res, s_kv, s_own,
                 rs_send, rs_recv, ag_send, ag_recv, dd_send, dd_recv):
    hidden, width_q, width_f = dims
    chips = tp // CORES
    half = hidden // CORES
    unit = half // UNITS
    rows_b = seq // chips
    heads = width_q // head_dim
    q_tiles = width_q // TILE
    f_tiles = width_f // TILE
    odd = width_f % TILE != 0
    n_tiles = CORES * UNITS
    per_ar = HOPS * UNITS
    lead = UNITS + 1
    last = 2 * prompts - 1
    lanes = head_dim
    add_rows = rows_b // 4 if rows_b % 64 == 0 else 16
    o_bufs = 2 * (width_f // width_q)
    row_groups = min(4, seq // X_PARTS // 16)
    norm_tiles = n_tiles - 2
    norm_rows = seq // norm_tiles
    span_q = min(lanes, seq)
    hidden_score = -1e30 * head_dim ** 0.5
    to_exp2 = head_dim ** -0.5 * 1.4426950408889634

    me = lax.axis_index('tp')
    core = lax.rem(me, CORES)
    chip = me // CORES
    ring = lax.rem(chip + core * (chips - 2 * chip), chips)
    nxt = CORES * lax.rem(chip + chips + 1 - 2 * core, chips) + core
    prv = CORES * lax.rem(chip + chips - 1 + 2 * core, chips) + core
    partner = me + 1 - 2 * core
    kv_col = pl.multiple_of((me // (tp // kv_heads)) * head_dim, head_dim)

    def remote(src, dst, send, recv, to):
        return pltpu.make_async_remote_copy(src_ref=src, dst_ref=dst, send_sem=send, recv_sem=recv,
                                            device_id={'tp': to}, device_id_type=MESH)

    def local(src, dst, sem):
        return pltpu.make_async_copy(src, dst, sem)

    def await_copy(ref, sem):
        local(ref, ref, sem).wait()

    def wrap(b):
        return jnp.where(b < 0, b + chips, b)

    def block_rows(b):
        return pl.ds(pl.multiple_of(b * rows_b, rows_b), rows_b)

    def a_place(t):
        b = t % A_BUFS if isinstance(t, int) else lax.bitwise_and(t, A_BUFS - 1)
        return b, gu.at[b // 2, :, pl.ds(pl.multiple_of(lax.rem(b, 2) * TILE, TILE), TILE)]

    def a_tile(t):
        if isinstance(t, int) and t == 0:
            return (local(wk.at[:, pl.ds(kv_col, lanes)], gu.at[0, :, pl.ds(0, lanes)], s_gu.at[0, 0]),
                    local(wv.at[:, pl.ds(kv_col, lanes)], gu.at[0, :, pl.ds(lanes, lanes)], s_gu.at[0, 1]))
        b, place = a_place(t)
        return (local(wq.at[:, pl.ds(pl.multiple_of((t - 1) * TILE, TILE), TILE)], place, s_gu.at[b, 0]),)

    def f_pair(b, col, width):
        cols = pl.ds(pl.multiple_of(col, lanes), width)
        return (local(wg.at[:, cols], gu.at[b, :, pl.ds(0, width)], s_gu.at[b, 0]),
                local(wu.at[:, cols], gu.at[b, :, pl.ds(width, width)], s_gu.at[b, 1]))

    def f_tile(t):
        return f_pair(lax.rem(t, 2), t * TILE, TILE)

    def f_rest():
        return f_pair(f_tiles % 2, f_tiles * TILE, lanes)

    def start_all(copies):
        for cp in copies:
            cp.start()

    def wait_all(copies):
        for cp in copies:
            cp.wait()

    def out_cols(n):
        side = jnp.where(lax.rem(n, 2) == 0, 1 - core, core)
        return pl.ds(pl.multiple_of(side * half + lax.shift_right_logical(n, 1) * unit, unit), unit)

    def o_place(n):
        b = lax.rem(n, o_bufs)
        return wd.at[b // (o_bufs // 2), pl.ds(pl.multiple_of(lax.rem(b, o_bufs // 2) * width_q, width_q), width_q), :]

    def o_tile(n):
        return local(wo.at[:, out_cols(n)], o_place(n), s_wd.at[lax.rem(n, o_bufs)])

    def d_place(n):
        return wd.at[lax.rem(n, 2)]

    def d_tile(n):
        return local(wdn.at[:, out_cols(n)], d_place(n), s_wd.at[lax.rem(n, 2)])

    def load_rows(src, i):
        part = seq // X_PARTS
        return [local(src.at[pl.ds(pl.multiple_of(i * seq + b * part, part), part), :], n2.at[pl.ds(b * part, part), :], s_x.at[b])
                for b in range(X_PARTS)]

    start_all(load_rows(tokens, 0))
    for t in range(A_BUFS - 1):
        start_all(a_tile(t))
    for n in range(o_bufs - 1):
        o_tile(n).start()
    for i in range(prompts):
        for g in range(UNITS):
            rows = pl.ds(pl.multiple_of(i * seq + ring * rows_b, rows_b), rows_b)
            cols = pl.ds(pl.multiple_of(core * half + g * unit, unit), unit)
            local(tokens.at[rows, cols], ownh.at[i * UNITS + g], s_res.at[i * UNITS + g]).start()
    barrier = pltpu.get_barrier_semaphore()
    for other in (nxt, prv, partner):
        pl.semaphore_signal(barrier, inc=1, device_id={'tp': other}, device_id_type=MESH)

    for v, gain in enumerate((n_attn, n_mlp)):
        wide = gain[...].astype(F32)
        for j in range(hidden // lanes):
            gains[v, :, j * lanes:(j + 1) * lanes] = jnp.broadcast_to(wide[None, j * lanes:(j + 1) * lanes], (16, lanes))
    key_at = lax.broadcasted_iota(jnp.int32, (span_q, span_q), 0)
    tri[...] = jnp.where(key_at <= lax.broadcasted_iota(jnp.int32, (span_q, span_q), 1), 1.0, 0.0)
    pl.semaphore_wait(barrier, 3)

    def ho_block(c, g, b, side):
        rows = pl.ds(pl.multiple_of(c * seq + b * rows_b, rows_b), rows_b)
        return ho.at[rows, pl.ds(pl.multiple_of(side * half + g * unit, unit), unit)]

    def send_partial(e, c, g):
        par = lax.bitwise_and(c, 1)
        u = par * UNITS + g
        rows = block_rows(wrap(ring - 1 - e))
        with jax.named_scope('w_rs'):
            if e == 0:
                await_copy(xp.at[u], s_xp.at[u])
            else:
                await_copy(land.at[par, g, e - 1], rs_recv.at[par, g, e - 1])
        mine, theirs, came = pp.at[u, rows], xp.at[u, rows], land.at[par, g, max(e - 1, 0)]

        def add(r, _):
            rr = pl.ds(pl.multiple_of(r * add_rows, 16), add_rows)
            total = mine[rr, :].astype(F32) + theirs[rr, :].astype(F32)
            if e > 0:
                total = total + came[rr, :].astype(F32)
            mine[rr, :] = total.astype(BF)
            return 0
        lax.fori_loop(0, rows_b // add_rows, add, 0)
        remote(mine, land.at[par, g, e], rs_send.at[par, g, e], rs_recv.at[par, g, e], nxt).start()

    def finish_sum(c, g):
        par = lax.bitwise_and(c, 1)
        u, w = par * UNITS + g, jnp.where(c < prompts, c, c - prompts) * UNITS + g
        rows = block_rows(ring)
        with jax.named_scope('w_rs3'):
            await_copy(land.at[par, g, 2], rs_recv.at[par, g, 2])

        @pl.when(c < prompts)
        def _():
            await_copy(ownh.at[w], s_res.at[w])
        mine, theirs, came, own = pp.at[u, rows], xp.at[u, rows], land.at[par, g, 2], ownh.at[w]

        def add(r, _):
            rr = pl.ds(pl.multiple_of(r * add_rows, 16), add_rows)
            total = came[rr, :].astype(F32) + (mine[rr, :].astype(F32) + theirs[rr, :].astype(F32))
            own[rr, :] = (own[rr, :].astype(F32) + total).astype(BF)
            return 0
        lax.fori_loop(0, rows_b // add_rows, add, 0)
        place = ho_block(c, g, ring, core)
        remote(own, place, ag_send.at[par, g, 0], ag_recv.at[par, g, 0], nxt).start()
        remote(own, place, dd_send.at[par, g, 0], dd_recv.at[par, g, 0], partner).start()
        local(own, place, s_own.at[par, g]).start()

    def pass_on(e, c, g):
        par = lax.bitwise_and(c, 1)
        place = ho_block(c, g, wrap(ring - e), core)
        with jax.named_scope('w_ag'):
            await_copy(place, ag_recv.at[par, g, e - 1])
        if e < 3:
            remote(place, place, ag_send.at[par, g, e], ag_recv.at[par, g, e], nxt).start()
        remote(place, place, dd_send.at[par, g, e], dd_recv.at[par, g, e], partner).start()
        if e == 1:
            await_copy(place, dd_recv.at[par, g, 0])
            for s in range(3):
                await_copy(land.at[par, g, s], rs_send.at[par, g, s])

    def settle(c, g):
        par = lax.bitwise_and(c, 1)
        place = ho_block(c, g, ring, core)
        await_copy(land.at[par, g, 0], s_own.at[par, g])
        for e in range(3):
            await_copy(place, ag_send.at[par, g, e])
        for e in range(4):
            await_copy(place, dd_send.at[par, g, e])
        for e in range(1, 4):
            await_copy(place, dd_recv.at[par, g, e])

    def slot(k):
        c = jnp.minimum(over(k, per_ar), last)
        diagonal = c == last
        d, q = split(k - c * per_ar, UNITS)
        g_d = jnp.minimum(d, UNITS - 1) - q
        e_d = jnp.where(g_d >= 0, d - g_d, HOPS)
        e = jnp.where(diagonal, e_d, d)
        g = jnp.where(diagonal, jnp.maximum(g_d, 0), q)
        @pl.when(e < 3)
        def _():
            for s in range(3):
                @pl.when(e == s)
                def _(s=s):
                    send_partial(s, c, g)
                    if s == 0:
                        @pl.when(c > 0)
                        def _():
                            pass_on(3, c - 1, g)

                            @pl.when((g > 0) & jnp.logical_not(diagonal))
                            def _():
                                settle(c - 1, g - 1)
                    if s == 1:
                        @pl.when((c > 0) & (diagonal | (g == 0)))
                        def _():
                            settle(c - 1, jnp.where(diagonal, g, UNITS - 1))

        @pl.when(e >= 3)
        def _():
            @pl.when(e == 3)
            def _():
                finish_sum(c, g)
            for s in range(2):
                @pl.when(e == 4 + s)
                def _(s=s):
                    pass_on(s + 1, c, g)

    def run_slots(lo, hi):
        def body(k, _):
            slot(k)
            return 0
        lax.fori_loop(lo, hi, body, 0)

    def norm_all(v):
        part = seq // X_PARTS
        for b in range(X_PARTS):
            await_copy(n2.at[pl.ds(b * part, part), :], s_x.at[b])

            def scales(r, _):
                for q in range(row_groups):
                    rr = pl.ds(pl.multiple_of(b * part + (r * row_groups + q) * 16, 16), 16)
                    acc = jnp.zeros((16, lanes), F32)
                    for j in range(hidden // lanes):
                        x = n2[rr, j * lanes:(j + 1) * lanes].astype(F32)
                        acc = acc + x * x
                    scale = lax.rsqrt(jnp.sum(acc, axis=-1, keepdims=True) * (1.0 / hidden) + EPSILON)
                    ybuf[0, rr, :lanes] = jnp.broadcast_to(scale, (16, lanes))
                return 0
            lax.fori_loop(0, part // 16 // row_groups, scales, 0)

        def apply(r, _):
            rr = pl.ds(pl.multiple_of(r * 16, 16), 16)
            scale = ybuf[0, rr, :lanes]
            for j in range(hidden // lanes):
                cols = slice(j * lanes, (j + 1) * lanes)
                n2[rr, cols] = (n2[rr, cols].astype(F32) * scale * gains[v, :, cols]).astype(BF)
            return 0
        lax.fori_loop(0, seq // 16, apply, 0)

    def norm_some(v, first):
        for q in range(norm_rows // 16):
            rr = pl.ds(pl.multiple_of(first + q * 16, 16), 16)
            acc = jnp.zeros((16, lanes), F32)
            for j in range(hidden // lanes):
                x = n2[rr, j * lanes:(j + 1) * lanes].astype(F32)
                acc = acc + x * x
            scale = jnp.broadcast_to(lax.rsqrt(jnp.sum(acc, axis=-1, keepdims=True) * (1.0 / hidden) + EPSILON), (16, lanes))
            for j in range(hidden // lanes):
                cols = slice(j * lanes, (j + 1) * lanes)
                n2[rr, cols] = (n2[rr, cols].astype(F32) * scale * gains[v, :, cols]).astype(BF)

    def project(lhs, fetch, place, ahead, c, v, bounds, begin, loaded):
        par = lax.bitwise_and(c, 1)

        def tile(n, norm):
            @pl.when(n + ahead < n_tiles)
            def _():
                fetch(n + ahead).start()
            with jax.named_scope('w_wd'):
                fetch(n).wait()
            g = n // 2
            away = lax.rem(n, 2) == 0
            count = c * UNITS + g
            stage = lax.rem(count, 2)
            u = jnp.where(away, 2 * UNITS + stage, par * UNITS + g)

            @pl.when(away & (count >= 2))
            def _():
                await_copy(pp.at[u], s_stage.at[stage])
            if norm:
                norm_some(v, pl.multiple_of((n - 2) * norm_rows, 16))
            pp[u] = dot(lhs[...], place(n)[...]).astype(BF)

            @pl.when(away)
            def _():
                to = par * UNITS + g
                remote(pp.at[u], xp.at[to], s_stage.at[stage], s_xp.at[to], partner).start()
            run_slots(*bounds(n))

        def plain(n, _):
            tile(n, False)
            return 0

        def normed(n, _):
            tile(n, True)
            return 0
        lax.fori_loop(0, 1, plain, 0)
        begin()
        lax.fori_loop(1, 2, plain, 0)
        loaded()
        lax.fori_loop(2, n_tiles, normed, 0)

    def turned(v, gain):
        v = v * lax.rsqrt(jnp.mean(v * v, axis=-1, keepdims=True) + EPSILON) * gain[...].astype(F32)[None]
        return v * cosb[...] + pltpu.roll(v, lanes // 2, 1) * sinb[...]

    def rope_rows(i):
        where = jnp.broadcast_to(positions[pl.ds(i, 1), :].astype(F32), (lanes, seq)).T * freq[...]
        sine = jnp.sin(where)
        cosb[...] = jnp.cos(where)
        sinb[...] = jnp.where(lax.broadcasted_iota(jnp.int32, (seq, lanes), 1) < lanes // 2, -sine, sine)

    def keep_kv(y, length):
        k_rot = turned(y[:, :lanes], k_gain)
        v_val = y[:, lanes:]
        kk[...] = k_rot.astype(BF)
        vt[...] = v_val.T.astype(BF)
        valid = lax.broadcasted_iota(jnp.int32, (seq, lanes), 0) < length
        seen[...] = jnp.where(valid, 1.0, 0.0)
        kco[...] = jnp.where(valid, k_rot, 0.0).astype(BF)
        vco[...] = jnp.where(valid, v_val, 0.0).astype(BF)

    def keep_q(t, y):
        for s in range(TILE // lanes):
            qs[:, pl.ds(pl.multiple_of(t * TILE + s * lanes, lanes), lanes)] = turned(y[:, s * lanes:(s + 1) * lanes], q_gain).astype(BF)

    def attend(hd):
        cols = pl.ds(pl.multiple_of(hd * lanes, lanes), lanes)
        for lo in range(0, seq, span_q):
            hi = lo + span_q
            q = qs[lo:hi, cols]
            s = dot_nt(kk[:hi, :], q)
            parts = [jnp.where((seen[lo:hi, :span_q] > 0.0) & (tri[...] > 0.0), s[lo:hi, :], hidden_score)]
            for r in range(0, lo, span_q):
                parts.append(jnp.where(seen[r:r + span_q, :span_q] > 0.0, s[r:r + span_q, :], hidden_score))
            top = parts[0].max(0, keepdims=True)
            for x in parts[1:]:
                top = jnp.maximum(top, x.max(0, keepdims=True))
            parts = [jnp.exp2((x - top) * to_exp2) for x in parts]
            total = parts[0].sum(0, keepdims=True)
            for x in parts[1:]:
                total = total + x.sum(0, keepdims=True)
            scale = 1.0 / total
            probs = [(x * scale).astype(BF) for x in parts[1:] + parts[:1]]
            probs = jnp.concatenate(probs, axis=0) if len(probs) > 1 else probs[0]
            os[lo:hi, cols] = dot(vt[:, :hi], probs).T.astype(BF)

    step_a = (per_ar + lead - UNITS) // (prompts - 1)
    w_q, w_h, w_o = 4, 7, 2
    weight_a = w_q * (q_tiles + 1) + w_h * (heads // HEADS_AT_ONCE) + w_o * n_tiles

    with jax.named_scope('norm_x'):
        norm_all(0)

    def attention_phase(i, _):
        def upto(w):
            return jnp.where(i == 0, 0, UNITS + (i - 1) * step_a + over(w * step_a, weight_a))
        length = lens[i]
        def kv_body(t, _):
            start_all(a_tile(A_BUFS - 1))
            with jax.named_scope('qkv'):
                wait_all(a_tile(0))
                rope_rows(i)
                ybuf[0] = dot(n2[...], a_place(0)[1][...])
            return 0
        lax.fori_loop(i, i + 1, kv_body, 0)

        def q0_body(t, _):
            start_all(a_tile(A_BUFS))
            with jax.named_scope('qkv'):
                wait_all(a_tile(1))
                keep_kv(ybuf[0], length)
                ybuf[1] = dot(n2[...], a_place(1)[1][...])
            return 0
        lax.fori_loop(i, i + 1, q0_body, 0)
        run_slots(upto(0), upto(2 * w_q))

        def q_body(t, _):
            with jax.named_scope('qkv'):
                wait_all(a_tile(t))
                keep_q(t - 2, ybuf[lax.rem(t - 1, 2)])
                ybuf[lax.rem(t, 2)] = dot(n2[...], a_place(t)[1][...])
            run_slots(upto(t * w_q), upto((t + 1) * w_q))
            return 0
        lax.fori_loop(2, q_tiles + 1, q_body, 0)

        @pl.when(i + 1 < prompts)
        def _():
            start_all(load_rows(tokens, i + 1))
            for t in range(A_BUFS - 1):
                start_all(a_tile(t))

        @pl.when(i + 1 == prompts)
        def _():
            start_all(f_tile(0))
        rows = pl.ds(pl.multiple_of(i * seq, seq), seq)
        caches = (local(kco, kc.at[rows, :], s_kv.at[0]), local(vco, vc.at[rows, :], s_kv.at[1]))
        start_all(caches)
        with jax.named_scope('keep_q'):
            keep_q(q_tiles - 1, ybuf[q_tiles % 2])
        base1 = (q_tiles + 1) * w_q

        def heads_body(t, _):
            with jax.named_scope('attend'):
                for hd in range(HEADS_AT_ONCE):
                    attend(t * HEADS_AT_ONCE + hd)
            run_slots(upto(base1 + t * w_h), upto(base1 + (t + 1) * w_h))
            return 0
        lax.fori_loop(0, heads // HEADS_AT_ONCE, heads_body, 0)
        base = base1 + heads // HEADS_AT_ONCE * w_h
        wait_all(caches)

        def bounds(n):
            return (jnp.where(i == 0, n // 2, upto(base + n * w_o)),
                    jnp.where(i == 0, (n + 1) // 2, upto(base + (n + 1) * w_o)))

        def loaded():
            @pl.when(i + 1 < prompts)
            def _():
                wait_all(load_rows(tokens, i + 1))
        with jax.named_scope('project_o'):
            project(os, o_tile, o_place, o_bufs - 1, i, 0, bounds, lambda: None, loaded)

        @pl.when(i + 1 < prompts)
        def _():
            for n in range(o_bufs - 1):
                o_tile(n).start()

        @pl.when(i + 1 == prompts)
        def _():
            d_tile(0).start()
        return 0
    lax.fori_loop(0, prompts, attention_phase, 0)

    a_end = UNITS + (prompts - 1) * step_a
    with jax.named_scope('pre_mlp'):
        run_slots(a_end, per_ar + lead)
    start_all(load_rows(ho, 0))
    with jax.named_scope('norm_h'):
        norm_all(1)
    starts = [(m + 1) * per_ar + v for m, v in zip(range(prompts), (lead, 18, 32))]
    mids = [(m + 2) * per_ar + v for m, v in zip(range(prompts), (3, 15, 30))]
    ones = [max((m + 2) * per_ar + lead, mids[m] + 2) if m + 1 < prompts else mids[m] for m in range(prompts)]
    ends = starts[1:] + [last * per_ar + UNITS * UNITS]

    soon = [0, 0, 1]
    for g in range(1, UNITS):
        soon += [g * UNITS, g * UNITS + (g + 2) // 2]
    soon = soon[:n_tiles] + [UNITS * UNITS]

    def mlp_phase(i, _):
        k0, k1, kt, k2 = pick(i, starts), pick(i, mids), pick(i, ones), pick(i, ends)

        def gated(y, width):
            gate, up = y[:, :width], y[:, width:]
            return (gate * jax.nn.sigmoid(gate) * up).astype(BF)

        def f_body(t, _):
            @pl.when(t + 1 < f_tiles)
            def _():
                start_all(f_tile(t + 1))
            if odd:
                @pl.when(t + 1 == f_tiles)
                def _():
                    start_all(f_rest())
            with jax.named_scope('w_gu'):
                wait_all(f_tile(t))
            act[:, pl.ds(pl.multiple_of(t * TILE, TILE), TILE)] = gated(dot(n2[...], gu[lax.rem(t, 2)]), TILE)
            run_slots(k0 + over(t * (k1 - k0), f_tiles), k0 + over((t + 1) * (k1 - k0), f_tiles))
            return 0
        with jax.named_scope('f_loop'):
            lax.fori_loop(0, f_tiles, f_body, 0)
        if odd:
            def rest_body(t, _):
                with jax.named_scope('f_rest'):
                    wait_all(f_rest())
                    act[:, f_tiles * TILE:] = gated(dot(n2[...], gu[f_tiles % 2, :, :TILE]), lanes)
                return 0
            lax.fori_loop(i, i + 1, rest_body, 0)

        @pl.when(i + 1 < prompts)
        def _():
            start_all(f_tile(0))

        def upto(n):
            spread = jnp.where(n <= 1, k1 + n * (kt - k1), kt + over(jnp.maximum(n - 1, 0) * (k2 - kt), n_tiles - 1))
            return jnp.where(i == prompts - 1, k1 + pick(n, soon), spread)

        def begin():
            @pl.when(i + 1 < prompts)
            def _():
                start_all(load_rows(ho, i + 1))

        def loaded():
            @pl.when(i + 1 < prompts)
            def _():
                wait_all(load_rows(ho, i + 1))
        with jax.named_scope('project_d'):
            project(act, d_tile, d_place, 1, prompts + i, 1, lambda n: (upto(n), upto(n + 1)), begin, loaded)

        @pl.when(i + 1 < prompts)
        def _():
            d_tile(0).start()
        return 0
    lax.fori_loop(0, prompts, mlp_phase, 0)

    with jax.named_scope('tail'):
        run_slots(last * per_ar + UNITS * UNITS, last * per_ar + (UNITS + HOPS - 1) * UNITS)

        def ring_end(g, _):
            pass_on(3, last, g)
            return 0
        lax.fori_loop(0, UNITS, ring_end, 0)

        def all_end(g, _):
            settle(last, g)
            return 0
        lax.fori_loop(0, UNITS, all_end, 0)
        for s in range(2):
            await_copy(pp.at[2 * UNITS + s], s_stage.at[s])


def copy_kernel(a, b, c, a_out, b_out, c_out):
    a_out[...] = a[...]
    b_out[...] = b[...]
    c_out[...] = c[...]


def layer_body(tokens, positions, lengths, norm_attn, norm_mlp, q_gain, k_gain, w_query, w_key, w_value, w_out, w_gate, w_up, w_down, tp_size):
    prompts, seq, hidden = tokens.shape
    head_dim = q_gain.shape[0]
    width_q, width_f = w_query.shape[1], w_gate.shape[1]
    kv_heads = w_key.shape[1] // head_dim
    chips = tp_size // CORES
    unit = hidden // CORES // UNITS
    rows_n = prompts * seq
    inv_freq = ROPE_THETA ** (-np.arange(head_dim // 2) / (head_dim // 2))
    freq = jnp.asarray(np.concatenate([inv_freq, inv_freq])[None], F32)
    any_spec = pl.BlockSpec(memory_space=pl.ANY)
    vmem = pl.BlockSpec(memory_space=pltpu.VMEM)
    smem = pl.BlockSpec(memory_space=pltpu.SMEM)
    kernel = functools.partial(layer_kernel, tp_size, prompts, seq, head_dim, kv_heads, (hidden, width_q, width_f))
    dma = pltpu.SemaphoreType.DMA
    o_bufs = 2 * (width_f // width_q)
    span_q = min(head_dim, seq)
    ho, kc, vc = pl.pallas_call(
        kernel,
        name='decoder_layer',
        out_shape=(jax.ShapeDtypeStruct((2 * rows_n, hidden), BF),
                   jax.ShapeDtypeStruct((rows_n, head_dim), BF),
                   jax.ShapeDtypeStruct((rows_n, head_dim), BF)),
        in_specs=[any_spec, vmem, smem, vmem, vmem, vmem, vmem, vmem] + [any_spec] * 7,
        out_specs=(any_spec, any_spec, any_spec),
        scratch_shapes=[
            pltpu.VMEM((seq, hidden), BF),
            pltpu.VMEM((seq, width_f), BF),
            pltpu.VMEM((seq, width_q), BF), pltpu.VMEM((seq, width_q), BF),
            pltpu.VMEM((seq, head_dim), BF), pltpu.VMEM((head_dim, seq), BF),
            pltpu.VMEM((seq, head_dim), BF), pltpu.VMEM((seq, head_dim), BF),
            pltpu.VMEM((seq, head_dim), F32), pltpu.VMEM((seq, head_dim), F32),
            pltpu.VMEM((2, seq, TILE), F32),
            pltpu.VMEM((seq, head_dim), F32),
            pltpu.VMEM((span_q, span_q), F32),
            pltpu.VMEM((2, 16, hidden), F32),
            pltpu.VMEM((2, hidden, 2 * TILE), BF),
            pltpu.VMEM((2, width_f, unit), BF),
            pltpu.VMEM((2 * UNITS + 2, seq, unit), BF),
            pltpu.VMEM((2 * UNITS, seq, unit), BF),
            pltpu.VMEM((2, UNITS, 3, seq // chips, unit), BF),
            pltpu.VMEM((prompts * UNITS, seq // chips, unit), BF),
            dma((X_PARTS,)), dma((A_BUFS, 2)), dma((o_bufs,)), dma((2,)), dma((2 * UNITS,)), dma((prompts * UNITS,)), dma((2,)), dma((2, UNITS)),
            dma((2, UNITS, 3)), dma((2, UNITS, 3)), dma((2, UNITS, 3)), dma((2, UNITS, 3)), dma((2, UNITS, 4)), dma((2, UNITS, 4)),
        ],
        compiler_params=pltpu.CompilerParams(collective_id=0, has_side_effects=True, vmem_limit_bytes=67043328),
    )(tokens.reshape(rows_n, hidden), positions, lengths, norm_attn, norm_mlp, q_gain, k_gain, freq,
      w_query, w_key, w_value, w_out, w_gate, w_up, w_down)
    shape = (prompts, seq, 1, head_dim)
    parts = 2 * prompts
    block = rows_n // parts
    out, kc, vc = pl.pallas_call(
        copy_kernel,
        name='copy_out',
        grid=(parts,),
        out_shape=(jax.ShapeDtypeStruct((rows_n, hidden), BF), jax.ShapeDtypeStruct(kc.shape, BF), jax.ShapeDtypeStruct(vc.shape, BF)),
        in_specs=[pl.BlockSpec((block, hidden), lambda b: (b + parts, 0))] + [pl.BlockSpec((block, head_dim), lambda b: (b, 0))] * 2,
        out_specs=[pl.BlockSpec((block, hidden), lambda b: (b, 0))] + [pl.BlockSpec((block, head_dim), lambda b: (b, 0))] * 2,
        compiler_params=pltpu.CompilerParams(vmem_limit_bytes=40 * 1024 * 1024),
    )(ho, kc, vc)
    return out.reshape(prompts, seq, hidden), kc.reshape(shape), vc.reshape(shape)


def solution(mesh):
    body = functools.partial(layer_body, tp_size=mesh.shape['tp'])
    in_specs = (P('dp', None, None), P('dp', None), P('dp'), P(), P(), P(), P(), P(None, 'tp'), P(), P(), P('tp', None), P(None, 'tp'), P(None, 'tp'), P('tp', None))
    out_specs = (P('dp', None, None), P('dp', None, 'tp', None), P('dp', None, 'tp', None))
    return jax.shard_map(body, mesh=mesh, in_specs=in_specs, out_specs=out_specs, check_vma=False)
```

```python
import functools
import jax
import jax.numpy as jnp
import numpy as np
from jax import lax
from jax.experimental import pallas as pl
from jax.experimental.pallas import tpu as pltpu
from jax.sharding import PartitionSpec as P

EPSILON = 1e-6
ROPE_THETA = 1000000.0
MESH = pl.DeviceIdType.MESH
CORES = 2
TILE = 256
UNITS = 5
HOPS = 6
A_BUFS = 4
X_PARTS = 4
HEADS_AT_ONCE = 4
BF = jnp.bfloat16
F32 = jnp.float32


def dot(a, b):
    return jnp.dot(a, b, preferred_element_type=F32)


def dot_nt(a, b):
    return lax.dot_general(a, b, (((1,), (1,)), ((), ())), preferred_element_type=F32)


def over(x, n):
    return lax.shift_right_logical(x * (65536 // n + 1), 16)


def split(x, n):
    q = over(x, n)
    return q, x - q * n


def pick(i, values):
    out = values[0]
    for n, v in enumerate(values[1:], 1):
        out = jnp.where(i >= n, v, out)
    return out


def layer_kernel(tp, prompts, seq, head_dim, kv_heads, dims,
                 tokens, positions, lens, n_attn, n_mlp, q_gain, k_gain, freq, wq, wk, wv, wo, wg, wu, wdn,
                 ho, kc, vc,
                 n2, act, qs, os, kk, vt, kco, vco, cosb, sinb, ybuf, seen, tri, gains, gu, wd, pp, xp, land, ownh,
                 s_x, s_gu, s_wd, s_stage, s_xp, s_res, s_kv, s_own,
                 rs_send, rs_recv, ag_send, ag_recv, dd_send, dd_recv):
    hidden, width_q, width_f = dims
    chips = tp // CORES
    half = hidden // CORES
    unit = half // UNITS
    rows_b = seq // chips
    heads = width_q // head_dim
    q_tiles = width_q // TILE
    f_tiles = width_f // TILE
    odd = width_f % TILE != 0
    n_tiles = CORES * UNITS
    per_ar = HOPS * UNITS
    lead = UNITS + 1
    last = 2 * prompts - 1
    lanes = head_dim
    add_rows = rows_b // 4 if rows_b % 64 == 0 else 16
    o_bufs = 2 * (width_f // width_q)
    row_groups = min(6, seq // X_PARTS // 16)
    norm_tiles = n_tiles - 2
    norm_rows = seq // norm_tiles
    span_q = min(lanes, seq)
    hidden_score = -1e30 * head_dim ** 0.5
    to_exp2 = head_dim ** -0.5 * 1.4426950408889634

    me = lax.axis_index('tp')
    core = lax.rem(me, CORES)
    chip = me // CORES
    ring = lax.rem(chip + core * (chips - 2 * chip), chips)
    nxt = CORES * lax.rem(chip + chips + 1 - 2 * core, chips) + core
    prv = CORES * lax.rem(chip + chips - 1 + 2 * core, chips) + core
    partner = me + 1 - 2 * core
    kv_col = pl.multiple_of((me // (tp // kv_heads)) * head_dim, head_dim)

    def remote(src, dst, send, recv, to):
        return pltpu.make_async_remote_copy(src_ref=src, dst_ref=dst, send_sem=send, recv_sem=recv,
                                            device_id={'tp': to}, device_id_type=MESH)

    def local(src, dst, sem):
        return pltpu.make_async_copy(src, dst, sem)

    def await_copy(ref, sem):
        local(ref, ref, sem).wait()

    def wrap(b):
        return jnp.where(b < 0, b + chips, b)

    def block_rows(b):
        return pl.ds(pl.multiple_of(b * rows_b, rows_b), rows_b)

    def a_place(t):
        b = t % A_BUFS if isinstance(t, int) else lax.bitwise_and(t, A_BUFS - 1)
        return b, gu.at[b // 2, :, pl.ds(pl.multiple_of(lax.rem(b, 2) * TILE, TILE), TILE)]

    def a_tile(t):
        if isinstance(t, int) and t == 0:
            return (local(wk.at[:, pl.ds(kv_col, lanes)], gu.at[0, :, pl.ds(0, lanes)], s_gu.at[0, 0]),
                    local(wv.at[:, pl.ds(kv_col, lanes)], gu.at[0, :, pl.ds(lanes, lanes)], s_gu.at[0, 1]))
        b, place = a_place(t)
        return (local(wq.at[:, pl.ds(pl.multiple_of((t - 1) * TILE, TILE), TILE)], place, s_gu.at[b, 0]),)

    def f_pair(b, col, width):
        cols = pl.ds(pl.multiple_of(col, lanes), width)
        return (local(wg.at[:, cols], gu.at[b, :, pl.ds(0, width)], s_gu.at[b, 0]),
                local(wu.at[:, cols], gu.at[b, :, pl.ds(width, width)], s_gu.at[b, 1]))

    def f_tile(t):
        return f_pair(lax.rem(t, 2), t * TILE, TILE)

    def f_rest():
        return f_pair(f_tiles % 2, f_tiles * TILE, lanes)

    def start_all(copies):
        for cp in copies:
            cp.start()

    def wait_all(copies):
        for cp in copies:
            cp.wait()

    def out_cols(n):
        side = jnp.where(lax.rem(n, 2) == 0, 1 - core, core)
        return pl.ds(pl.multiple_of(side * half + lax.shift_right_logical(n, 1) * unit, unit), unit)

    def o_place(n):
        b = lax.rem(n, o_bufs)
        return wd.at[b // (o_bufs // 2), pl.ds(pl.multiple_of(lax.rem(b, o_bufs // 2) * width_q, width_q), width_q), :]

    def o_tile(n):
        return local(wo.at[:, out_cols(n)], o_place(n), s_wd.at[lax.rem(n, o_bufs)])

    def d_place(n):
        return wd.at[lax.rem(n, 2)]

    def d_tile(n):
        return local(wdn.at[:, out_cols(n)], d_place(n), s_wd.at[lax.rem(n, 2)])

    def load_rows(src, i):
        part = seq // X_PARTS
        return [local(src.at[pl.ds(pl.multiple_of(i * seq + b * part, part), part), :], n2.at[pl.ds(b * part, part), :], s_x.at[b])
                for b in range(X_PARTS)]

    start_all(load_rows(tokens, 0))
    for t in range(A_BUFS - 1):
        start_all(a_tile(t))
    barrier = pltpu.get_barrier_semaphore()
    for other in (nxt, prv, partner):
        pl.semaphore_signal(barrier, inc=1, device_id={'tp': other}, device_id_type=MESH)

    for v, gain in enumerate((n_attn, n_mlp)):
        wide = gain[...].astype(F32)
        for j in range(hidden // lanes):
            gains[v, :, j * lanes:(j + 1) * lanes] = jnp.broadcast_to(wide[None, j * lanes:(j + 1) * lanes], (16, lanes))
    key_at = lax.broadcasted_iota(jnp.int32, (span_q, span_q), 0)
    tri[...] = jnp.where(key_at <= lax.broadcasted_iota(jnp.int32, (span_q, span_q), 1), 1.0, 0.0)
    pl.semaphore_wait(barrier, 3)

    def ho_block(c, g, b, side):
        rows = pl.ds(pl.multiple_of(c * seq + b * rows_b, rows_b), rows_b)
        return ho.at[rows, pl.ds(pl.multiple_of(side * half + g * unit, unit), unit)]

    def send_partial(e, c, g):
        par = lax.bitwise_and(c, 1)
        u = par * UNITS + g
        rows = block_rows(wrap(ring - 1 - e))
        with jax.named_scope('w_rs'):
            if e == 0:
                await_copy(xp.at[u], s_xp.at[u])
            else:
                await_copy(land.at[par, g, e - 1], rs_recv.at[par, g, e - 1])
        mine, theirs, came = pp.at[u, rows], xp.at[u, rows], land.at[par, g, max(e - 1, 0)]

        def add(r, _):
            rr = pl.ds(pl.multiple_of(r * add_rows, 16), add_rows)
            total = mine[rr, :].astype(F32) + theirs[rr, :].astype(F32)
            if e > 0:
                total = total + came[rr, :].astype(F32)
            mine[rr, :] = total.astype(BF)
            return 0
        lax.fori_loop(0, rows_b // add_rows, add, 0)
        remote(mine, land.at[par, g, e], rs_send.at[par, g, e], rs_recv.at[par, g, e], nxt).start()

    def finish_sum(c, g):
        par = lax.bitwise_and(c, 1)
        u, w = par * UNITS + g, jnp.where(c < prompts, c, c - prompts) * UNITS + g
        rows = block_rows(ring)
        with jax.named_scope('w_rs3'):
            await_copy(land.at[par, g, 2], rs_recv.at[par, g, 2])

        @pl.when(c < prompts)
        def _():
            await_copy(ownh.at[w], s_res.at[w])
        mine, theirs, came, own = pp.at[u, rows], xp.at[u, rows], land.at[par, g, 2], ownh.at[w]

        def add(r, _):
            rr = pl.ds(pl.multiple_of(r * add_rows, 16), add_rows)
            total = came[rr, :].astype(F32) + (mine[rr, :].astype(F32) + theirs[rr, :].astype(F32))
            own[rr, :] = (own[rr, :].astype(F32) + total).astype(BF)
            return 0
        lax.fori_loop(0, rows_b // add_rows, add, 0)
        place = ho_block(c, g, ring, core)
        remote(own, place, ag_send.at[par, g, 0], ag_recv.at[par, g, 0], nxt).start()
        remote(own, place, dd_send.at[par, g, 0], dd_recv.at[par, g, 0], partner).start()
        local(own, place, s_own.at[par, g]).start()

    def pass_on(e, c, g):
        par = lax.bitwise_and(c, 1)
        place = ho_block(c, g, wrap(ring - e), core)
        with jax.named_scope('w_ag'):
            await_copy(place, ag_recv.at[par, g, e - 1])
        if e < 3:
            remote(place, place, ag_send.at[par, g, e], ag_recv.at[par, g, e], nxt).start()
        remote(place, place, dd_send.at[par, g, e], dd_recv.at[par, g, e], partner).start()
        if e == 1:
            await_copy(place, dd_recv.at[par, g, 0])
            for s in range(3):
                await_copy(land.at[par, g, s], rs_send.at[par, g, s])

    def settle(c, g):
        par = lax.bitwise_and(c, 1)
        place = ho_block(c, g, ring, core)
        await_copy(land.at[par, g, 0], s_own.at[par, g])
        for e in range(3):
            await_copy(place, ag_send.at[par, g, e])
        for e in range(4):
            await_copy(place, dd_send.at[par, g, e])
        for e in range(1, 4):
            await_copy(place, dd_recv.at[par, g, e])

    def slot(k):
        c = jnp.minimum(over(k, per_ar), last)
        diagonal = c == last
        d, q = split(k - c * per_ar, UNITS)
        g_d = jnp.minimum(d, UNITS - 1) - q
        e_d = jnp.where(g_d >= 0, d - g_d, HOPS)
        e = jnp.where(diagonal, e_d, d)
        g = jnp.where(diagonal, jnp.maximum(g_d, 0), q)
        @pl.when(e < 3)
        def _():
            for s in range(3):
                @pl.when(e == s)
                def _(s=s):
                    send_partial(s, c, g)
                    if s == 0:
                        @pl.when(c > 0)
                        def _():
                            pass_on(3, c - 1, g)

                            @pl.when((g > 0) & jnp.logical_not(diagonal))
                            def _():
                                settle(c - 1, g - 1)
                    if s == 1:
                        @pl.when((c > 0) & (diagonal | (g == 0)))
                        def _():
                            settle(c - 1, jnp.where(diagonal, g, UNITS - 1))

        @pl.when(e >= 3)
        def _():
            @pl.when(e == 3)
            def _():
                finish_sum(c, g)
            for s in range(2):
                @pl.when(e == 4 + s)
                def _(s=s):
                    pass_on(s + 1, c, g)

    def run_slots(lo, hi):
        def body(k, _):
            slot(k)
            return 0
        lax.fori_loop(lo, hi, body, 0)

    def norm_all(v):
        part = seq // X_PARTS
        for b in range(X_PARTS):
            await_copy(n2.at[pl.ds(b * part, part), :], s_x.at[b])

            def scales(r, _):
                for q in range(row_groups):
                    rr = pl.ds(pl.multiple_of(b * part + (r * row_groups + q) * 16, 16), 16)
                    acc = jnp.zeros((16, lanes), F32)
                    for j in range(hidden // lanes):
                        x = n2[rr, j * lanes:(j + 1) * lanes].astype(F32)
                        acc = acc + x * x
                    scale = lax.rsqrt(jnp.sum(acc, axis=-1, keepdims=True) * (1.0 / hidden) + EPSILON)
                    ybuf[0, rr, :lanes] = jnp.broadcast_to(scale, (16, lanes))
                return 0
            lax.fori_loop(0, part // 16 // row_groups, scales, 0)

        def apply(r, _):
            rr = pl.ds(pl.multiple_of(r * 16, 16), 16)
            scale = ybuf[0, rr, :lanes]
            for j in range(hidden // lanes):
                cols = slice(j * lanes, (j + 1) * lanes)
                n2[rr, cols] = (n2[rr, cols].astype(F32) * scale * gains[v, :, cols]).astype(BF)
            return 0
        lax.fori_loop(0, seq // 16, apply, 0)

    def norm_some(v, first):
        for q in range(norm_rows // 16):
            rr = pl.ds(pl.multiple_of(first + q * 16, 16), 16)
            acc = jnp.zeros((16, lanes), F32)
            for j in range(hidden // lanes):
                x = n2[rr, j * lanes:(j + 1) * lanes].astype(F32)
                acc = acc + x * x
            scale = jnp.broadcast_to(lax.rsqrt(jnp.sum(acc, axis=-1, keepdims=True) * (1.0 / hidden) + EPSILON), (16, lanes))
            for j in range(hidden // lanes):
                cols = slice(j * lanes, (j + 1) * lanes)
                n2[rr, cols] = (n2[rr, cols].astype(F32) * scale * gains[v, :, cols]).astype(BF)

    def project(lhs, fetch, place, ahead, c, v, bounds, begin, loaded):
        par = lax.bitwise_and(c, 1)

        def tile(n, norm):
            @pl.when(n + ahead < n_tiles)
            def _():
                fetch(n + ahead).start()
            with jax.named_scope('w_wd'):
                fetch(n).wait()
            g = n // 2
            away = lax.rem(n, 2) == 0
            count = c * UNITS + g
            stage = lax.rem(count, 2)
            u = jnp.where(away, 2 * UNITS + stage, par * UNITS + g)

            @pl.when(away & (count >= 2))
            def _():
                await_copy(pp.at[u], s_stage.at[stage])
            if norm:
                norm_some(v, pl.multiple_of((n - 2) * norm_rows, 16))
            pp[u] = dot(lhs[...], place(n)[...]).astype(BF)

            @pl.when(away)
            def _():
                to = par * UNITS + g
                remote(pp.at[u], xp.at[to], s_stage.at[stage], s_xp.at[to], partner).start()
            run_slots(*bounds(n))

        def plain(n, _):
            tile(n, False)
            return 0

        def normed(n, _):
            tile(n, True)
            return 0
        lax.fori_loop(0, 1, plain, 0)
        begin()
        lax.fori_loop(1, 2, plain, 0)
        loaded()
        lax.fori_loop(2, n_tiles, normed, 0)

    def turned(v, gain):
        v = v * lax.rsqrt(jnp.mean(v * v, axis=-1, keepdims=True) + EPSILON) * gain[...].astype(F32)[None]
        return v * cosb[...] + pltpu.roll(v, lanes // 2, 1) * sinb[...]

    def rope_rows(i):
        where = jnp.broadcast_to(positions[pl.ds(i, 1), :].astype(F32), (lanes, seq)).T * freq[...]
        sine = jnp.sin(where)
        cosb[...] = jnp.cos(where)
        sinb[...] = jnp.where(lax.broadcasted_iota(jnp.int32, (seq, lanes), 1) < lanes // 2, -sine, sine)

    def keep_kv(y, length):
        k_rot = turned(y[:, :lanes], k_gain)
        v_val = y[:, lanes:]
        kk[...] = k_rot.astype(BF)
        vt[...] = v_val.T.astype(BF)
        valid = lax.broadcasted_iota(jnp.int32, (seq, lanes), 0) < length
        seen[...] = jnp.where(valid, 1.0, 0.0)
        kco[...] = jnp.where(valid, k_rot, 0.0).astype(BF)
        vco[...] = jnp.where(valid, v_val, 0.0).astype(BF)

    def keep_q(t, y):
        for s in range(TILE // lanes):
            qs[:, pl.ds(pl.multiple_of(t * TILE + s * lanes, lanes), lanes)] = turned(y[:, s * lanes:(s + 1) * lanes], q_gain).astype(BF)

    def attend(hd):
        cols = pl.ds(pl.multiple_of(hd * lanes, lanes), lanes)
        for lo in range(0, seq, span_q):
            hi = lo + span_q
            q = qs[lo:hi, cols]
            s = dot_nt(kk[:hi, :], q)
            parts = [jnp.where((seen[lo:hi, :span_q] > 0.0) & (tri[...] > 0.0), s[lo:hi, :], hidden_score)]
            for r in range(0, lo, span_q):
                parts.append(jnp.where(seen[r:r + span_q, :span_q] > 0.0, s[r:r + span_q, :], hidden_score))
            top = parts[0].max(0, keepdims=True)
            for x in parts[1:]:
                top = jnp.maximum(top, x.max(0, keepdims=True))
            parts = [jnp.exp2((x - top) * to_exp2) for x in parts]
            total = parts[0].sum(0, keepdims=True)
            for x in parts[1:]:
                total = total + x.sum(0, keepdims=True)
            scale = 1.0 / total
            probs = [(x * scale).astype(BF) for x in parts[1:] + parts[:1]]
            probs = jnp.concatenate(probs, axis=0) if len(probs) > 1 else probs[0]
            os[lo:hi, cols] = dot(vt[:, :hi], probs).T.astype(BF)

    step_a = (per_ar + lead - UNITS) // (prompts - 1)
    w_q, w_h, w_o = 4, 7, 2
    weight_a = w_q * (q_tiles + 1) + w_h * (heads // HEADS_AT_ONCE) + w_o * n_tiles

    with jax.named_scope('norm_x'):
        norm_all(0)
    for n in range(o_bufs - 1):
        o_tile(n).start()
    for i in range(prompts):
        for g in range(UNITS):
            rows = pl.ds(pl.multiple_of(i * seq + ring * rows_b, rows_b), rows_b)
            cols = pl.ds(pl.multiple_of(core * half + g * unit, unit), unit)
            local(tokens.at[rows, cols], ownh.at[i * UNITS + g], s_res.at[i * UNITS + g]).start()

    def attention_phase(i, _):
        def upto(w):
            return jnp.where(i == 0, 0, UNITS + (i - 1) * step_a + over(w * step_a, weight_a))
        length = lens[i]
        def kv_body(t, _):
            start_all(a_tile(A_BUFS - 1))
            with jax.named_scope('qkv'):
                wait_all(a_tile(0))
                rope_rows(i)
                ybuf[0] = dot(n2[...], a_place(0)[1][...])
            return 0
        lax.fori_loop(i, i + 1, kv_body, 0)

        def q0_body(t, _):
            start_all(a_tile(A_BUFS))
            with jax.named_scope('qkv'):
                wait_all(a_tile(1))
                keep_kv(ybuf[0], length)
                ybuf[1] = dot(n2[...], a_place(1)[1][...])
            return 0
        lax.fori_loop(i, i + 1, q0_body, 0)
        run_slots(upto(0), upto(2 * w_q))

        def q_body(t, _):
            with jax.named_scope('qkv'):
                wait_all(a_tile(t))
                keep_q(t - 2, ybuf[lax.rem(t - 1, 2)])
                ybuf[lax.rem(t, 2)] = dot(n2[...], a_place(t)[1][...])
            run_slots(upto(t * w_q), upto((t + 1) * w_q))
            return 0
        lax.fori_loop(2, q_tiles + 1, q_body, 0)

        @pl.when(i + 1 < prompts)
        def _():
            start_all(load_rows(tokens, i + 1))
            for t in range(A_BUFS - 1):
                start_all(a_tile(t))

        @pl.when(i + 1 == prompts)
        def _():
            start_all(f_tile(0))
        rows = pl.ds(pl.multiple_of(i * seq, seq), seq)
        caches = (local(kco, kc.at[rows, :], s_kv.at[0]), local(vco, vc.at[rows, :], s_kv.at[1]))
        start_all(caches)
        with jax.named_scope('keep_q'):
            keep_q(q_tiles - 1, ybuf[q_tiles % 2])
        base1 = (q_tiles + 1) * w_q

        def heads_body(t, _):
            with jax.named_scope('attend'):
                for hd in range(HEADS_AT_ONCE):
                    attend(t * HEADS_AT_ONCE + hd)
            run_slots(upto(base1 + t * w_h), upto(base1 + (t + 1) * w_h))
            return 0
        lax.fori_loop(0, heads // HEADS_AT_ONCE, heads_body, 0)
        base = base1 + heads // HEADS_AT_ONCE * w_h
        wait_all(caches)

        def bounds(n):
            return (jnp.where(i == 0, n // 2, upto(base + n * w_o)),
                    jnp.where(i == 0, (n + 1) // 2, upto(base + (n + 1) * w_o)))

        def loaded():
            @pl.when(i + 1 < prompts)
            def _():
                wait_all(load_rows(tokens, i + 1))
        with jax.named_scope('project_o'):
            project(os, o_tile, o_place, o_bufs - 1, i, 0, bounds, lambda: None, loaded)

        @pl.when(i + 1 < prompts)
        def _():
            for n in range(o_bufs - 1):
                o_tile(n).start()

        @pl.when(i + 1 == prompts)
        def _():
            d_tile(0).start()
        return 0
    lax.fori_loop(0, prompts, attention_phase, 0)

    a_end = UNITS + (prompts - 1) * step_a
    with jax.named_scope('pre_mlp'):
        run_slots(a_end, per_ar + lead)
    start_all(load_rows(ho, 0))
    with jax.named_scope('norm_h'):
        norm_all(1)
    starts = [(m + 1) * per_ar + v for m, v in zip(range(prompts), (lead, 18, 32))]
    mids = [(m + 2) * per_ar + v for m, v in zip(range(prompts), (3, 15, 30))]
    ones = [max((m + 2) * per_ar + lead, mids[m] + 2) if m + 1 < prompts else mids[m] for m in range(prompts)]
    ends = starts[1:] + [last * per_ar + UNITS * UNITS]

    soon = [0, 0, 1]
    for g in range(1, UNITS):
        soon += [g * UNITS, g * UNITS + (g + 2) // 2]
    soon = soon[:n_tiles] + [UNITS * UNITS]

    def mlp_phase(i, _):
        k0, k1, kt, k2 = pick(i, starts), pick(i, mids), pick(i, ones), pick(i, ends)

        def gated(y, width):
            gate, up = y[:, :width], y[:, width:]
            return (gate * jax.nn.sigmoid(gate) * up).astype(BF)

        def f_body(t, _):
            @pl.when(t + 1 < f_tiles)
            def _():
                start_all(f_tile(t + 1))
            if odd:
                @pl.when(t + 1 == f_tiles)
                def _():
                    start_all(f_rest())
            with jax.named_scope('w_gu'):
                wait_all(f_tile(t))
            act[:, pl.ds(pl.multiple_of(t * TILE, TILE), TILE)] = gated(dot(n2[...], gu[lax.rem(t, 2)]), TILE)
            run_slots(k0 + over(t * (k1 - k0), f_tiles), k0 + over((t + 1) * (k1 - k0), f_tiles))
            return 0
        with jax.named_scope('f_loop'):
            lax.fori_loop(0, f_tiles, f_body, 0)
        if odd:
            def rest_body(t, _):
                with jax.named_scope('f_rest'):
                    wait_all(f_rest())
                    act[:, f_tiles * TILE:] = gated(dot(n2[...], gu[f_tiles % 2, :, :TILE]), lanes)
                return 0
            lax.fori_loop(i, i + 1, rest_body, 0)

        @pl.when(i + 1 < prompts)
        def _():
            start_all(f_tile(0))

        def upto(n):
            spread = jnp.where(n <= 1, k1 + n * (kt - k1), kt + over(jnp.maximum(n - 1, 0) * (k2 - kt), n_tiles - 1))
            return jnp.where(i == prompts - 1, k1 + pick(n, soon), spread)

        def begin():
            @pl.when(i + 1 < prompts)
            def _():
                start_all(load_rows(ho, i + 1))

        def loaded():
            @pl.when(i + 1 < prompts)
            def _():
                wait_all(load_rows(ho, i + 1))
        with jax.named_scope('project_d'):
            project(act, d_tile, d_place, 1, prompts + i, 1, lambda n: (upto(n), upto(n + 1)), begin, loaded)

        @pl.when(i + 1 < prompts)
        def _():
            d_tile(0).start()
        return 0
    lax.fori_loop(0, prompts, mlp_phase, 0)

    with jax.named_scope('tail'):
        run_slots(last * per_ar + UNITS * UNITS, last * per_ar + (UNITS + HOPS - 1) * UNITS)

        def ring_end(g, _):
            pass_on(3, last, g)
            return 0
        lax.fori_loop(0, UNITS, ring_end, 0)

        def all_end(g, _):
            settle(last, g)
            return 0
        lax.fori_loop(0, UNITS, all_end, 0)
        for s in range(2):
            await_copy(pp.at[2 * UNITS + s], s_stage.at[s])


def copy_kernel(a, b, c, a_out, b_out, c_out):
    a_out[...] = a[...]
    b_out[...] = b[...]
    c_out[...] = c[...]


def layer_body(tokens, positions, lengths, norm_attn, norm_mlp, q_gain, k_gain, w_query, w_key, w_value, w_out, w_gate, w_up, w_down, tp_size):
    prompts, seq, hidden = tokens.shape
    head_dim = q_gain.shape[0]
    width_q, width_f = w_query.shape[1], w_gate.shape[1]
    kv_heads = w_key.shape[1] // head_dim
    chips = tp_size // CORES
    unit = hidden // CORES // UNITS
    rows_n = prompts * seq
    inv_freq = ROPE_THETA ** (-np.arange(head_dim // 2) / (head_dim // 2))
    freq = jnp.asarray(np.concatenate([inv_freq, inv_freq])[None], F32)
    any_spec = pl.BlockSpec(memory_space=pl.ANY)
    vmem = pl.BlockSpec(memory_space=pltpu.VMEM)
    smem = pl.BlockSpec(memory_space=pltpu.SMEM)
    kernel = functools.partial(layer_kernel, tp_size, prompts, seq, head_dim, kv_heads, (hidden, width_q, width_f))
    dma = pltpu.SemaphoreType.DMA
    o_bufs = 2 * (width_f // width_q)
    span_q = min(head_dim, seq)
    ho, kc, vc = pl.pallas_call(
        kernel,
        name='decoder_layer',
        out_shape=(jax.ShapeDtypeStruct((2 * rows_n, hidden), BF),
                   jax.ShapeDtypeStruct((rows_n, head_dim), BF),
                   jax.ShapeDtypeStruct((rows_n, head_dim), BF)),
        in_specs=[any_spec, vmem, smem, vmem, vmem, vmem, vmem, vmem] + [any_spec] * 7,
        out_specs=(any_spec, any_spec, any_spec),
        scratch_shapes=[
            pltpu.VMEM((seq, hidden), BF),
            pltpu.VMEM((seq, width_f), BF),
            pltpu.VMEM((seq, width_q), BF), pltpu.VMEM((seq, width_q), BF),
            pltpu.VMEM((seq, head_dim), BF), pltpu.VMEM((head_dim, seq), BF),
            pltpu.VMEM((seq, head_dim), BF), pltpu.VMEM((seq, head_dim), BF),
            pltpu.VMEM((seq, head_dim), F32), pltpu.VMEM((seq, head_dim), F32),
            pltpu.VMEM((2, seq, TILE), F32),
            pltpu.VMEM((seq, head_dim), F32),
            pltpu.VMEM((span_q, span_q), F32),
            pltpu.VMEM((2, 16, hidden), F32),
            pltpu.VMEM((2, hidden, 2 * TILE), BF),
            pltpu.VMEM((2, width_f, unit), BF),
            pltpu.VMEM((2 * UNITS + 2, seq, unit), BF),
            pltpu.VMEM((2 * UNITS, seq, unit), BF),
            pltpu.VMEM((2, UNITS, 3, seq // chips, unit), BF),
            pltpu.VMEM((prompts * UNITS, seq // chips, unit), BF),
            dma((X_PARTS,)), dma((A_BUFS, 2)), dma((o_bufs,)), dma((2,)), dma((2 * UNITS,)), dma((prompts * UNITS,)), dma((2,)), dma((2, UNITS)),
            dma((2, UNITS, 3)), dma((2, UNITS, 3)), dma((2, UNITS, 3)), dma((2, UNITS, 3)), dma((2, UNITS, 4)), dma((2, UNITS, 4)),
        ],
        compiler_params=pltpu.CompilerParams(collective_id=0, has_side_effects=True, vmem_limit_bytes=67043328),
    )(tokens.reshape(rows_n, hidden), positions, lengths, norm_attn, norm_mlp, q_gain, k_gain, freq,
      w_query, w_key, w_value, w_out, w_gate, w_up, w_down)
    shape = (prompts, seq, 1, head_dim)
    parts = 4 * prompts
    block = rows_n // parts
    out, kc, vc = pl.pallas_call(
        copy_kernel,
        name='copy_out',
        grid=(parts,),
        out_shape=(jax.ShapeDtypeStruct((rows_n, hidden), BF), jax.ShapeDtypeStruct(kc.shape, BF), jax.ShapeDtypeStruct(vc.shape, BF)),
        in_specs=[pl.BlockSpec((block, hidden), lambda b: (b + parts, 0))] + [pl.BlockSpec((block, head_dim), lambda b: (b, 0))] * 2,
        out_specs=[pl.BlockSpec((block, hidden), lambda b: (b, 0))] + [pl.BlockSpec((block, head_dim), lambda b: (b, 0))] * 2,
        compiler_params=pltpu.CompilerParams(vmem_limit_bytes=60 * 1024 * 1024),
    )(ho, kc, vc)
    return out.reshape(prompts, seq, hidden), kc.reshape(shape), vc.reshape(shape)


def solution(mesh):
    body = functools.partial(layer_body, tp_size=mesh.shape['tp'])
    in_specs = (P('dp', None, None), P('dp', None), P('dp'), P(), P(), P(), P(), P(None, 'tp'), P(), P(), P('tp', None), P(None, 'tp'), P(None, 'tp'), P('tp', None))
    out_specs = (P('dp', None, None), P('dp', None, 'tp', None), P('dp', None, 'tp', None))
    return jax.shard_map(body, mesh=mesh, in_specs=in_specs, out_specs=out_specs, check_vma=False)
```

```python
import functools
import jax
import jax.numpy as jnp
import numpy as np
from jax import lax
from jax.experimental import pallas as pl
from jax.experimental.pallas import tpu as pltpu
from jax.sharding import PartitionSpec as P

EPSILON = 1e-6
ROPE_THETA = 1000000.0
MESH = pl.DeviceIdType.MESH
CORES = 2
TILE = 256
UNITS = 5
HOPS = 6
A_BUFS = 4
X_PARTS = 4
HEADS_AT_ONCE = 4
BF = jnp.bfloat16
F32 = jnp.float32


def dot(a, b):
    return jnp.dot(a, b, preferred_element_type=F32)


def dot_nt(a, b):
    return lax.dot_general(a, b, (((1,), (1,)), ((), ())), preferred_element_type=F32)


def over(x, n):
    return lax.shift_right_logical(x * (65536 // n + 1), 16)


def split(x, n):
    q = over(x, n)
    return q, x - q * n


def pick(i, values):
    out = values[0]
    for n, v in enumerate(values[1:], 1):
        out = jnp.where(i >= n, v, out)
    return out


def layer_kernel(tp, prompts, seq, head_dim, kv_heads, dims,
                 tokens, positions, lens, n_attn, n_mlp, q_gain, k_gain, freq, wq, wk, wv, wo, wg, wu, wdn,
                 ho, kc, vc,
                 n2, act, qs, os, kk, vt, kco, vco, cosb, sinb, ybuf, seen, tri, gains, gu, wd, pp, xp, land, ownh,
                 s_x, s_gu, s_wd, s_stage, s_xp, s_res, s_kv, s_own,
                 rs_send, rs_recv, ag_send, ag_recv, dd_send, dd_recv):
    hidden, width_q, width_f = dims
    chips = tp // CORES
    half = hidden // CORES
    unit = half // UNITS
    rows_b = seq // chips
    heads = width_q // head_dim
    q_tiles = width_q // TILE
    f_tiles = width_f // TILE
    odd = width_f % TILE != 0
    n_tiles = CORES * UNITS
    per_ar = HOPS * UNITS
    lead = UNITS + 1
    last = 2 * prompts - 1
    lanes = head_dim
    add_rows = rows_b // 4 if rows_b % 64 == 0 else 16
    o_bufs = 2 * (width_f // width_q)
    row_groups = min(6, seq // X_PARTS // 16)
    norm_tiles = n_tiles - 2
    norm_rows = seq // norm_tiles
    span_q = min(lanes, seq)
    hidden_score = -1e30 * head_dim ** 0.5
    to_exp2 = head_dim ** -0.5 * 1.4426950408889634

    me = lax.axis_index('tp')
    core = lax.rem(me, CORES)
    chip = me // CORES
    ring = lax.rem(chip + core * (chips - 2 * chip), chips)
    nxt = CORES * lax.rem(chip + chips + 1 - 2 * core, chips) + core
    prv = CORES * lax.rem(chip + chips - 1 + 2 * core, chips) + core
    partner = me + 1 - 2 * core
    kv_col = pl.multiple_of((me // (tp // kv_heads)) * head_dim, head_dim)

    def remote(src, dst, send, recv, to):
        return pltpu.make_async_remote_copy(src_ref=src, dst_ref=dst, send_sem=send, recv_sem=recv,
                                            device_id={'tp': to}, device_id_type=MESH)

    def local(src, dst, sem):
        return pltpu.make_async_copy(src, dst, sem)

    def await_copy(ref, sem):
        local(ref, ref, sem).wait()

    def wrap(b):
        return jnp.where(b < 0, b + chips, b)

    def block_rows(b):
        return pl.ds(pl.multiple_of(b * rows_b, rows_b), rows_b)

    def a_place(t):
        b = t % A_BUFS if isinstance(t, int) else lax.bitwise_and(t, A_BUFS - 1)
        return b, gu.at[b // 2, :, pl.ds(pl.multiple_of(lax.rem(b, 2) * TILE, TILE), TILE)]

    def a_tile(t):
        if isinstance(t, int) and t == 0:
            return (local(wk.at[:, pl.ds(kv_col, lanes)], gu.at[0, :, pl.ds(0, lanes)], s_gu.at[0, 0]),
                    local(wv.at[:, pl.ds(kv_col, lanes)], gu.at[0, :, pl.ds(lanes, lanes)], s_gu.at[0, 1]))
        b, place = a_place(t)
        return (local(wq.at[:, pl.ds(pl.multiple_of((t - 1) * TILE, TILE), TILE)], place, s_gu.at[b, 0]),)

    def f_pair(b, col, width):
        cols = pl.ds(pl.multiple_of(col, lanes), width)
        return (local(wg.at[:, cols], gu.at[b, :, pl.ds(0, width)], s_gu.at[b, 0]),
                local(wu.at[:, cols], gu.at[b, :, pl.ds(width, width)], s_gu.at[b, 1]))

    def f_tile(t):
        return f_pair(lax.rem(t, 2), t * TILE, TILE)

    def f_rest():
        return f_pair(f_tiles % 2, f_tiles * TILE, lanes)

    def start_all(copies):
        for cp in copies:
            cp.start()

    def wait_all(copies):
        for cp in copies:
            cp.wait()

    def out_cols(n):
        side = jnp.where(lax.rem(n, 2) == 0, 1 - core, core)
        return pl.ds(pl.multiple_of(side * half + lax.shift_right_logical(n, 1) * unit, unit), unit)

    def o_place(n):
        b = lax.rem(n, o_bufs)
        return wd.at[b // (o_bufs // 2), pl.ds(pl.multiple_of(lax.rem(b, o_bufs // 2) * width_q, width_q), width_q), :]

    def o_tile(n):
        return local(wo.at[:, out_cols(n)], o_place(n), s_wd.at[lax.rem(n, o_bufs)])

    def d_place(n):
        return wd.at[lax.rem(n, 2)]

    def d_tile(n):
        return local(wdn.at[:, out_cols(n)], d_place(n), s_wd.at[lax.rem(n, 2)])

    def load_rows(src, i):
        part = seq // X_PARTS
        return [local(src.at[pl.ds(pl.multiple_of(i * seq + b * part, part), part), :], n2.at[pl.ds(b * part, part), :], s_x.at[b])
                for b in range(X_PARTS)]

    start_all(load_rows(tokens, 0))
    for t in range(A_BUFS - 1):
        start_all(a_tile(t))
    barrier = pltpu.get_barrier_semaphore()
    for other in (nxt, prv, partner):
        pl.semaphore_signal(barrier, inc=1, device_id={'tp': other}, device_id_type=MESH)

    for v, gain in enumerate((n_attn, n_mlp)):
        wide = gain[...].astype(F32)
        for j in range(hidden // lanes):
            gains[v, :, j * lanes:(j + 1) * lanes] = jnp.broadcast_to(wide[None, j * lanes:(j + 1) * lanes], (16, lanes))
    key_at = lax.broadcasted_iota(jnp.int32, (span_q, span_q), 0)
    tri[...] = jnp.where(key_at <= lax.broadcasted_iota(jnp.int32, (span_q, span_q), 1), 1.0, 0.0)

    def ho_block(c, g, b, side):
        rows = pl.ds(pl.multiple_of(c * seq + b * rows_b, rows_b), rows_b)
        return ho.at[rows, pl.ds(pl.multiple_of(side * half + g * unit, unit), unit)]

    def send_partial(e, c, g):
        par = lax.bitwise_and(c, 1)
        u = par * UNITS + g
        rows = block_rows(wrap(ring - 1 - e))
        with jax.named_scope('w_rs'):
            if e == 0:
                await_copy(xp.at[u], s_xp.at[u])
            else:
                await_copy(land.at[par, g, e - 1], rs_recv.at[par, g, e - 1])
        mine, theirs, came = pp.at[u, rows], xp.at[u, rows], land.at[par, g, max(e - 1, 0)]

        def add(r, _):
            rr = pl.ds(pl.multiple_of(r * add_rows, 16), add_rows)
            total = mine[rr, :].astype(F32) + theirs[rr, :].astype(F32)
            if e > 0:
                total = total + came[rr, :].astype(F32)
            mine[rr, :] = total.astype(BF)
            return 0
        lax.fori_loop(0, rows_b // add_rows, add, 0)
        remote(mine, land.at[par, g, e], rs_send.at[par, g, e], rs_recv.at[par, g, e], nxt).start()

    def finish_sum(c, g):
        par = lax.bitwise_and(c, 1)
        u, w = par * UNITS + g, jnp.where(c < prompts, c, c - prompts) * UNITS + g
        rows = block_rows(ring)
        with jax.named_scope('w_rs3'):
            await_copy(land.at[par, g, 2], rs_recv.at[par, g, 2])

        @pl.when(c < prompts)
        def _():
            await_copy(ownh.at[w], s_res.at[w])
        mine, theirs, came, own = pp.at[u, rows], xp.at[u, rows], land.at[par, g, 2], ownh.at[w]

        def add(r, _):
            rr = pl.ds(pl.multiple_of(r * add_rows, 16), add_rows)
            total = came[rr, :].astype(F32) + (mine[rr, :].astype(F32) + theirs[rr, :].astype(F32))
            own[rr, :] = (own[rr, :].astype(F32) + total).astype(BF)
            return 0
        lax.fori_loop(0, rows_b // add_rows, add, 0)
        place = ho_block(c, g, ring, core)
        remote(own, place, ag_send.at[par, g, 0], ag_recv.at[par, g, 0], nxt).start()
        remote(own, place, dd_send.at[par, g, 0], dd_recv.at[par, g, 0], partner).start()
        local(own, place, s_own.at[par, g]).start()

    def pass_on(e, c, g):
        par = lax.bitwise_and(c, 1)
        place = ho_block(c, g, wrap(ring - e), core)
        with jax.named_scope('w_ag'):
            await_copy(place, ag_recv.at[par, g, e - 1])
        if e < 3:
            remote(place, place, ag_send.at[par, g, e], ag_recv.at[par, g, e], nxt).start()
        remote(place, place, dd_send.at[par, g, e], dd_recv.at[par, g, e], partner).start()
        if e == 1:
            await_copy(place, dd_recv.at[par, g, 0])
            for s in range(3):
                await_copy(land.at[par, g, s], rs_send.at[par, g, s])

    def settle(c, g):
        par = lax.bitwise_and(c, 1)
        place = ho_block(c, g, ring, core)
        await_copy(land.at[par, g, 0], s_own.at[par, g])
        for e in range(3):
            await_copy(place, ag_send.at[par, g, e])
        for e in range(4):
            await_copy(place, dd_send.at[par, g, e])
        for e in range(1, 4):
            await_copy(place, dd_recv.at[par, g, e])

    def slot(k):
        c = jnp.minimum(over(k, per_ar), last)
        diagonal = c == last
        d, q = split(k - c * per_ar, UNITS)
        g_d = jnp.minimum(d, UNITS - 1) - q
        e_d = jnp.where(g_d >= 0, d - g_d, HOPS)
        e = jnp.where(diagonal, e_d, d)
        g = jnp.where(diagonal, jnp.maximum(g_d, 0), q)
        @pl.when(e < 3)
        def _():
            for s in range(3):
                @pl.when(e == s)
                def _(s=s):
                    send_partial(s, c, g)
                    if s == 0:
                        @pl.when(c > 0)
                        def _():
                            pass_on(3, c - 1, g)

                            @pl.when((g > 0) & jnp.logical_not(diagonal))
                            def _():
                                settle(c - 1, g - 1)
                    if s == 1:
                        @pl.when((c > 0) & (diagonal | (g == 0)))
                        def _():
                            settle(c - 1, jnp.where(diagonal, g, UNITS - 1))

        @pl.when(e >= 3)
        def _():
            @pl.when(e == 3)
            def _():
                finish_sum(c, g)
            for s in range(2):
                @pl.when(e == 4 + s)
                def _(s=s):
                    pass_on(s + 1, c, g)

    def run_slots(lo, hi):
        def body(k, _):
            slot(k)
            return 0
        lax.fori_loop(lo, hi, body, 0)

    def norm_all(v):
        part = seq // X_PARTS
        for b in range(X_PARTS):
            await_copy(n2.at[pl.ds(b * part, part), :], s_x.at[b])

            def scales(r, _):
                for q in range(row_groups):
                    rr = pl.ds(pl.multiple_of(b * part + (r * row_groups + q) * 16, 16), 16)
                    acc = jnp.zeros((16, lanes), F32)
                    for j in range(hidden // lanes):
                        x = n2[rr, j * lanes:(j + 1) * lanes].astype(F32)
                        acc = acc + x * x
                    scale = lax.rsqrt(jnp.sum(acc, axis=-1, keepdims=True) * (1.0 / hidden) + EPSILON)
                    ybuf[0, rr, :lanes] = jnp.broadcast_to(scale, (16, lanes))
                return 0
            lax.fori_loop(0, part // 16 // row_groups, scales, 0)

        def apply(r, _):
            rr = pl.ds(pl.multiple_of(r * 16, 16), 16)
            scale = ybuf[0, rr, :lanes]
            for j in range(hidden // lanes):
                cols = slice(j * lanes, (j + 1) * lanes)
                n2[rr, cols] = (n2[rr, cols].astype(F32) * scale * gains[v, :, cols]).astype(BF)
            return 0
        lax.fori_loop(0, seq // 16, apply, 0)

    def norm_some(v, first):
        for q in range(norm_rows // 16):
            rr = pl.ds(pl.multiple_of(first + q * 16, 16), 16)
            acc = jnp.zeros((16, lanes), F32)
            for j in range(hidden // lanes):
                x = n2[rr, j * lanes:(j + 1) * lanes].astype(F32)
                acc = acc + x * x
            scale = jnp.broadcast_to(lax.rsqrt(jnp.sum(acc, axis=-1, keepdims=True) * (1.0 / hidden) + EPSILON), (16, lanes))
            for j in range(hidden // lanes):
                cols = slice(j * lanes, (j + 1) * lanes)
                n2[rr, cols] = (n2[rr, cols].astype(F32) * scale * gains[v, :, cols]).astype(BF)

    def project(lhs, fetch, place, ahead, c, v, bounds, begin, loaded):
        par = lax.bitwise_and(c, 1)

        def tile(n, norm):
            @pl.when(n + ahead < n_tiles)
            def _():
                fetch(n + ahead).start()
            with jax.named_scope('w_wd'):
                fetch(n).wait()
            g = n // 2
            away = lax.rem(n, 2) == 0
            count = c * UNITS + g
            stage = lax.rem(count, 2)
            u = jnp.where(away, 2 * UNITS + stage, par * UNITS + g)

            @pl.when(away & (count >= 2))
            def _():
                await_copy(pp.at[u], s_stage.at[stage])
            if norm:
                norm_some(v, pl.multiple_of((n - 2) * norm_rows, 16))
            pp[u] = dot(lhs[...], place(n)[...]).astype(BF)

            @pl.when(away)
            def _():
                to = par * UNITS + g
                remote(pp.at[u], xp.at[to], s_stage.at[stage], s_xp.at[to], partner).start()
            run_slots(*bounds(n))

        def plain(n, _):
            tile(n, False)
            return 0

        def normed(n, _):
            tile(n, True)
            return 0
        lax.fori_loop(0, 1, plain, 0)
        begin()
        lax.fori_loop(1, 2, plain, 0)
        loaded()
        lax.fori_loop(2, n_tiles, normed, 0)

    def turned(v, gain):
        v = v * lax.rsqrt(jnp.mean(v * v, axis=-1, keepdims=True) + EPSILON) * gain[...].astype(F32)[None]
        return v * cosb[...] + pltpu.roll(v, lanes // 2, 1) * sinb[...]

    def rope_rows(i):
        where = jnp.broadcast_to(positions[pl.ds(i, 1), :].astype(F32), (lanes, seq)).T * freq[...]
        sine = jnp.sin(where)
        cosb[...] = jnp.cos(where)
        sinb[...] = jnp.where(lax.broadcasted_iota(jnp.int32, (seq, lanes), 1) < lanes // 2, -sine, sine)

    def keep_kv(y, length):
        k_rot = turned(y[:, :lanes], k_gain)
        v_val = y[:, lanes:]
        kk[...] = k_rot.astype(BF)
        vt[...] = v_val.T.astype(BF)
        valid = lax.broadcasted_iota(jnp.int32, (seq, lanes), 0) < length
        seen[...] = jnp.where(valid, 1.0, 0.0)
        kco[...] = jnp.where(valid, k_rot, 0.0).astype(BF)
        vco[...] = jnp.where(valid, v_val, 0.0).astype(BF)

    def keep_q(t, y):
        for s in range(TILE // lanes):
            qs[:, pl.ds(pl.multiple_of(t * TILE + s * lanes, lanes), lanes)] = turned(y[:, s * lanes:(s + 1) * lanes], q_gain).astype(BF)

    def attend(hd):
        cols = pl.ds(pl.multiple_of(hd * lanes, lanes), lanes)
        for lo in range(0, seq, span_q):
            hi = lo + span_q
            q = qs[lo:hi, cols]
            s = dot_nt(kk[:hi, :], q)
            parts = [jnp.where((seen[lo:hi, :span_q] > 0.0) & (tri[...] > 0.0), s[lo:hi, :], hidden_score)]
            for r in range(0, lo, span_q):
                parts.append(jnp.where(seen[r:r + span_q, :span_q] > 0.0, s[r:r + span_q, :], hidden_score))
            top = parts[0].max(0, keepdims=True)
            for x in parts[1:]:
                top = jnp.maximum(top, x.max(0, keepdims=True))
            parts = [jnp.exp2((x - top) * to_exp2) for x in parts]
            total = parts[0].sum(0, keepdims=True)
            for x in parts[1:]:
                total = total + x.sum(0, keepdims=True)
            scale = 1.0 / total
            probs = [(x * scale).astype(BF) for x in parts[1:] + parts[:1]]
            probs = jnp.concatenate(probs, axis=0) if len(probs) > 1 else probs[0]
            os[lo:hi, cols] = dot(vt[:, :hi], probs).T.astype(BF)

    step_a = (per_ar + lead - UNITS + 1) // (prompts - 1)
    w_q, w_h, w_o = 4, 7, 2
    weight_a = w_q * (q_tiles + 1) + w_h * (heads // HEADS_AT_ONCE) + w_o * n_tiles

    with jax.named_scope('norm_x'):
        norm_all(0)
    pl.semaphore_wait(barrier, 3)
    for n in range(o_bufs - 1):
        o_tile(n).start()
    for i in range(prompts):
        for g in range(UNITS):
            rows = pl.ds(pl.multiple_of(i * seq + ring * rows_b, rows_b), rows_b)
            cols = pl.ds(pl.multiple_of(core * half + g * unit, unit), unit)
            local(tokens.at[rows, cols], ownh.at[i * UNITS + g], s_res.at[i * UNITS + g]).start()

    def attention_phase(i, _):
        def upto(w):
            return jnp.where(i == 0, 0, UNITS - 1 + (i - 1) * step_a + over(w * step_a, weight_a))
        length = lens[i]
        def kv_body(t, _):
            start_all(a_tile(A_BUFS - 1))
            with jax.named_scope('qkv'):
                wait_all(a_tile(0))
                rope_rows(i)
                ybuf[0] = dot(n2[...], a_place(0)[1][...])
            return 0
        lax.fori_loop(i, i + 1, kv_body, 0)

        def q0_body(t, _):
            start_all(a_tile(A_BUFS))
            with jax.named_scope('qkv'):
                wait_all(a_tile(1))
                keep_kv(ybuf[0], length)
                ybuf[1] = dot(n2[...], a_place(1)[1][...])
            return 0
        lax.fori_loop(i, i + 1, q0_body, 0)
        run_slots(upto(0), upto(2 * w_q))

        def q_body(t, _):
            with jax.named_scope('qkv'):
                wait_all(a_tile(t))
                keep_q(t - 2, ybuf[lax.rem(t - 1, 2)])
                ybuf[lax.rem(t, 2)] = dot(n2[...], a_place(t)[1][...])
            run_slots(upto(t * w_q), upto((t + 1) * w_q))
            return 0
        lax.fori_loop(2, q_tiles + 1, q_body, 0)

        @pl.when(i + 1 < prompts)
        def _():
            start_all(load_rows(tokens, i + 1))
            for t in range(A_BUFS - 1):
                start_all(a_tile(t))

        @pl.when(i + 1 == prompts)
        def _():
            start_all(f_tile(0))
        rows = pl.ds(pl.multiple_of(i * seq, seq), seq)
        caches = (local(kco, kc.at[rows, :], s_kv.at[0]), local(vco, vc.at[rows, :], s_kv.at[1]))
        start_all(caches)
        with jax.named_scope('keep_q'):
            keep_q(q_tiles - 1, ybuf[q_tiles % 2])
        base1 = (q_tiles + 1) * w_q

        def heads_body(t, _):
            with jax.named_scope('attend'):
                for hd in range(HEADS_AT_ONCE):
                    attend(t * HEADS_AT_ONCE + hd)
            run_slots(upto(base1 + t * w_h), upto(base1 + (t + 1) * w_h))
            return 0
        lax.fori_loop(0, heads // HEADS_AT_ONCE, heads_body, 0)
        base = base1 + heads // HEADS_AT_ONCE * w_h
        wait_all(caches)

        def bounds(n):
            early = lax.shift_right_logical(jnp.maximum(n - 2, 0), 1), lax.shift_right_logical(jnp.maximum(n - 1, 0), 1)
            return (jnp.where(i == 0, early[0], upto(base + n * w_o)),
                    jnp.where(i == 0, early[1], upto(base + (n + 1) * w_o)))

        def loaded():
            @pl.when(i + 1 < prompts)
            def _():
                wait_all(load_rows(tokens, i + 1))
        with jax.named_scope('project_o'):
            project(os, o_tile, o_place, o_bufs - 1, i, 0, bounds, lambda: None, loaded)

        @pl.when(i + 1 < prompts)
        def _():
            for n in range(o_bufs - 1):
                o_tile(n).start()

        @pl.when(i + 1 == prompts)
        def _():
            d_tile(0).start()
        return 0
    lax.fori_loop(0, prompts, attention_phase, 0)

    a_end = UNITS - 1 + (prompts - 1) * step_a
    with jax.named_scope('pre_mlp'):
        run_slots(a_end, per_ar + lead)
    start_all(load_rows(ho, 0))
    with jax.named_scope('norm_h'):
        norm_all(1)
    starts = [(m + 1) * per_ar + v for m, v in zip(range(prompts), (lead, 18, 32))]
    mids = [(m + 2) * per_ar + v for m, v in zip(range(prompts), (3, 15, 30))]
    ones = [max((m + 2) * per_ar + lead, mids[m] + 2) if m + 1 < prompts else mids[m] for m in range(prompts)]
    ends = starts[1:] + [last * per_ar + UNITS * UNITS]

    soon = [0, 0, 1]
    for g in range(1, UNITS):
        soon += [g * UNITS, g * UNITS + (g + 2) // 2]
    soon = soon[:n_tiles] + [UNITS * UNITS]

    def mlp_phase(i, _):
        k0, k1, kt, k2 = pick(i, starts), pick(i, mids), pick(i, ones), pick(i, ends)

        def gated(y, width):
            gate, up = y[:, :width], y[:, width:]
            return (gate * jax.nn.sigmoid(gate) * up).astype(BF)

        def f_body(t, _):
            @pl.when(t + 1 < f_tiles)
            def _():
                start_all(f_tile(t + 1))
            if odd:
                @pl.when(t + 1 == f_tiles)
                def _():
                    start_all(f_rest())
            with jax.named_scope('w_gu'):
                wait_all(f_tile(t))
            act[:, pl.ds(pl.multiple_of(t * TILE, TILE), TILE)] = gated(dot(n2[...], gu[lax.rem(t, 2)]), TILE)
            run_slots(k0 + over(t * (k1 - k0), f_tiles), k0 + over((t + 1) * (k1 - k0), f_tiles))
            return 0
        with jax.named_scope('f_loop'):
            lax.fori_loop(0, f_tiles, f_body, 0)
        if odd:
            def rest_body(t, _):
                with jax.named_scope('f_rest'):
                    wait_all(f_rest())
                    act[:, f_tiles * TILE:] = gated(dot(n2[...], gu[f_tiles % 2, :, :TILE]), lanes)
                return 0
            lax.fori_loop(i, i + 1, rest_body, 0)

        @pl.when(i + 1 < prompts)
        def _():
            start_all(f_tile(0))

        def upto(n):
            spread = jnp.where(n <= 1, k1 + n * (kt - k1), kt + over(jnp.maximum(n - 1, 0) * (k2 - kt), n_tiles - 1))
            return jnp.where(i == prompts - 1, k1 + pick(n, soon), spread)

        def begin():
            @pl.when(i + 1 < prompts)
            def _():
                start_all(load_rows(ho, i + 1))

        def loaded():
            @pl.when(i + 1 < prompts)
            def _():
                wait_all(load_rows(ho, i + 1))
        with jax.named_scope('project_d'):
            project(act, d_tile, d_place, 1, prompts + i, 1, lambda n: (upto(n), upto(n + 1)), begin, loaded)

        @pl.when(i + 1 < prompts)
        def _():
            d_tile(0).start()
        return 0
    lax.fori_loop(0, prompts, mlp_phase, 0)

    with jax.named_scope('tail'):
        run_slots(last * per_ar + UNITS * UNITS, last * per_ar + (UNITS + HOPS - 1) * UNITS)

        def ring_end(g, _):
            pass_on(3, last, g)
            return 0
        lax.fori_loop(0, UNITS, ring_end, 0)

        def all_end(g, _):
            settle(last, g)
            return 0
        lax.fori_loop(0, UNITS, all_end, 0)
        for s in range(2):
            await_copy(pp.at[2 * UNITS + s], s_stage.at[s])


def copy_kernel(first, a, b, c, a_out, b_out, c_out, a_buf, b_buf, c_buf, s_in, s_out):
    pieces, rows = a_buf.shape[0], a_buf.shape[1]
    moves = [(a.at[pl.ds(first + p * rows, rows), :], a_buf.at[p], a_out.at[pl.ds(p * rows, rows), :]) for p in range(pieces)]
    moves += [(b, b_buf, b_out), (c, c_buf, c_out)]
    for m, (src, buf, _) in enumerate(moves):
        pltpu.make_async_copy(src, buf, s_in.at[m]).start()
    for m, (src, buf, dst) in enumerate(moves):
        pltpu.make_async_copy(src, buf, s_in.at[m]).wait()
        pltpu.make_async_copy(buf, dst, s_out.at[m]).start()
    for m, (_, buf, dst) in enumerate(moves):
        pltpu.make_async_copy(buf, dst, s_out.at[m]).wait()


def layer_body(tokens, positions, lengths, norm_attn, norm_mlp, q_gain, k_gain, w_query, w_key, w_value, w_out, w_gate, w_up, w_down, tp_size):
    prompts, seq, hidden = tokens.shape
    head_dim = q_gain.shape[0]
    width_q, width_f = w_query.shape[1], w_gate.shape[1]
    kv_heads = w_key.shape[1] // head_dim
    chips = tp_size // CORES
    unit = hidden // CORES // UNITS
    rows_n = prompts * seq
    inv_freq = ROPE_THETA ** (-np.arange(head_dim // 2) / (head_dim // 2))
    freq = jnp.asarray(np.concatenate([inv_freq, inv_freq])[None], F32)
    any_spec = pl.BlockSpec(memory_space=pl.ANY)
    vmem = pl.BlockSpec(memory_space=pltpu.VMEM)
    smem = pl.BlockSpec(memory_space=pltpu.SMEM)
    kernel = functools.partial(layer_kernel, tp_size, prompts, seq, head_dim, kv_heads, (hidden, width_q, width_f))
    dma = pltpu.SemaphoreType.DMA
    o_bufs = 2 * (width_f // width_q)
    span_q = min(head_dim, seq)
    ho, kc, vc = pl.pallas_call(
        kernel,
        name='decoder_layer',
        out_shape=(jax.ShapeDtypeStruct((2 * rows_n, hidden), BF),
                   jax.ShapeDtypeStruct((rows_n, head_dim), BF),
                   jax.ShapeDtypeStruct((rows_n, head_dim), BF)),
        in_specs=[any_spec, vmem, smem, vmem, vmem, vmem, vmem, vmem] + [any_spec] * 7,
        out_specs=(any_spec, any_spec, any_spec),
        scratch_shapes=[
            pltpu.VMEM((seq, hidden), BF),
            pltpu.VMEM((seq, width_f), BF),
            pltpu.VMEM((seq, width_q), BF), pltpu.VMEM((seq, width_q), BF),
            pltpu.VMEM((seq, head_dim), BF), pltpu.VMEM((head_dim, seq), BF),
            pltpu.VMEM((seq, head_dim), BF), pltpu.VMEM((seq, head_dim), BF),
            pltpu.VMEM((seq, head_dim), F32), pltpu.VMEM((seq, head_dim), F32),
            pltpu.VMEM((2, seq, TILE), F32),
            pltpu.VMEM((seq, head_dim), F32),
            pltpu.VMEM((span_q, span_q), F32),
            pltpu.VMEM((2, 16, hidden), F32),
            pltpu.VMEM((2, hidden, 2 * TILE), BF),
            pltpu.VMEM((2, width_f, unit), BF),
            pltpu.VMEM((2 * UNITS + 2, seq, unit), BF),
            pltpu.VMEM((2 * UNITS, seq, unit), BF),
            pltpu.VMEM((2, UNITS, 3, seq // chips, unit), BF),
            pltpu.VMEM((prompts * UNITS, seq // chips, unit), BF),
            dma((X_PARTS,)), dma((A_BUFS, 2)), dma((o_bufs,)), dma((2,)), dma((2 * UNITS,)), dma((prompts * UNITS,)), dma((2,)), dma((2, UNITS)),
            dma((2, UNITS, 3)), dma((2, UNITS, 3)), dma((2, UNITS, 3)), dma((2, UNITS, 3)), dma((2, UNITS, 4)), dma((2, UNITS, 4)),
        ],
        compiler_params=pltpu.CompilerParams(collective_id=0, has_side_effects=True, vmem_limit_bytes=67043328),
    )(tokens.reshape(rows_n, hidden), positions, lengths, norm_attn, norm_mlp, q_gain, k_gain, freq,
      w_query, w_key, w_value, w_out, w_gate, w_up, w_down)
    shape = (prompts, seq, 1, head_dim)
    parts = 4 * prompts
    block = rows_n // parts
    out, kc, vc = pl.pallas_call(
        functools.partial(copy_kernel, rows_n),
        name='copy_out',
        out_shape=(jax.ShapeDtypeStruct((rows_n, hidden), BF), jax.ShapeDtypeStruct(kc.shape, BF), jax.ShapeDtypeStruct(vc.shape, BF)),
        in_specs=[any_spec] * 3,
        out_specs=[any_spec] * 3,
        scratch_shapes=[pltpu.VMEM((parts, block, hidden), BF), pltpu.VMEM(kc.shape, BF), pltpu.VMEM(vc.shape, BF), dma((parts + 2,)), dma((parts + 2,))],
        compiler_params=pltpu.CompilerParams(vmem_limit_bytes=60 * 1024 * 1024),
    )(ho, kc, vc)
    return out.reshape(prompts, seq, hidden), kc.reshape(shape), vc.reshape(shape)


def solution(mesh):
    body = functools.partial(layer_body, tp_size=mesh.shape['tp'])
    in_specs = (P('dp', None, None), P('dp', None), P('dp'), P(), P(), P(), P(), P(None, 'tp'), P(), P(), P('tp', None), P(None, 'tp'), P(None, 'tp'), P('tp', None))
    out_specs = (P('dp', None, None), P('dp', None, 'tp', None), P('dp', None, 'tp', None))
    return jax.shard_map(body, mesh=mesh, in_specs=in_specs, out_specs=out_specs, check_vma=False)
```

```python
import functools
import jax
import jax.numpy as jnp
import numpy as np
from jax import lax
from jax.experimental import pallas as pl
from jax.experimental.pallas import tpu as pltpu
from jax.sharding import PartitionSpec as P

EPSILON = 1e-6
ROPE_THETA = 1000000.0
MESH = pl.DeviceIdType.MESH
CORES = 2
TILE = 256
UNITS = 5
HOPS = 6
A_BUFS = 4
X_PARTS = 4
HEADS_AT_ONCE = 4
BF = jnp.bfloat16
F32 = jnp.float32


def dot(a, b):
    return jnp.dot(a, b, preferred_element_type=F32)


def dot_nt(a, b):
    return lax.dot_general(a, b, (((1,), (1,)), ((), ())), preferred_element_type=F32)


def over(x, n):
    return lax.shift_right_logical(x * (65536 // n + 1), 16)


def split(x, n):
    q = over(x, n)
    return q, x - q * n


def pick(i, values):
    out = values[0]
    for n, v in enumerate(values[1:], 1):
        out = jnp.where(i >= n, v, out)
    return out


def layer_kernel(tp, prompts, seq, head_dim, kv_heads, dims,
                 tokens, positions, lens, n_attn, n_mlp, q_gain, k_gain, freq, wq, wk, wv, wo, wg, wu, wdn,
                 ho, kc, vc,
                 n2, act, qs, os, kk, vt, kco, vco, cosb, sinb, ybuf, seen, tri, gains, gu, wd, pp, xp, land, ownh,
                 s_x, s_gu, s_wd, s_stage, s_xp, s_res, s_kv, s_own,
                 rs_send, rs_recv, ag_send, ag_recv, dd_send, dd_recv):
    hidden, width_q, width_f = dims
    chips = tp // CORES
    half = hidden // CORES
    unit = half // UNITS
    rows_b = seq // chips
    heads = width_q // head_dim
    q_tiles = width_q // TILE
    f_tiles = width_f // TILE
    odd = width_f % TILE != 0
    n_tiles = CORES * UNITS
    per_ar = HOPS * UNITS
    lead = UNITS + 1
    last = 2 * prompts - 1
    lanes = head_dim
    add_rows = rows_b // 4 if rows_b % 64 == 0 else 16
    o_bufs = 2 * (width_f // width_q)
    row_groups = min(6, seq // X_PARTS // 16)
    norm_tiles = n_tiles - 2
    norm_rows = seq // norm_tiles
    span_q = min(lanes, seq)
    hidden_score = -1e30 * head_dim ** 0.5
    to_exp2 = head_dim ** -0.5 * 1.4426950408889634

    me = lax.axis_index('tp')
    core = lax.rem(me, CORES)
    chip = me // CORES
    ring = lax.rem(chip + core * (chips - 2 * chip), chips)
    nxt = CORES * lax.rem(chip + chips + 1 - 2 * core, chips) + core
    prv = CORES * lax.rem(chip + chips - 1 + 2 * core, chips) + core
    partner = me + 1 - 2 * core
    kv_col = pl.multiple_of((me // (tp // kv_heads)) * head_dim, head_dim)

    def remote(src, dst, send, recv, to):
        return pltpu.make_async_remote_copy(src_ref=src, dst_ref=dst, send_sem=send, recv_sem=recv,
                                            device_id={'tp': to}, device_id_type=MESH)

    def local(src, dst, sem):
        return pltpu.make_async_copy(src, dst, sem)

    def await_copy(ref, sem):
        local(ref, ref, sem).wait()

    def wrap(b):
        return jnp.where(b < 0, b + chips, b)

    def block_rows(b):
        return pl.ds(pl.multiple_of(b * rows_b, rows_b), rows_b)

    def a_place(t):
        b = t % A_BUFS if isinstance(t, int) else lax.bitwise_and(t, A_BUFS - 1)
        return b, gu.at[b // 2, :, pl.ds(pl.multiple_of(lax.rem(b, 2) * TILE, TILE), TILE)]

    def a_tile(t):
        if isinstance(t, int) and t == 0:
            return (local(wk.at[:, pl.ds(kv_col, lanes)], gu.at[0, :, pl.ds(0, lanes)], s_gu.at[0, 0]),
                    local(wv.at[:, pl.ds(kv_col, lanes)], gu.at[0, :, pl.ds(lanes, lanes)], s_gu.at[0, 1]))
        b, place = a_place(t)
        return (local(wq.at[:, pl.ds(pl.multiple_of((t - 1) * TILE, TILE), TILE)], place, s_gu.at[b, 0]),)

    def f_pair(b, col, width):
        cols = pl.ds(pl.multiple_of(col, lanes), width)
        return (local(wg.at[:, cols], gu.at[b, :, pl.ds(0, width)], s_gu.at[b, 0]),
                local(wu.at[:, cols], gu.at[b, :, pl.ds(width, width)], s_gu.at[b, 1]))

    def f_tile(t):
        return f_pair(lax.rem(t, 2), t * TILE, TILE)

    def f_rest():
        return f_pair(f_tiles % 2, f_tiles * TILE, lanes)

    def start_all(copies):
        for cp in copies:
            cp.start()

    def wait_all(copies):
        for cp in copies:
            cp.wait()

    def out_cols(n):
        side = jnp.where(lax.rem(n, 2) == 0, 1 - core, core)
        return pl.ds(pl.multiple_of(side * half + lax.shift_right_logical(n, 1) * unit, unit), unit)

    def o_place(n):
        b = lax.rem(n, o_bufs)
        return wd.at[b // (o_bufs // 2), pl.ds(pl.multiple_of(lax.rem(b, o_bufs // 2) * width_q, width_q), width_q), :]

    def o_tile(n):
        return local(wo.at[:, out_cols(n)], o_place(n), s_wd.at[lax.rem(n, o_bufs)])

    def d_place(n):
        return wd.at[lax.rem(n, 2)]

    def d_tile(n):
        return local(wdn.at[:, out_cols(n)], d_place(n), s_wd.at[lax.rem(n, 2)])

    def load_rows(src, i):
        part = seq // X_PARTS
        return [local(src.at[pl.ds(pl.multiple_of(i * seq + b * part, part), part), :], n2.at[pl.ds(b * part, part), :], s_x.at[b])
                for b in range(X_PARTS)]

    start_all(load_rows(tokens, 0))
    for t in range(A_BUFS - 1):
        start_all(a_tile(t))
    barrier = pltpu.get_barrier_semaphore()
    for other in (nxt, prv, partner):
        pl.semaphore_signal(barrier, inc=1, device_id={'tp': other}, device_id_type=MESH)

    for v, gain in enumerate((n_attn, n_mlp)):
        wide = gain[...].astype(F32)
        for j in range(hidden // lanes):
            gains[v, :, j * lanes:(j + 1) * lanes] = jnp.broadcast_to(wide[None, j * lanes:(j + 1) * lanes], (16, lanes))
    key_at = lax.broadcasted_iota(jnp.int32, (span_q, span_q), 0)
    tri[...] = jnp.where(key_at <= lax.broadcasted_iota(jnp.int32, (span_q, span_q), 1), 1.0, 0.0)

    def ho_block(c, g, b, side):
        rows = pl.ds(pl.multiple_of(c * seq + b * rows_b, rows_b), rows_b)
        return ho.at[rows, pl.ds(pl.multiple_of(side * half + g * unit, unit), unit)]

    def send_partial(e, c, g):
        par = lax.bitwise_and(c, 1)
        u = par * UNITS + g
        rows = block_rows(wrap(ring - 1 - e))
        with jax.named_scope('w_rs'):
            if e == 0:
                await_copy(xp.at[u], s_xp.at[u])
            else:
                await_copy(land.at[par, g, e - 1], rs_recv.at[par, g, e - 1])
        mine, theirs, came = pp.at[u, rows], xp.at[u, rows], land.at[par, g, max(e - 1, 0)]

        def add(r, _):
            rr = pl.ds(pl.multiple_of(r * add_rows, 16), add_rows)
            total = mine[rr, :].astype(F32) + theirs[rr, :].astype(F32)
            if e > 0:
                total = total + came[rr, :].astype(F32)
            mine[rr, :] = total.astype(BF)
            return 0
        lax.fori_loop(0, rows_b // add_rows, add, 0)
        remote(mine, land.at[par, g, e], rs_send.at[par, g, e], rs_recv.at[par, g, e], nxt).start()

    def finish_sum(c, g):
        par = lax.bitwise_and(c, 1)
        u, w = par * UNITS + g, jnp.where(c < prompts, c, c - prompts) * UNITS + g
        rows = block_rows(ring)
        with jax.named_scope('w_rs3'):
            await_copy(land.at[par, g, 2], rs_recv.at[par, g, 2])

        @pl.when(c < prompts)
        def _():
            await_copy(ownh.at[w], s_res.at[w])
        mine, theirs, came, own = pp.at[u, rows], xp.at[u, rows], land.at[par, g, 2], ownh.at[w]

        def add(r, _):
            rr = pl.ds(pl.multiple_of(r * add_rows, 16), add_rows)
            total = came[rr, :].astype(F32) + (mine[rr, :].astype(F32) + theirs[rr, :].astype(F32))
            own[rr, :] = (own[rr, :].astype(F32) + total).astype(BF)
            return 0
        lax.fori_loop(0, rows_b // add_rows, add, 0)
        place = ho_block(c, g, ring, core)
        remote(own, place, ag_send.at[par, g, 0], ag_recv.at[par, g, 0], nxt).start()
        remote(own, place, dd_send.at[par, g, 0], dd_recv.at[par, g, 0], partner).start()
        local(own, place, s_own.at[par, g]).start()

    def pass_on(e, c, g):
        par = lax.bitwise_and(c, 1)
        place = ho_block(c, g, wrap(ring - e), core)
        with jax.named_scope('w_ag'):
            await_copy(place, ag_recv.at[par, g, e - 1])
        if e < 3:
            remote(place, place, ag_send.at[par, g, e], ag_recv.at[par, g, e], nxt).start()
        remote(place, place, dd_send.at[par, g, e], dd_recv.at[par, g, e], partner).start()
        if e == 1:
            await_copy(place, dd_recv.at[par, g, 0])
            for s in range(3):
                await_copy(land.at[par, g, s], rs_send.at[par, g, s])

    def settle(c, g):
        par = lax.bitwise_and(c, 1)
        place = ho_block(c, g, ring, core)
        await_copy(land.at[par, g, 0], s_own.at[par, g])
        for e in range(3):
            await_copy(place, ag_send.at[par, g, e])
        for e in range(4):
            await_copy(place, dd_send.at[par, g, e])
        for e in range(1, 4):
            await_copy(place, dd_recv.at[par, g, e])

    def slot(k):
        c = jnp.minimum(over(k, per_ar), last)
        diagonal = c == last
        d, q = split(k - c * per_ar, UNITS)
        g_d = jnp.minimum(d, UNITS - 1) - q
        e_d = jnp.where(g_d >= 0, d - g_d, HOPS)
        e = jnp.where(diagonal, e_d, d)
        g = jnp.where(diagonal, jnp.maximum(g_d, 0), q)
        @pl.when(e < 3)
        def _():
            for s in range(3):
                @pl.when(e == s)
                def _(s=s):
                    send_partial(s, c, g)
                    if s == 0:
                        @pl.when(c > 0)
                        def _():
                            pass_on(3, c - 1, g)

                            @pl.when((g > 0) & jnp.logical_not(diagonal))
                            def _():
                                settle(c - 1, g - 1)
                    if s == 1:
                        @pl.when((c > 0) & (diagonal | (g == 0)))
                        def _():
                            settle(c - 1, jnp.where(diagonal, g, UNITS - 1))

        @pl.when(e >= 3)
        def _():
            @pl.when(e == 3)
            def _():
                finish_sum(c, g)
            for s in range(2):
                @pl.when(e == 4 + s)
                def _(s=s):
                    pass_on(s + 1, c, g)

    def run_slots(lo, hi):
        def body(k, _):
            slot(k)
            return 0
        lax.fori_loop(lo, hi, body, 0)

    def norm_all(v):
        part = seq // X_PARTS
        for b in range(X_PARTS):
            await_copy(n2.at[pl.ds(b * part, part), :], s_x.at[b])

            def scales(r, _):
                for q in range(row_groups):
                    rr = pl.ds(pl.multiple_of(b * part + (r * row_groups + q) * 16, 16), 16)
                    acc = jnp.zeros((16, lanes), F32)
                    for j in range(hidden // lanes):
                        x = n2[rr, j * lanes:(j + 1) * lanes].astype(F32)
                        acc = acc + x * x
                    scale = lax.rsqrt(jnp.sum(acc, axis=-1, keepdims=True) * (1.0 / hidden) + EPSILON)
                    ybuf[0, rr, :lanes] = jnp.broadcast_to(scale, (16, lanes))
                return 0
            lax.fori_loop(0, part // 16 // row_groups, scales, 0)

        def apply(r, _):
            rr = pl.ds(pl.multiple_of(r * 16, 16), 16)
            scale = ybuf[0, rr, :lanes]
            for j in range(hidden // lanes):
                cols = slice(j * lanes, (j + 1) * lanes)
                n2[rr, cols] = (n2[rr, cols].astype(F32) * scale * gains[v, :, cols]).astype(BF)
            return 0
        lax.fori_loop(0, seq // 16, apply, 0)

    def norm_some(v, first):
        for q in range(norm_rows // 16):
            rr = pl.ds(pl.multiple_of(first + q * 16, 16), 16)
            acc = jnp.zeros((16, lanes), F32)
            for j in range(hidden // lanes):
                x = n2[rr, j * lanes:(j + 1) * lanes].astype(F32)
                acc = acc + x * x
            scale = jnp.broadcast_to(lax.rsqrt(jnp.sum(acc, axis=-1, keepdims=True) * (1.0 / hidden) + EPSILON), (16, lanes))
            for j in range(hidden // lanes):
                cols = slice(j * lanes, (j + 1) * lanes)
                n2[rr, cols] = (n2[rr, cols].astype(F32) * scale * gains[v, :, cols]).astype(BF)

    def project(lhs, fetch, place, ahead, c, v, bounds, begin, loaded):
        par = lax.bitwise_and(c, 1)

        def tile(n, norm):
            @pl.when(n + ahead < n_tiles)
            def _():
                fetch(n + ahead).start()
            with jax.named_scope('w_wd'):
                fetch(n).wait()
            g = n // 2
            away = lax.rem(n, 2) == 0
            count = c * UNITS + g
            stage = lax.rem(count, 2)
            u = jnp.where(away, 2 * UNITS + stage, par * UNITS + g)

            @pl.when(away & (count >= 2))
            def _():
                await_copy(pp.at[u], s_stage.at[stage])
            if norm:
                norm_some(v, pl.multiple_of((n - 2) * norm_rows, 16))
            pp[u] = dot(lhs[...], place(n)[...]).astype(BF)

            @pl.when(away)
            def _():
                to = par * UNITS + g
                remote(pp.at[u], xp.at[to], s_stage.at[stage], s_xp.at[to], partner).start()
            run_slots(*bounds(n))

        def plain(n, _):
            tile(n, False)
            return 0

        def normed(n, _):
            tile(n, True)
            return 0
        lax.fori_loop(0, 1, plain, 0)
        begin()
        lax.fori_loop(1, 2, plain, 0)
        loaded()
        lax.fori_loop(2, n_tiles, normed, 0)

    def turned(v, gain):
        v = v * lax.rsqrt(jnp.mean(v * v, axis=-1, keepdims=True) + EPSILON) * gain[...].astype(F32)[None]
        return v * cosb[...] + pltpu.roll(v, lanes // 2, 1) * sinb[...]

    def rope_rows(i):
        where = jnp.broadcast_to(positions[pl.ds(i, 1), :].astype(F32), (lanes, seq)).T * freq[...]
        sine = jnp.sin(where)
        cosb[...] = jnp.cos(where)
        sinb[...] = jnp.where(lax.broadcasted_iota(jnp.int32, (seq, lanes), 1) < lanes // 2, -sine, sine)

    def keep_kv(y, length):
        k_rot = turned(y[:, :lanes], k_gain)
        v_val = y[:, lanes:]
        kk[...] = k_rot.astype(BF)
        vt[...] = v_val.T.astype(BF)
        valid = lax.broadcasted_iota(jnp.int32, (seq, lanes), 0) < length
        seen[...] = jnp.where(valid, 1.0, 0.0)
        kco[...] = jnp.where(valid, k_rot, 0.0).astype(BF)
        vco[...] = jnp.where(valid, v_val, 0.0).astype(BF)

    def keep_q(t, y):
        for s in range(TILE // lanes):
            qs[:, pl.ds(pl.multiple_of(t * TILE + s * lanes, lanes), lanes)] = turned(y[:, s * lanes:(s + 1) * lanes], q_gain).astype(BF)

    def attend(hd):
        cols = pl.ds(pl.multiple_of(hd * lanes, lanes), lanes)
        for lo in range(0, seq, span_q):
            hi = lo + span_q
            q = qs[lo:hi, cols]
            s = dot_nt(kk[:hi, :], q)
            parts = [jnp.where((seen[lo:hi, :span_q] > 0.0) & (tri[...] > 0.0), s[lo:hi, :], hidden_score)]
            for r in range(0, lo, span_q):
                parts.append(jnp.where(seen[r:r + span_q, :span_q] > 0.0, s[r:r + span_q, :], hidden_score))
            top = parts[0].max(0, keepdims=True)
            for x in parts[1:]:
                top = jnp.maximum(top, x.max(0, keepdims=True))
            parts = [jnp.exp2((x - top) * to_exp2) for x in parts]
            total = parts[0].sum(0, keepdims=True)
            for x in parts[1:]:
                total = total + x.sum(0, keepdims=True)
            scale = 1.0 / total
            probs = [(x * scale).astype(BF) for x in parts[1:] + parts[:1]]
            probs = jnp.concatenate(probs, axis=0) if len(probs) > 1 else probs[0]
            os[lo:hi, cols] = dot(vt[:, :hi], probs).T.astype(BF)

    step_a = (per_ar + lead - UNITS + 1) // (prompts - 1)
    w_q, w_h, w_o = 4, 7, 2
    weight_a = w_q * (q_tiles + 1) + w_h * (heads // HEADS_AT_ONCE) + w_o * n_tiles

    with jax.named_scope('norm_x'):
        norm_all(0)
    pl.semaphore_wait(barrier, 3)
    for n in range(o_bufs - 1):
        o_tile(n).start()
    for i in range(prompts):
        for g in range(UNITS):
            rows = pl.ds(pl.multiple_of(i * seq + ring * rows_b, rows_b), rows_b)
            cols = pl.ds(pl.multiple_of(core * half + g * unit, unit), unit)
            local(tokens.at[rows, cols], ownh.at[i * UNITS + g], s_res.at[i * UNITS + g]).start()

    def attention_phase(i, _):
        def upto(w):
            return jnp.where(i == 0, 0, UNITS - 1 + (i - 1) * step_a + over(w * step_a, weight_a))
        length = lens[i]
        def kv_body(t, _):
            start_all(a_tile(A_BUFS - 1))
            with jax.named_scope('qkv'):
                wait_all(a_tile(0))
                rope_rows(i)
                ybuf[0] = dot(n2[...], a_place(0)[1][...])
            return 0
        lax.fori_loop(i, i + 1, kv_body, 0)

        def q0_body(t, _):
            start_all(a_tile(A_BUFS))
            with jax.named_scope('qkv'):
                wait_all(a_tile(1))
                keep_kv(ybuf[0], length)
                ybuf[1] = dot(n2[...], a_place(1)[1][...])
            return 0
        lax.fori_loop(i, i + 1, q0_body, 0)
        run_slots(upto(0), upto(2 * w_q))

        def q_body(t, _):
            with jax.named_scope('qkv'):
                wait_all(a_tile(t))
                keep_q(t - 2, ybuf[lax.rem(t - 1, 2)])
                ybuf[lax.rem(t, 2)] = dot(n2[...], a_place(t)[1][...])
            run_slots(upto(t * w_q), upto((t + 1) * w_q))
            return 0
        lax.fori_loop(2, q_tiles + 1, q_body, 0)

        @pl.when(i + 1 < prompts)
        def _():
            start_all(load_rows(tokens, i + 1))
            for t in range(A_BUFS - 1):
                start_all(a_tile(t))

        @pl.when(i + 1 == prompts)
        def _():
            start_all(f_tile(0))
        rows = pl.ds(pl.multiple_of(i * seq, seq), seq)
        caches = (local(kco, kc.at[rows, :], s_kv.at[0]), local(vco, vc.at[rows, :], s_kv.at[1]))
        start_all(caches)
        with jax.named_scope('keep_q'):
            keep_q(q_tiles - 1, ybuf[q_tiles % 2])
        base1 = (q_tiles + 1) * w_q

        def heads_body(t, _):
            with jax.named_scope('attend'):
                for hd in range(HEADS_AT_ONCE):
                    attend(t * HEADS_AT_ONCE + hd)
            run_slots(upto(base1 + t * w_h), upto(base1 + (t + 1) * w_h))
            return 0
        lax.fori_loop(0, heads // HEADS_AT_ONCE, heads_body, 0)
        base = base1 + heads // HEADS_AT_ONCE * w_h
        wait_all(caches)

        def bounds(n):
            early = lax.shift_right_logical(jnp.maximum(n - 2, 0), 1), lax.shift_right_logical(jnp.maximum(n - 1, 0), 1)
            return (jnp.where(i == 0, early[0], upto(base + n * w_o)),
                    jnp.where(i == 0, early[1], upto(base + (n + 1) * w_o)))

        def loaded():
            @pl.when(i + 1 < prompts)
            def _():
                wait_all(load_rows(tokens, i + 1))
        with jax.named_scope('project_o'):
            project(os, o_tile, o_place, o_bufs - 1, i, 0, bounds, lambda: None, loaded)

        @pl.when(i + 1 < prompts)
        def _():
            for n in range(o_bufs - 1):
                o_tile(n).start()

        @pl.when(i + 1 == prompts)
        def _():
            d_tile(0).start()
        return 0
    lax.fori_loop(0, prompts, attention_phase, 0)

    a_end = UNITS - 1 + (prompts - 1) * step_a
    with jax.named_scope('pre_mlp'):
        run_slots(a_end, per_ar + lead)
    start_all(load_rows(ho, 0))
    with jax.named_scope('norm_h'):
        norm_all(1)
    starts = [(m + 1) * per_ar + v for m, v in zip(range(prompts), (lead, 20, 34))]
    mids = [(m + 2) * per_ar + v for m, v in zip(range(prompts), (3, 17, 30))]
    ones = [max((m + 2) * per_ar + lead, mids[m] + 2) if m + 1 < prompts else mids[m] for m in range(prompts)]
    ends = starts[1:] + [last * per_ar + UNITS * UNITS]

    soon = [0, 0, 1]
    for g in range(1, UNITS):
        soon += [g * UNITS, g * UNITS + (g + 2) // 2]
    soon = soon[:n_tiles] + [UNITS * UNITS]

    def mlp_phase(i, _):
        k0, k1, kt, k2 = pick(i, starts), pick(i, mids), pick(i, ones), pick(i, ends)

        def gated(y, width):
            gate, up = y[:, :width], y[:, width:]
            return (gate * jax.nn.sigmoid(gate) * up).astype(BF)

        def f_body(t, _):
            @pl.when(t + 1 < f_tiles)
            def _():
                start_all(f_tile(t + 1))
            if odd:
                @pl.when(t + 1 == f_tiles)
                def _():
                    start_all(f_rest())
            with jax.named_scope('w_gu'):
                wait_all(f_tile(t))
            act[:, pl.ds(pl.multiple_of(t * TILE, TILE), TILE)] = gated(dot(n2[...], gu[lax.rem(t, 2)]), TILE)
            run_slots(k0 + over(t * (k1 - k0), f_tiles), k0 + over((t + 1) * (k1 - k0), f_tiles))
            return 0
        with jax.named_scope('f_loop'):
            lax.fori_loop(0, f_tiles, f_body, 0)
        if odd:
            def rest_body(t, _):
                with jax.named_scope('f_rest'):
                    wait_all(f_rest())
                    act[:, f_tiles * TILE:] = gated(dot(n2[...], gu[f_tiles % 2, :, :TILE]), lanes)
                return 0
            lax.fori_loop(i, i + 1, rest_body, 0)

        @pl.when(i + 1 < prompts)
        def _():
            start_all(f_tile(0))

        def upto(n):
            spread = jnp.where(n <= 1, k1 + n * (kt - k1), kt + over(jnp.maximum(n - 1, 0) * (k2 - kt), n_tiles - 1))
            return jnp.where(i == prompts - 1, k1 + pick(n, soon), spread)

        def begin():
            @pl.when(i + 1 < prompts)
            def _():
                start_all(load_rows(ho, i + 1))

        def loaded():
            @pl.when(i + 1 < prompts)
            def _():
                wait_all(load_rows(ho, i + 1))
        with jax.named_scope('project_d'):
            project(act, d_tile, d_place, 1, prompts + i, 1, lambda n: (upto(n), upto(n + 1)), begin, loaded)

        @pl.when(i + 1 < prompts)
        def _():
            d_tile(0).start()
        return 0
    lax.fori_loop(0, prompts, mlp_phase, 0)

    with jax.named_scope('tail'):
        run_slots(last * per_ar + UNITS * UNITS, last * per_ar + (UNITS + HOPS - 1) * UNITS)

        def ring_end(g, _):
            pass_on(3, last, g)
            return 0
        lax.fori_loop(0, UNITS, ring_end, 0)

        def all_end(g, _):
            settle(last, g)
            return 0
        lax.fori_loop(0, UNITS, all_end, 0)
        for s in range(2):
            await_copy(pp.at[2 * UNITS + s], s_stage.at[s])


def copy_kernel(first, a, b, c, a_out, b_out, c_out, a_buf, b_buf, c_buf, s_in, s_out):
    pieces, rows = a_buf.shape[0], a_buf.shape[1]
    moves = [(a.at[pl.ds(first + p * rows, rows), :], a_buf.at[p], a_out.at[pl.ds(p * rows, rows), :]) for p in range(pieces)]
    moves += [(b, b_buf, b_out), (c, c_buf, c_out)]
    for m, (src, buf, _) in enumerate(moves):
        pltpu.make_async_copy(src, buf, s_in.at[m]).start()
    for m, (src, buf, dst) in enumerate(moves):
        pltpu.make_async_copy(src, buf, s_in.at[m]).wait()
        pltpu.make_async_copy(buf, dst, s_out.at[m]).start()
    for m, (_, buf, dst) in enumerate(moves):
        pltpu.make_async_copy(buf, dst, s_out.at[m]).wait()


def layer_body(tokens, positions, lengths, norm_attn, norm_mlp, q_gain, k_gain, w_query, w_key, w_value, w_out, w_gate, w_up, w_down, tp_size):
    prompts, seq, hidden = tokens.shape
    head_dim = q_gain.shape[0]
    width_q, width_f = w_query.shape[1], w_gate.shape[1]
    kv_heads = w_key.shape[1] // head_dim
    chips = tp_size // CORES
    unit = hidden // CORES // UNITS
    rows_n = prompts * seq
    inv_freq = ROPE_THETA ** (-np.arange(head_dim // 2) / (head_dim // 2))
    freq = jnp.asarray(np.concatenate([inv_freq, inv_freq])[None], F32)
    any_spec = pl.BlockSpec(memory_space=pl.ANY)
    vmem = pl.BlockSpec(memory_space=pltpu.VMEM)
    smem = pl.BlockSpec(memory_space=pltpu.SMEM)
    kernel = functools.partial(layer_kernel, tp_size, prompts, seq, head_dim, kv_heads, (hidden, width_q, width_f))
    dma = pltpu.SemaphoreType.DMA
    o_bufs = 2 * (width_f // width_q)
    span_q = min(head_dim, seq)
    ho, kc, vc = pl.pallas_call(
        kernel,
        name='decoder_layer',
        out_shape=(jax.ShapeDtypeStruct((2 * rows_n, hidden), BF),
                   jax.ShapeDtypeStruct((rows_n, head_dim), BF),
                   jax.ShapeDtypeStruct((rows_n, head_dim), BF)),
        in_specs=[any_spec, vmem, smem, vmem, vmem, vmem, vmem, vmem] + [any_spec] * 7,
        out_specs=(any_spec, any_spec, any_spec),
        scratch_shapes=[
            pltpu.VMEM((seq, hidden), BF),
            pltpu.VMEM((seq, width_f), BF),
            pltpu.VMEM((seq, width_q), BF), pltpu.VMEM((seq, width_q), BF),
            pltpu.VMEM((seq, head_dim), BF), pltpu.VMEM((head_dim, seq), BF),
            pltpu.VMEM((seq, head_dim), BF), pltpu.VMEM((seq, head_dim), BF),
            pltpu.VMEM((seq, head_dim), F32), pltpu.VMEM((seq, head_dim), F32),
            pltpu.VMEM((2, seq, TILE), F32),
            pltpu.VMEM((seq, head_dim), F32),
            pltpu.VMEM((span_q, span_q), F32),
            pltpu.VMEM((2, 16, hidden), F32),
            pltpu.VMEM((2, hidden, 2 * TILE), BF),
            pltpu.VMEM((2, width_f, unit), BF),
            pltpu.VMEM((2 * UNITS + 2, seq, unit), BF),
            pltpu.VMEM((2 * UNITS, seq, unit), BF),
            pltpu.VMEM((2, UNITS, 3, seq // chips, unit), BF),
            pltpu.VMEM((prompts * UNITS, seq // chips, unit), BF),
            dma((X_PARTS,)), dma((A_BUFS, 2)), dma((o_bufs,)), dma((2,)), dma((2 * UNITS,)), dma((prompts * UNITS,)), dma((2,)), dma((2, UNITS)),
            dma((2, UNITS, 3)), dma((2, UNITS, 3)), dma((2, UNITS, 3)), dma((2, UNITS, 3)), dma((2, UNITS, 4)), dma((2, UNITS, 4)),
        ],
        compiler_params=pltpu.CompilerParams(collective_id=0, has_side_effects=True, vmem_limit_bytes=67043328),
    )(tokens.reshape(rows_n, hidden), positions, lengths, norm_attn, norm_mlp, q_gain, k_gain, freq,
      w_query, w_key, w_value, w_out, w_gate, w_up, w_down)
    shape = (prompts, seq, 1, head_dim)
    parts = 4 * prompts
    block = rows_n // parts
    out, kc, vc = pl.pallas_call(
        functools.partial(copy_kernel, rows_n),
        name='copy_out',
        out_shape=(jax.ShapeDtypeStruct((rows_n, hidden), BF), jax.ShapeDtypeStruct(kc.shape, BF), jax.ShapeDtypeStruct(vc.shape, BF)),
        in_specs=[any_spec] * 3,
        out_specs=[any_spec] * 3,
        scratch_shapes=[pltpu.VMEM((parts, block, hidden), BF), pltpu.VMEM(kc.shape, BF), pltpu.VMEM(vc.shape, BF), dma((parts + 2,)), dma((parts + 2,))],
        compiler_params=pltpu.CompilerParams(vmem_limit_bytes=60 * 1024 * 1024),
    )(ho, kc, vc)
    return out.reshape(prompts, seq, hidden), kc.reshape(shape), vc.reshape(shape)


def solution(mesh):
    body = functools.partial(layer_body, tp_size=mesh.shape['tp'])
    in_specs = (P('dp', None, None), P('dp', None), P('dp'), P(), P(), P(), P(), P(None, 'tp'), P(), P(), P('tp', None), P(None, 'tp'), P(None, 'tp'), P('tp', None))
    out_specs = (P('dp', None, None), P('dp', None, 'tp', None), P('dp', None, 'tp', None))
    return jax.shard_map(body, mesh=mesh, in_specs=in_specs, out_specs=out_specs, check_vma=False)
```
